32 devices in a mesh: dp: 2 (over x), col: 4 (over z), row: 4 (over y, core).
Axes of the slice: x: 2, y: 2, z: 4, core: 2. Of those that a mesh axis runs over, the one named last changes fastest.
Arguments:
- hidden: bfloat16 [256, 1024], P('dp', 'row'), parts along dimension 0
- cache_len: int32 [256], P('dp'), parts along dimension 0
- k_cache: bfloat16 [2, 256, 16, 512, 64], P(None, 'dp', ('col', 'row')), parts along dimension 1
- v_cache: bfloat16 [2, 256, 16, 512, 64], P(None, 'dp', ('col', 'row')), parts along dimension 1
- ln1_g: bfloat16 [2, 1024], P(None, 'row')
- ln1_b: bfloat16 [2, 1024], P(None, 'row')
- w_q: bfloat16 [2, 1024, 1024], P(None, 'row', 'col')
- b_q: bfloat16 [2, 1024], P(None, 'col')
- w_k: bfloat16 [2, 1024, 1024], P(None, 'row', 'col')
- b_k: bfloat16 [2, 1024], P(None, 'col')
- w_v: bfloat16 [2, 1024, 1024], P(None, 'row', 'col')
- b_v: bfloat16 [2, 1024], P(None, 'col')
- w_o: bfloat16 [2, 1024, 1024], P(None, 'col', 'row')
- b_o: bfloat16 [2, 1024], P(None, 'row')
- ln2_g: bfloat16 [2, 1024], P(None, 'row')
- ln2_b: bfloat16 [2, 1024], P(None, 'row')
- w_fc1: bfloat16 [2, 1024, 4096], P(None, 'row', 'col')
- b_fc1: bfloat16 [2, 4096], P(None, 'col')
- w_fc2: bfloat16 [2, 4096, 1024], P(None, 'col', 'row')
- b_fc2: bfloat16 [2, 1024], P(None, 'row')
Outputs:
- output 1: bfloat16 [256, 1024], P('dp', 'row'), parts along dimension 0
- output 2: bfloat16 [2, 256, 16, 64], P(None, 'dp', ('col', 'row')), parts along dimension 1
- output 3: bfloat16 [2, 256, 16, 64], P(None, 'dp', ('col', 'row')), parts along dimension 1
There are 2 independent parts. The reference program is written for one: setup_inputs(seed, part) draws one part's arguments, and reference() takes and returns one part's arrays. A program takes and returns all parts, laid end to end along the dimension named above; an argument that names none is the same for every part.
All inputs are finite; a program needn't handle non-finite values.
Results may differ from the reference program's by a relative error of at most 0.0190479.
Values are sent between devices in bfloat16 or wider.
A program may use at most 1 GiB of HBM per device.

```python
import jax
import jax.numpy as jnp
from jax import lax

BATCH = 128
D_MODEL = 1024
HEADS = 16
S_MAX = 512
LAYERS = 2
HEAD_DIM = D_MODEL // HEADS
FF_DIM = 4 * D_MODEL
EPS_LN = 1e-5


def setup_inputs(seed: int = 0, part: int = 0) -> dict:
    shared_key = jax.random.key(seed)
    part_key = jax.random.fold_in(shared_key, part)
    part_keys = jax.random.split(part_key, 6)
    weight_keys = jax.random.split(shared_key, 16)

    def normal(rng_key, shape):
        return jax.random.normal(rng_key, shape, jnp.float32)

    def weight(rng_key, shape, fan_in, gain):
        return (gain * fan_in ** -0.5 * normal(rng_key, shape)).astype(jnp.bfloat16)

    def vector(rng_key, shape, center, spread):
        return (center + spread * normal(rng_key, shape)).astype(jnp.bfloat16)

    hidden = normal(part_keys[0], (BATCH, D_MODEL)) + 0.7 * normal(part_keys[1], (BATCH, 1))
    lengths = jax.random.randint(part_keys[2], (BATCH,), 0, S_MAX)
    lengths = lengths.at[0].set(S_MAX - 1).at[1].set(0)
    cache_shape = (LAYERS, BATCH, HEADS, S_MAX, HEAD_DIM)
    k_cache = 1.5 * normal(part_keys[3], cache_shape)
    v_cache = normal(part_keys[4], cache_shape) + 0.8 * normal(part_keys[5], (LAYERS, BATCH, HEADS, 1, HEAD_DIM))
    vec_shape = (LAYERS, D_MODEL)
    square_shape = (LAYERS, D_MODEL, D_MODEL)
    return {
        "hidden": hidden.astype(jnp.bfloat16),
        "cache_len": lengths.astype(jnp.int32),
        "k_cache": k_cache.astype(jnp.bfloat16),
        "v_cache": v_cache.astype(jnp.bfloat16),
        "ln1_g": vector(weight_keys[0], vec_shape, 1.0, 0.3),
        "ln1_b": vector(weight_keys[1], vec_shape, 0.0, 0.3),
        "w_q": weight(weight_keys[2], square_shape, D_MODEL, 1.5),
        "b_q": vector(weight_keys[3], vec_shape, 0.0, 0.5),
        "w_k": weight(weight_keys[4], square_shape, D_MODEL, 1.0),
        "b_k": vector(weight_keys[5], vec_shape, 0.0, 0.5),
        "w_v": weight(weight_keys[6], square_shape, D_MODEL, 1.0),
        "b_v": vector(weight_keys[7], vec_shape, 0.0, 0.5),
        "w_o": weight(weight_keys[8], square_shape, D_MODEL, 1.0),
        "b_o": vector(weight_keys[9], vec_shape, 0.0, 0.3),
        "ln2_g": vector(weight_keys[10], vec_shape, 1.0, 0.3),
        "ln2_b": vector(weight_keys[11], vec_shape, 0.0, 0.3),
        "w_fc1": weight(weight_keys[12], (LAYERS, D_MODEL, FF_DIM), D_MODEL, 1.0),
        "b_fc1": vector(weight_keys[13], (LAYERS, FF_DIM), 0.0, 0.5),
        "w_fc2": weight(weight_keys[14], (LAYERS, FF_DIM, D_MODEL), FF_DIM, 1.0),
        "b_fc2": vector(weight_keys[15], vec_shape, 0.0, 0.3),
    }


def layer_norm(state, gain, shift):
    state_f32 = state.astype(jnp.float32)
    mean_val = jnp.sum(state_f32, axis=-1, keepdims=True) / D_MODEL
    mean_sq = jnp.sum(state_f32 * state_f32, axis=-1, keepdims=True) / D_MODEL
    variance = mean_sq - mean_val * mean_val
    normed = (state_f32 - mean_val) * lax.rsqrt(variance + EPS_LN) * gain.astype(jnp.float32) + shift.astype(jnp.float32)
    return normed.astype(jnp.bfloat16)


def project(normed, weight, bias):
    return jnp.dot(normed, weight, preferred_element_type=jnp.float32) + bias.astype(jnp.float32)


def attend_row(row_args):
    q_row, k_row, v_row, k_fresh, v_fresh, length = row_args
    positions = jnp.arange(S_MAX)
    at_new = (positions == length)[None, :, None]
    keys_all = jnp.where(at_new, k_fresh[:, None, :], k_row)
    values_all = jnp.where(at_new, v_fresh[:, None, :], v_row)
    scores = jnp.einsum("hd,hsd->hs", q_row.astype(jnp.float32), keys_all.astype(jnp.float32))
    scores = jnp.where((positions <= length)[None, :], scores, -jnp.inf)
    probs = jax.nn.softmax(scores, axis=-1).astype(jnp.bfloat16)
    mixed = jnp.einsum("hs,hsd->hd", probs.astype(jnp.float32), values_all.astype(jnp.float32))
    return mixed.astype(jnp.bfloat16)


def reference(hidden, cache_len, k_cache, v_cache, ln1_g, ln1_b, w_q, b_q, w_k, b_k, w_v, b_v, w_o, b_o, ln2_g, ln2_b, w_fc1, b_fc1, w_fc2, b_fc2):
    scale = HEAD_DIM ** -0.5

    def layer_step(state, layer_args):
        (k_layer, v_layer, gain_one, shift_one, wq_layer, bq_layer, wk_layer, bk_layer, wv_layer, bv_layer,
         wo_layer, bo_layer, gain_two, shift_two, fc1_layer, bfc1_layer, fc2_layer, bfc2_layer) = layer_args
        normed = layer_norm(state, gain_one, shift_one)
        q_all = (project(normed, wq_layer, bq_layer) * scale).astype(jnp.bfloat16).reshape(BATCH, HEADS, HEAD_DIM)
        k_all = project(normed, wk_layer, bk_layer).astype(jnp.bfloat16).reshape(BATCH, HEADS, HEAD_DIM)
        v_all = project(normed, wv_layer, bv_layer).astype(jnp.bfloat16).reshape(BATCH, HEADS, HEAD_DIM)
        attended = lax.map(attend_row, (q_all, k_layer, v_layer, k_all, v_all, cache_len))
        state_mid = (state.astype(jnp.float32) + project(attended.reshape(BATCH, D_MODEL), wo_layer, bo_layer)).astype(jnp.bfloat16)
        normed_two = layer_norm(state_mid, gain_two, shift_two)
        inner = jnp.maximum(project(normed_two, fc1_layer, bfc1_layer).astype(jnp.bfloat16), 0)
        state_out = (state_mid.astype(jnp.float32) + project(inner, fc2_layer, bfc2_layer)).astype(jnp.bfloat16)
        return state_out, (k_all, v_all)

    layer_inputs = (k_cache, v_cache, ln1_g, ln1_b, w_q, b_q, w_k, b_k, w_v, b_v, w_o, b_o, ln2_g, ln2_b, w_fc1, b_fc1, w_fc2, b_fc2)
    state_final, fresh_rows = lax.scan(layer_step, hidden, layer_inputs)
    return state_final, fresh_rows[0], fresh_rows[1]
```

```python
import functools

import jax
import jax.numpy as jnp
from jax import lax
from jax.experimental import pallas as pl
from jax.experimental.pallas import tpu as pltpu
from jax.sharding import PartitionSpec as P

EPS_LN = 1e-5
MESH = pl.DeviceIdType.MESH
F32 = jnp.float32
BF16 = jnp.bfloat16

LAYERS = 2
BATCH = 128
STREAMS = 2
ROWS = BATCH // STREAMS
HALF = ROWS // 2
GROUP = 16
N_ROW = 4
N_COL = 4
HEAD = 64
SEQ = 512
WIDTH = 256
D_MODEL = 1024
FF_LOC = 1024

VEC_NAMES = ("g1", "b1", "bq", "bk", "bv", "bo", "g2", "b2", "bf2")
MAT_NAMES = ("wq", "wk", "wv", "wo", "wf1", "wf2")


def lane_iota(shape):
    return lax.broadcasted_iota(jnp.int32, shape, len(shape) - 1)


def swap_halves(val):
    return pltpu.roll(val, HEAD, 1)


def low_half(shape):
    return lane_iota(shape) < HEAD


def step_kernel(*refs):
    (x_in, len_in, k_in, v_in, g1_in, b1_in, wq_in, bq_in, wk_in, bk_in, wv_in, bv_in,
     wo_in, bo_in, g2_in, b2_in, wf1_in, bf1_in, wf2_in, bf2_in,
     h_out, k_out, v_out,
     x_buf, len_buf, k_buf, v_buf, g1, b1, wq, bq, wk, bk, wv, bv, wo, bo, g2, b2, wf1, bf1, wf2, bf2,
     len_mat, kf_buf, vf_buf, s_buf, p_buf, o_mix,
     st_send, st_recv, gb_send, gb_recv, qkv_send, qkv_recv, o_recv, proj_recv, f1_send, f1_recv, u_recv, out_recv,
     load_sem, big_sem, store_sem, send_sem, recv_sem) = refs

    row = lax.axis_index("row")
    col = lax.axis_index("col")

    loads = {}

    def load(name, src, dst, sem):
        copy = pltpu.make_async_copy(src, dst, sem)
        copy.start()
        loads[name] = copy

    n_load = [0]

    def small(name, src, dst):
        load(name, src, dst, load_sem.at[n_load[0]])
        n_load[0] += 1

    small("x", x_in, x_buf)
    small("g1", g1_in, g1)
    for layer in range(LAYERS):
        for name, src, dst in (("wq", wq_in, wq), ("wk", wk_in, wk), ("wv", wv_in, wv)):
            if layer == 0:
                small((name, layer), src.at[layer], dst.at[layer])
    for name, src, dst in (("b1", b1_in, b1), ("bq", bq_in, bq), ("bk", bk_in, bk), ("bv", bv_in, bv),
                           ("len", len_in, len_buf), ("bo", bo_in, bo), ("g2", g2_in, g2), ("b2", b2_in, b2),
                           ("bf1", bf1_in, bf1), ("bf2", bf2_in, bf2)):
        small(name, src, dst)

    barrier = pltpu.get_barrier_semaphore()
    for off in range(1, 4):
        pl.semaphore_signal(barrier, inc=1, device_id={"row": lax.rem(row + off, N_ROW)}, device_id_type=MESH)
        pl.semaphore_signal(barrier, inc=1, device_id={"col": lax.rem(col + off, N_COL)}, device_id_type=MESH)

    def big(layer, stream, which):
        src, dst = (k_in, k_buf) if which == 0 else (v_in, v_buf)
        span = pl.ds(stream * ROWS * HEAD, ROWS * HEAD)
        load(("kv", layer, stream, which), src.at[layer, span], dst.at[layer, span],
             big_sem.at[(layer * STREAMS + stream) * 2 + which])

    for stream in range(STREAMS):
        for which in range(2):
            big(0, stream, which)
    for name, src, dst in (("wo", wo_in, wo), ("wf1", wf1_in, wf1), ("wf2", wf2_in, wf2)):
        small((name, 0), src.at[0], dst.at[0])
    for name, src, dst in (("wq", wq_in, wq), ("wk", wk_in, wk), ("wv", wv_in, wv), ("wo", wo_in, wo),
                           ("wf1", wf1_in, wf1), ("wf2", wf2_in, wf2)):
        small((name, 1), src.at[1], dst.at[1])
    for stream in range(STREAMS):
        for which in range(2):
            big(1, stream, which)

    waited = set()

    def need(name):
        if name not in waited:
            waited.add(name)
            loads[name].wait()

    sends = []
    recvs = {}
    n_sem = [0]

    def exchange(tag, axis, src_of, dst_of):
        me = row if axis == "row" else col
        waits = []
        for off in (2, 3, 1):
            dest = lax.rem(me + off, 4)
            source = lax.rem(me + 4 - off, 4)
            index = n_sem[0]
            n_sem[0] += 1
            out = pltpu.make_async_remote_copy(
                src_ref=src_of(dest), dst_ref=dst_of(me), send_sem=send_sem.at[index],
                recv_sem=recv_sem.at[index], device_id={axis: dest}, device_id_type=MESH)
            out.start()
            sends.append(out)
            waits.append(pltpu.make_async_remote_copy(
                src_ref=src_of(dest), dst_ref=dst_of(source), send_sem=send_sem.at[index],
                recv_sem=recv_sem.at[index], device_id={axis: dest}, device_id_type=MESH))
        recvs[tag] = waits

    def arrived(tag):
        for copy in recvs[tag]:
            copy.wait_recv()

    def local_norm(state, gain):
        mean = jnp.sum(state, axis=-1, keepdims=True) * (1.0 / WIDTH)
        delta = state - mean
        var = jnp.sum(delta * delta, axis=-1, keepdims=True) * (1.0 / WIDTH)
        normed = (delta * lax.rsqrt(var + EPS_LN) * gain).astype(BF16)
        lanes = lane_iota((ROWS, 128))
        tile = jnp.where(lanes == 0, mean, jnp.where(lanes == 1, var, 0.0))
        if ROWS < 128:
            tile = jnp.concatenate([tile] * (128 // ROWS), axis=0)
        return normed, jnp.transpose(tile)[0:8]

    def stat_columns(stats):
        means = [stats[r, 0:1] for r in range(N_ROW)]
        variances = [stats[r, 1:2] for r in range(N_ROW)]
        mean = (means[0] + means[1] + means[2] + means[3]) * 0.25
        gaps = [m - mean for m in means]
        var = (variances[0] + variances[1] + variances[2] + variances[3]
               + gaps[0] * gaps[0] + gaps[1] * gaps[1] + gaps[2] * gaps[2] + gaps[3] * gaps[3]) * 0.25
        inv = lax.rsqrt(var + EPS_LN)
        lines = [jnp.sqrt(v + EPS_LN) * inv for v in variances] + [g * inv for g in gaps]
        sub = lax.broadcasted_iota(jnp.int32, (8, 128), 0)
        tile = jnp.zeros((8, 128), F32)
        for i, line in enumerate(lines):
            tile = jnp.where(sub == i, line, tile)
        turned = jnp.transpose(jnp.concatenate([tile] * 16, axis=0))[0:ROWS]
        return [turned[:, i:i + 1] for i in range(8)]

    def pack_heads(q, k, v, j, rows):
        half = rows // 2
        lo = (j // 2) * 128
        q, k, v = q[:, lo:lo + 128], k[:, lo:lo + 128], v[:, lo:lo + 128]
        if j % 2 == 0:
            first = jnp.where(low_half((rows, 128)), q, swap_halves(k))
            second = jnp.where(low_half((half, 128)), v[:half], swap_halves(v[half:]))
        else:
            first = jnp.where(low_half((rows, 128)), swap_halves(q), k)
            second = jnp.where(low_half((half, 128)), swap_halves(v[:half]), v[half:])
        return first, second

    def dot(a, b):
        return jnp.dot(a, b, preferred_element_type=F32)

    def send_qkv(layer, stream):
        slot = layer * STREAMS + stream
        need("x")
        need("g1")
        state = x_buf[stream * ROWS:(stream + 1) * ROWS, :].astype(F32)
        normed, tile = local_norm(state, g1[layer:layer + 1, :].astype(F32))
        st_send[2 * slot] = tile
        st_recv[2 * slot, row] = tile
        for name in ("wq", "wk", "wv"):
            need((name, layer))
        q, k, v = dot(normed, wq[layer]), dot(normed, wk[layer]), dot(normed, wv[layer])
        for j in range(N_ROW):
            first, second = pack_heads(q, k, v, j, ROWS)
            qkv_send[slot, j, 0:ROWS] = first.astype(BF16)
            qkv_send[slot, j, ROWS:ROWS + HALF] = second.astype(BF16)
        qkv_recv[slot, row] = qkv_send[slot, row]
        if layer == 0 and stream == 0:
            pl.semaphore_wait(barrier, 6)
        exchange(("st1", slot), "row", lambda d: st_send.at[2 * slot], lambda s: st_recv.at[2 * slot, s])
        exchange(("qkv", slot), "row", lambda d: qkv_send.at[slot, d], lambda s: qkv_recv.at[slot, s])

    def affine_rows(gain, shift):
        sub = lax.broadcasted_iota(jnp.int32, (16, WIDTH), 0)
        return jnp.where(sub == 0, gain.astype(F32), jnp.where(sub == 1, shift.astype(F32), 0.0)).astype(BF16)

    def send_affine(layer, kind):
        slot = layer * 2 + kind
        bias_on = jnp.where(row == 0, 1.0, 0.0)
        sub = lax.broadcasted_iota(jnp.int32, (8, 128), 0)
        if kind == 0:
            for name in ("b1", "bq", "bk", "bv"):
                need(name)
            rows = affine_rows(g1[layer:layer + 1, :], b1[layer:layer + 1, :])
            parts = []
            for w, b in ((wq, bq), (wk, bk), (wv, bv)):
                bias = b[layer:layer + 1, :].astype(F32) * bias_on
                part = dot(rows, w[layer])[0:8]
                sub_w = lax.broadcasted_iota(jnp.int32, (8, WIDTH), 0)
                parts.append(part + jnp.where(sub_w == 1, bias, 0.0))
            q, k, v = parts
            for j in range(N_ROW):
                lo = (j // 2) * 128
                qj, kj, vj = q[:, lo:lo + 128], k[:, lo:lo + 128], v[:, lo:lo + 128]
                if j % 2 == 0:
                    first = jnp.where(low_half((8, 128)), qj, swap_halves(kj))
                    second = jnp.where(low_half((8, 128)), vj, swap_halves(vj))
                else:
                    first = jnp.where(low_half((8, 128)), swap_halves(qj), kj)
                    second = jnp.where(low_half((8, 128)), swap_halves(vj), vj)
                gb_send[slot, j] = jnp.concatenate([first, second], axis=1)
        else:
            for name in ("g2", "b2", "bf1", ("wf1", layer)):
                need(name)
            rows = affine_rows(g2[layer:layer + 1, :], b2[layer:layer + 1, :])
            part = dot(rows, wf1[layer])[0:8]
            sub_w = lax.broadcasted_iota(jnp.int32, (8, FF_LOC), 0)
            part = part + jnp.where(sub_w == 1, bf1[layer:layer + 1, :].astype(F32) * bias_on, 0.0)
            for j in range(N_ROW):
                gb_send[slot, j] = part[:, j * WIDTH:(j + 1) * WIDTH]
        gb_recv[slot, row] = gb_send[slot, row]
        exchange(("gb", slot), "row", lambda d: gb_send.at[slot, d], lambda s: gb_recv.at[slot, s])

    gb_done = set()

    def affine_lines(layer, kind):
        slot = layer * 2 + kind
        if slot not in gb_done:
            gb_done.add(slot)
            arrived(("gb", slot))
        tiles = [gb_recv[slot, r] for r in range(N_ROW)]
        gains = [t[0:1] for t in tiles]
        const = tiles[0][1:2] + tiles[1][1:2] + tiles[2][1:2] + tiles[3][1:2]
        return gains, const

    def attend(layer, stream):
        slot = layer * STREAMS + stream
        span = slice(stream * ROWS, (stream + 1) * ROWS)
        arrived(("st1", slot))
        cols = stat_columns(st_recv[2 * slot])
        gains, const = affine_lines(layer, 0)
        arrived(("qkv", slot))
        low = low_half((HALF, 128))
        qk = const[:, 0:128]
        vv = const[:, 128:256]
        for r in range(N_ROW):
            part = qkv_recv[slot, r].astype(F32)
            scale, shift = cols[r], cols[4 + r]
            qk = qk + part[0:ROWS] * scale + shift * gains[r][:, 0:128]
            scale_v = jnp.where(low, scale[0:HALF], scale[HALF:ROWS])
            shift_v = jnp.where(low, shift[0:HALF], shift[HALF:ROWS])
            vv = vv + part[ROWS:ROWS + HALF] * scale_v + shift_v * gains[r][:, 128:256]
        full_low = low_half((ROWS, 128))
        qk_turn = swap_halves(qk)
        q2 = (jnp.where(full_low, qk, qk_turn) * (HEAD ** -0.5)).astype(BF16)
        k2 = jnp.where(full_low, qk_turn, qk).astype(BF16)
        vv_turn = swap_halves(vv)
        v2 = jnp.concatenate([jnp.where(low, vv, vv_turn), jnp.where(low, vv_turn, vv)], axis=0).astype(BF16)
        kf_buf[layer, span, :] = k2[:, 0:HEAD]
        vf_buf[layer, span, :] = v2[:, 0:HEAD]
        score_new = jnp.sum(jnp.where(full_low, q2.astype(F32) * k2.astype(F32), 0.0), axis=-1, keepdims=True)

        need(("kv", layer, stream, 0))
        q_row = lax.broadcasted_iota(jnp.int32, (GROUP, 128), 0)
        q_half = lane_iota((GROUP, 128)) // HEAD
        for g in range(ROWS // GROUP):
            base = (stream * ROWS + g * GROUP) * HEAD
            qg = q2[g * GROUP:(g + 1) * GROUP].astype(F32)
            spread = [jnp.where(q_row == 2 * j + q_half, qg, 0.0).astype(BF16) for j in range(GROUP // 2)]
            s_buf[g * GROUP:(g + 1) * GROUP, :] = dot(jnp.concatenate(spread, axis=1),
                                                      k_buf[layer, base:base + GROUP * HEAD, :])
        positions = lane_iota((ROWS, SEQ)).astype(F32)
        limit = len_mat[span, 0:1]
        scores = jnp.where(positions < limit, s_buf[...], -jnp.inf)
        peak = jnp.maximum(jnp.max(scores, axis=-1, keepdims=True), score_new)
        exp_cache = jnp.exp(scores - peak)
        exp_new = jnp.exp(score_new - peak)
        inv = 1.0 / (jnp.sum(exp_cache, axis=-1, keepdims=True) + exp_new)
        p_buf[...] = (exp_cache * inv).astype(BF16)
        prob_new = (exp_new * inv).astype(BF16).astype(F32)

        need(("kv", layer, stream, 1))
        for g in range(ROWS // GROUP):
            base = (stream * ROWS + g * GROUP) * HEAD
            wide = lax.dot_general(p_buf[g * GROUP:(g + 1) * GROUP, :], v_buf[layer, base:base + GROUP * HEAD, :],
                                   (((1,), (1,)), ((), ())), preferred_element_type=F32)
            acc = jnp.zeros((GROUP, 128), F32)
            for j in range(GROUP // 2):
                acc = acc + jnp.where(q_row == 2 * j + q_half, wide[:, j * 128:(j + 1) * 128], 0.0)
            o_mix[g * GROUP:(g + 1) * GROUP, :] = acc + swap_halves(acc)
        o2 = o_mix[...] + prob_new * v2.astype(F32)
        o_recv[slot, row] = jnp.where(low, o2[0:HALF], o2[HALF:ROWS]).astype(BF16)
        exchange(("o", slot), "row", lambda d: o_recv.at[slot, row], lambda s: o_recv.at[slot, s])

    def project(layer, stream):
        slot = layer * STREAMS + stream
        need(("wo", layer))
        arrived(("o", slot))
        low = low_half((HALF, 128))
        parts = [o_recv[slot, r].astype(F32) for r in range(N_ROW)]
        turns = [swap_halves(p) for p in parts]
        pairs = []
        for a, b in ((0, 1), (2, 3)):
            top = jnp.where(low, parts[a], turns[b])
            bottom = jnp.where(low, turns[a], parts[b])
            pairs.append(jnp.concatenate([top, bottom], axis=0).astype(BF16))
        proj_recv[slot, col] = dot(jnp.concatenate(pairs, axis=1), wo[layer]).astype(BF16)
        exchange(("proj", slot), "col", lambda d: proj_recv.at[slot, col], lambda s: proj_recv.at[slot, s])

    def residual(slot, buf, bias, stream):
        span = slice(stream * ROWS, (stream + 1) * ROWS)
        total = buf[slot, 0].astype(F32)
        for c in range(1, N_COL):
            total = total + buf[slot, c].astype(F32)
        new = (x_buf[span, :].astype(F32) + (total + bias)).astype(BF16)
        x_buf[span, :] = new
        return new.astype(F32)

    def send_inner(layer, stream):
        slot = layer * STREAMS + stream
        need("bo")
        need("g2")
        need(("wf1", layer))
        arrived(("proj", slot))
        state = residual(slot, proj_recv, bo[layer:layer + 1, :].astype(F32), stream)
        normed, tile = local_norm(state, g2[layer:layer + 1, :].astype(F32))
        st_send[2 * slot + 1] = tile
        st_recv[2 * slot + 1, row] = tile
        exchange(("st2", slot), "row", lambda d: st_send.at[2 * slot + 1], lambda s: st_recv.at[2 * slot + 1, s])
        for j in range(N_ROW):
            f1_send[slot, j] = dot(normed, wf1[layer, :, j * WIDTH:(j + 1) * WIDTH]).astype(BF16)
        f1_recv[slot, row] = f1_send[slot, row]
        exchange(("f1", slot), "row", lambda d: f1_send.at[slot, d], lambda s: f1_recv.at[slot, s])

    def send_act(layer, stream):
        slot = layer * STREAMS + stream
        arrived(("st2", slot))
        cols = stat_columns(st_recv[2 * slot + 1])
        gains, const = affine_lines(layer, 1)
        arrived(("f1", slot))
        total = const
        for r in range(N_ROW):
            total = total + f1_recv[slot, r].astype(F32) * cols[r] + cols[4 + r] * gains[r]
        u_recv[slot, row] = jnp.maximum(total, 0.0).astype(BF16)
        exchange(("u", slot), "row", lambda d: u_recv.at[slot, row], lambda s: u_recv.at[slot, s])

    def send_out(layer, stream):
        slot = layer * STREAMS + stream
        need(("wf2", layer))
        arrived(("u", slot))
        acc = dot(u_recv[slot, 0], wf2[layer, 0:WIDTH, :])
        for r in range(1, N_ROW):
            acc = acc + dot(u_recv[slot, r], wf2[layer, r * WIDTH:(r + 1) * WIDTH, :])
        out_recv[slot, col] = acc.astype(BF16)
        exchange(("out", slot), "col", lambda d: out_recv.at[slot, col], lambda s: out_recv.at[slot, s])

    def finish(layer, stream):
        slot = layer * STREAMS + stream
        need("bf2")
        arrived(("out", slot))
        residual(slot, out_recv, bf2[layer:layer + 1, :].astype(F32), stream)

    stores = []

    def store(src, dst, index):
        copy = pltpu.make_async_copy(src, dst, store_sem.at[index])
        copy.start()
        stores.append(copy)

    for stream in range(STREAMS):
        send_qkv(0, stream)
    send_affine(0, 0)
    need("len")
    len_mat[...] = jnp.transpose(jnp.broadcast_to(len_buf[...].astype(F32), (128, 128)))
    for layer in range(LAYERS):
        for stream in range(STREAMS):
            attend(layer, stream)
        store(kf_buf.at[layer], k_out.at[layer], 2 * layer)
        store(vf_buf.at[layer], v_out.at[layer], 2 * layer + 1)
        if layer == 0:
            send_affine(0, 1)
        for stream in range(STREAMS):
            project(layer, stream)
        if layer == 0:
            for name in MAT_NAMES[:3]:
                need((name, 1))
            send_affine(1, 0)
            send_affine(1, 1)
        for stream in range(STREAMS):
            send_inner(layer, stream)
        for stream in range(STREAMS):
            send_act(layer, stream)
        for stream in range(STREAMS):
            send_out(layer, stream)
        for stream in range(STREAMS):
            finish(layer, stream)
            if layer + 1 < LAYERS:
                send_qkv(layer + 1, stream)
            else:
                span = pl.ds(stream * ROWS, ROWS)
                store(x_buf.at[span], h_out.at[span], 2 * LAYERS + stream)
    for copy in stores:
        copy.wait()
    for copy in sends:
        copy.wait_send()


N_SLOT = LAYERS * STREAMS
N_COPY = 3 * (8 * N_SLOT - 0 + 2 * LAYERS)


def run_step(x, lens, k_cache, v_cache, g1, b1, wq, bq, wk, bk, wv, bv, wo, bo, g2, b2, wf1, bf1, wf2, bf2):
    any_spec = pl.BlockSpec(memory_space=pl.ANY)
    args = (x, lens.reshape(1, BATCH),
            jnp.swapaxes(k_cache, 3, 4).reshape(LAYERS, BATCH * HEAD, SEQ),
            jnp.swapaxes(v_cache, 3, 4).reshape(LAYERS, BATCH * HEAD, SEQ),
            g1, b1, wq, bq, wk, bk, wv, bv, wo, bo, g2, b2, wf1, bf1, wf2, bf2)
    vm = pltpu.VMEM
    in_scratch = [vm(a.shape, a.dtype) for a in args]
    scratch = in_scratch + [
        vm((BATCH, 128), F32),
        vm((LAYERS, BATCH, HEAD), BF16),
        vm((LAYERS, BATCH, HEAD), BF16),
        vm((ROWS, SEQ), F32),
        vm((ROWS, SEQ), BF16),
        vm((ROWS, 128), F32),
        vm((2 * N_SLOT, 8, 128), F32),
        vm((2 * N_SLOT, N_ROW, 8, 128), F32),
        vm((2 * LAYERS, N_ROW, 8, WIDTH), F32),
        vm((2 * LAYERS, N_ROW, 8, WIDTH), F32),
        vm((N_SLOT, N_ROW, ROWS + HALF, 128), BF16),
        vm((N_SLOT, N_ROW, ROWS + HALF, 128), BF16),
        vm((N_SLOT, N_ROW, HALF, 128), BF16),
        vm((N_SLOT, N_COL, ROWS, WIDTH), BF16),
        vm((N_SLOT, N_ROW, ROWS, WIDTH), BF16),
        vm((N_SLOT, N_ROW, ROWS, WIDTH), BF16),
        vm((N_SLOT, N_ROW, ROWS, WIDTH), BF16),
        vm((N_SLOT, N_COL, ROWS, WIDTH), BF16),
        pltpu.SemaphoreType.DMA((32,)),
        pltpu.SemaphoreType.DMA((2 * N_SLOT,)),
        pltpu.SemaphoreType.DMA((2 * LAYERS + STREAMS,)),
        pltpu.SemaphoreType.DMA((N_COPY,)),
        pltpu.SemaphoreType.DMA((N_COPY,)),
    ]
    h_out, k_new, v_new = pl.pallas_call(
        step_kernel,
        out_shape=(jax.ShapeDtypeStruct((BATCH, WIDTH), BF16),
                   jax.ShapeDtypeStruct((LAYERS, BATCH, HEAD), BF16),
                   jax.ShapeDtypeStruct((LAYERS, BATCH, HEAD), BF16)),
        in_specs=[any_spec] * len(args),
        out_specs=(any_spec,) * 3,
        scratch_shapes=scratch,
        compiler_params=pltpu.CompilerParams(
            collective_id=0, has_side_effects=True, vmem_limit_bytes=60 * 1024 * 1024),
        name="decode_step",
    )(*args)
    return h_out, k_new.reshape(LAYERS, BATCH, 1, HEAD), v_new.reshape(LAYERS, BATCH, 1, HEAD)


def solution(mesh):
    act_spec = P("dp", "row")
    cache_spec = P(None, "dp", ("col", "row"), None, None)
    fresh_spec = P(None, "dp", ("col", "row"), None)
    in_weight = P(None, "row", "col")
    out_weight = P(None, "col", "row")
    col_vec = P(None, "col")
    row_vec = P(None, "row")
    in_specs = (act_spec, P("dp"), cache_spec, cache_spec, row_vec, row_vec,
                in_weight, col_vec, in_weight, col_vec, in_weight, col_vec,
                out_weight, row_vec, row_vec, row_vec, in_weight, col_vec, out_weight, row_vec)
    return jax.shard_map(run_step, mesh=mesh, in_specs=in_specs,
                         out_specs=(act_spec, fresh_spec, fresh_spec), check_vma=False)
```

```python
import functools

import jax
import jax.numpy as jnp
from jax import lax
from jax.experimental import pallas as pl
from jax.experimental.pallas import tpu as pltpu
from jax.sharding import PartitionSpec as P

EPS_LN = 1e-5
MESH = pl.DeviceIdType.MESH
F32 = jnp.float32
BF16 = jnp.bfloat16

LAYERS = 2
BATCH = 128
STREAMS = 4
ROWS = BATCH // STREAMS
HALF = ROWS // 2
GROUP = 16
N_ROW = 4
N_COL = 4
HEAD = 64
SEQ = 512
WIDTH = 256
D_MODEL = 1024
FF_LOC = 1024

VEC_NAMES = ("g1", "b1", "bq", "bk", "bv", "bo", "g2", "b2", "bf2")
MAT_NAMES = ("wq", "wk", "wv", "wo", "wf1", "wf2")


def lane_iota(shape):
    return lax.broadcasted_iota(jnp.int32, shape, len(shape) - 1)


def swap_halves(val):
    return pltpu.roll(val, HEAD, 1)


def low_half(shape):
    return lane_iota(shape) < HEAD


def step_kernel(*refs):
    (x_in, len_in, k_in, v_in, g1_in, b1_in, wq_in, bq_in, wk_in, bk_in, wv_in, bv_in,
     wo_in, bo_in, g2_in, b2_in, wf1_in, bf1_in, wf2_in, bf2_in,
     h_out, k_out, v_out,
     x_buf, len_buf, k_buf, v_buf, g1, b1, wq, bq, wk, bk, wv, bv, wo, bo, g2, b2, wf1, bf1, wf2, bf2,
     len_mat, kv_mix, kv_turn, s_buf, p_buf, o_mix,
     st_send, st_recv, gb_send, gb_recv, qkv_send, qkv_recv, o_recv, proj_recv, f1_send, f1_recv, u_recv, out_recv,
     load_sem, big_sem, store_sem, send_sem, recv_sem) = refs

    row = lax.axis_index("row")
    col = lax.axis_index("col")

    loads = {}

    def load(name, src, dst, sem):
        copy = pltpu.make_async_copy(src, dst, sem)
        copy.start()
        loads[name] = copy

    n_load = [0]

    def small(name, src, dst):
        load(name, src, dst, load_sem.at[n_load[0]])
        n_load[0] += 1

    small("x", x_in, x_buf)
    small("g1", g1_in, g1)
    for layer in range(LAYERS):
        for name, src, dst in (("wq", wq_in, wq), ("wk", wk_in, wk), ("wv", wv_in, wv)):
            if layer == 0:
                small((name, layer), src.at[layer], dst.at[layer])
    for name, src, dst in (("b1", b1_in, b1), ("bq", bq_in, bq), ("bk", bk_in, bk), ("bv", bv_in, bv),
                           ("len", len_in, len_buf), ("bo", bo_in, bo), ("g2", g2_in, g2), ("b2", b2_in, b2),
                           ("bf1", bf1_in, bf1), ("bf2", bf2_in, bf2)):
        small(name, src, dst)

    barrier = pltpu.get_barrier_semaphore()
    for off in range(1, 4):
        pl.semaphore_signal(barrier, inc=1, device_id={"row": lax.rem(row + off, N_ROW)}, device_id_type=MESH)
        pl.semaphore_signal(barrier, inc=1, device_id={"col": lax.rem(col + off, N_COL)}, device_id_type=MESH)

    def big(layer, stream, which):
        src, dst = (k_in, k_buf) if which == 0 else (v_in, v_buf)
        span = pl.ds(stream * ROWS * HEAD, ROWS * HEAD)
        load(("kv", layer, stream, which), src.at[layer, span], dst.at[layer, span],
             big_sem.at[(layer * STREAMS + stream) * 2 + which])

    for stream in range(STREAMS):
        for which in range(2):
            big(0, stream, which)
    for name, src, dst in (("wo", wo_in, wo), ("wf1", wf1_in, wf1), ("wf2", wf2_in, wf2)):
        small((name, 0), src.at[0], dst.at[0])
    for name, src, dst in (("wq", wq_in, wq), ("wk", wk_in, wk), ("wv", wv_in, wv), ("wo", wo_in, wo),
                           ("wf1", wf1_in, wf1), ("wf2", wf2_in, wf2)):
        small((name, 1), src.at[1], dst.at[1])
    for stream in range(STREAMS):
        for which in range(2):
            big(1, stream, which)

    waited = set()

    def need(name):
        if name not in waited:
            waited.add(name)
            loads[name].wait()

    sends = []
    recvs = {}
    n_sem = [0]

    def exchange(tag, axis, src_of, dst_of):
        me = row if axis == "row" else col
        waits = []
        for off in (2, 3, 1):
            dest = lax.rem(me + off, 4)
            source = lax.rem(me + 4 - off, 4)
            index = n_sem[0]
            n_sem[0] += 1
            out = pltpu.make_async_remote_copy(
                src_ref=src_of(dest), dst_ref=dst_of(me), send_sem=send_sem.at[index],
                recv_sem=recv_sem.at[index], device_id={axis: dest}, device_id_type=MESH)
            out.start()
            sends.append(out)
            waits.append(pltpu.make_async_remote_copy(
                src_ref=src_of(dest), dst_ref=dst_of(source), send_sem=send_sem.at[index],
                recv_sem=recv_sem.at[index], device_id={axis: dest}, device_id_type=MESH))
        recvs[tag] = waits

    def arrived(tag):
        for copy in recvs[tag]:
            copy.wait_recv()

    def local_norm(state, gain):
        mean = jnp.sum(state, axis=-1, keepdims=True) * (1.0 / WIDTH)
        delta = state - mean
        var = jnp.sum(delta * delta, axis=-1, keepdims=True) * (1.0 / WIDTH)
        normed = (delta * lax.rsqrt(var + EPS_LN) * gain).astype(BF16)
        lanes = lane_iota((ROWS, 128))
        tile = jnp.where(lanes == 0, mean, jnp.where(lanes == 1, var, 0.0))
        if ROWS < 128:
            tile = jnp.concatenate([tile] * (128 // ROWS), axis=0)
        return normed, jnp.transpose(tile)[0:8]

    def stat_columns(stats):
        means = [stats[r, 0:1] for r in range(N_ROW)]
        variances = [stats[r, 1:2] for r in range(N_ROW)]
        mean = (means[0] + means[1] + means[2] + means[3]) * 0.25
        gaps = [m - mean for m in means]
        var = (variances[0] + variances[1] + variances[2] + variances[3]
               + gaps[0] * gaps[0] + gaps[1] * gaps[1] + gaps[2] * gaps[2] + gaps[3] * gaps[3]) * 0.25
        inv = lax.rsqrt(var + EPS_LN)
        lines = [jnp.sqrt(v + EPS_LN) * inv for v in variances] + [g * inv for g in gaps]
        sub = lax.broadcasted_iota(jnp.int32, (8, 128), 0)
        tile = jnp.zeros((8, 128), F32)
        for i, line in enumerate(lines):
            tile = jnp.where(sub == i, line, tile)
        turned = jnp.transpose(jnp.concatenate([tile] * 16, axis=0))[0:ROWS]
        return [turned[:, i:i + 1] for i in range(8)]

    def pack_heads(q, k, v, j, rows):
        half = rows // 2
        lo = (j // 2) * 128
        q, k, v = q[:, lo:lo + 128], k[:, lo:lo + 128], v[:, lo:lo + 128]
        if j % 2 == 0:
            first = jnp.where(low_half((rows, 128)), q, swap_halves(k))
            second = jnp.where(low_half((half, 128)), v[:half], swap_halves(v[half:]))
        else:
            first = jnp.where(low_half((rows, 128)), swap_halves(q), k)
            second = jnp.where(low_half((half, 128)), swap_halves(v[:half]), v[half:])
        return first, second

    def dot(a, b):
        return jnp.dot(a, b, preferred_element_type=F32)

    def send_qkv(layer, stream):
        slot = layer * STREAMS + stream
        need("x")
        need("g1")
        state = x_buf[stream * ROWS:(stream + 1) * ROWS, :].astype(F32)
        normed, tile = local_norm(state, g1[layer:layer + 1, :].astype(F32))
        st_send[2 * slot] = tile
        st_recv[2 * slot, row] = tile
        for name in ("wq", "wk", "wv"):
            need((name, layer))
        q, k, v = dot(normed, wq[layer]), dot(normed, wk[layer]), dot(normed, wv[layer])
        for j in range(N_ROW):
            first, second = pack_heads(q, k, v, j, ROWS)
            qkv_send[slot, j, 0:ROWS] = first.astype(BF16)
            qkv_send[slot, j, ROWS:ROWS + HALF] = second.astype(BF16)
        qkv_recv[slot, row] = qkv_send[slot, row]
        if layer == 0 and stream == 0:
            pl.semaphore_wait(barrier, 6)
        exchange(("st1", slot), "row", lambda d: st_send.at[2 * slot], lambda s: st_recv.at[2 * slot, s])
        exchange(("qkv", slot), "row", lambda d: qkv_send.at[slot, d], lambda s: qkv_recv.at[slot, s])

    def affine_rows(gain, shift):
        sub = lax.broadcasted_iota(jnp.int32, (16, WIDTH), 0)
        return jnp.where(sub == 0, gain.astype(F32), jnp.where(sub == 1, shift.astype(F32), 0.0)).astype(BF16)

    def send_affine(layer, kind):
        slot = layer * 2 + kind
        bias_on = jnp.where(row == 0, 1.0, 0.0)
        sub = lax.broadcasted_iota(jnp.int32, (8, 128), 0)
        if kind == 0:
            for name in ("b1", "bq", "bk", "bv"):
                need(name)
            rows = affine_rows(g1[layer:layer + 1, :], b1[layer:layer + 1, :])
            parts = []
            for w, b in ((wq, bq), (wk, bk), (wv, bv)):
                bias = b[layer:layer + 1, :].astype(F32) * bias_on
                part = dot(rows, w[layer])[0:8]
                sub_w = lax.broadcasted_iota(jnp.int32, (8, WIDTH), 0)
                parts.append(part + jnp.where(sub_w == 1, bias, 0.0))
            q, k, v = parts
            for j in range(N_ROW):
                lo = (j // 2) * 128
                qj, kj, vj = q[:, lo:lo + 128], k[:, lo:lo + 128], v[:, lo:lo + 128]
                if j % 2 == 0:
                    first = jnp.where(low_half((8, 128)), qj, swap_halves(kj))
                    second = jnp.where(low_half((8, 128)), vj, swap_halves(vj))
                else:
                    first = jnp.where(low_half((8, 128)), swap_halves(qj), kj)
                    second = jnp.where(low_half((8, 128)), swap_halves(vj), vj)
                gb_send[slot, j] = jnp.concatenate([first, second], axis=1)
        else:
            for name in ("g2", "b2", "bf1", ("wf1", layer)):
                need(name)
            rows = affine_rows(g2[layer:layer + 1, :], b2[layer:layer + 1, :])
            part = dot(rows, wf1[layer])[0:8]
            sub_w = lax.broadcasted_iota(jnp.int32, (8, FF_LOC), 0)
            part = part + jnp.where(sub_w == 1, bf1[layer:layer + 1, :].astype(F32) * bias_on, 0.0)
            for j in range(N_ROW):
                gb_send[slot, j] = part[:, j * WIDTH:(j + 1) * WIDTH]
        gb_recv[slot, row] = gb_send[slot, row]
        exchange(("gb", slot), "row", lambda d: gb_send.at[slot, d], lambda s: gb_recv.at[slot, s])

    gb_done = set()

    def affine_lines(layer, kind):
        slot = layer * 2 + kind
        if slot not in gb_done:
            gb_done.add(slot)
            arrived(("gb", slot))
        tiles = [gb_recv[slot, r] for r in range(N_ROW)]
        gains = [t[0:1] for t in tiles]
        const = tiles[0][1:2] + tiles[1][1:2] + tiles[2][1:2] + tiles[3][1:2]
        return gains, const

    def attend(layer, stream):
        slot = layer * STREAMS + stream
        span = slice(stream * ROWS, (stream + 1) * ROWS)
        arrived(("st1", slot))
        cols = stat_columns(st_recv[2 * slot])
        gains, const = affine_lines(layer, 0)
        arrived(("qkv", slot))
        low = low_half((HALF, 128))
        qk = const[:, 0:128]
        vv = const[:, 128:256]
        for r in range(N_ROW):
            part = qkv_recv[slot, r].astype(F32)
            scale, shift = cols[r], cols[4 + r]
            qk = qk + part[0:ROWS] * scale + shift * gains[r][:, 0:128]
            scale_v = jnp.where(low, scale[0:HALF], scale[HALF:ROWS])
            shift_v = jnp.where(low, shift[0:HALF], shift[HALF:ROWS])
            vv = vv + part[ROWS:ROWS + HALF] * scale_v + shift_v * gains[r][:, 128:256]
        full_low = low_half((ROWS, 128))
        qk_turn = swap_halves(qk)
        q2 = (jnp.where(full_low, qk, qk_turn) * (HEAD ** -0.5)).astype(BF16)
        k2 = jnp.where(full_low, qk_turn, qk).astype(BF16)
        vv_turn = swap_halves(vv)
        v2 = jnp.concatenate([jnp.where(low, vv, vv_turn), jnp.where(low, vv_turn, vv)], axis=0).astype(BF16)
        kv_mix[layer, span, :] = jnp.where(full_low, k2.astype(F32), v2.astype(F32))
        score_new = jnp.sum(jnp.where(full_low, q2.astype(F32) * k2.astype(F32), 0.0), axis=-1, keepdims=True)

        need(("kv", layer, stream, 0))
        q_row = lax.broadcasted_iota(jnp.int32, (GROUP, 128), 0)
        q_half = lane_iota((GROUP, 128)) // HEAD
        for g in range(ROWS // GROUP):
            base = (stream * ROWS + g * GROUP) * HEAD
            qg = q2[g * GROUP:(g + 1) * GROUP].astype(F32)
            spread = [jnp.where(q_row == 2 * j + q_half, qg, 0.0).astype(BF16) for j in range(GROUP // 2)]
            s_buf[g * GROUP:(g + 1) * GROUP, :] = dot(jnp.concatenate(spread, axis=1),
                                                      k_buf[layer, base:base + GROUP * HEAD, :])
        positions = lane_iota((ROWS, SEQ)).astype(F32)
        limit = len_mat[span, 0:1]
        scores = jnp.where(positions < limit, s_buf[...], -jnp.inf)
        peak = jnp.maximum(jnp.max(scores, axis=-1, keepdims=True), score_new)
        exp_cache = jnp.exp(scores - peak)
        exp_new = jnp.exp(score_new - peak)
        inv = 1.0 / (jnp.sum(exp_cache, axis=-1, keepdims=True) + exp_new)
        p_buf[...] = (exp_cache * inv).astype(BF16)
        prob_new = (exp_new * inv).astype(BF16).astype(F32)

        need(("kv", layer, stream, 1))
        for g in range(ROWS // GROUP):
            base = (stream * ROWS + g * GROUP) * HEAD
            wide = lax.dot_general(p_buf[g * GROUP:(g + 1) * GROUP, :], v_buf[layer, base:base + GROUP * HEAD, :],
                                   (((1,), (1,)), ((), ())), preferred_element_type=F32)
            acc = jnp.zeros((GROUP, 128), F32)
            for j in range(GROUP // 2):
                acc = acc + jnp.where(q_row == 2 * j + q_half, wide[:, j * 128:(j + 1) * 128], 0.0)
            o_mix[g * GROUP:(g + 1) * GROUP, :] = acc + swap_halves(acc)
        o2 = o_mix[...] + prob_new * v2.astype(F32)
        o_recv[slot, row] = jnp.where(low, o2[0:HALF], o2[HALF:ROWS]).astype(BF16)
        exchange(("o", slot), "row", lambda d: o_recv.at[slot, row], lambda s: o_recv.at[slot, s])

    def project(layer, stream):
        slot = layer * STREAMS + stream
        need(("wo", layer))
        arrived(("o", slot))
        low = low_half((HALF, 128))
        parts = [o_recv[slot, r].astype(F32) for r in range(N_ROW)]
        turns = [swap_halves(p) for p in parts]
        pairs = []
        for a, b in ((0, 1), (2, 3)):
            top = jnp.where(low, parts[a], turns[b])
            bottom = jnp.where(low, turns[a], parts[b])
            pairs.append(jnp.concatenate([top, bottom], axis=0).astype(BF16))
        proj_recv[slot, col] = dot(jnp.concatenate(pairs, axis=1), wo[layer]).astype(BF16)
        exchange(("proj", slot), "col", lambda d: proj_recv.at[slot, col], lambda s: proj_recv.at[slot, s])

    def residual(slot, buf, bias, stream):
        span = slice(stream * ROWS, (stream + 1) * ROWS)
        total = buf[slot, 0].astype(F32)
        for c in range(1, N_COL):
            total = total + buf[slot, c].astype(F32)
        new = (x_buf[span, :].astype(F32) + (total + bias)).astype(BF16)
        x_buf[span, :] = new
        return new.astype(F32)

    def send_inner(layer, stream):
        slot = layer * STREAMS + stream
        need("bo")
        need("g2")
        need(("wf1", layer))
        arrived(("proj", slot))
        state = residual(slot, proj_recv, bo[layer:layer + 1, :].astype(F32), stream)
        normed, tile = local_norm(state, g2[layer:layer + 1, :].astype(F32))
        st_send[2 * slot + 1] = tile
        st_recv[2 * slot + 1, row] = tile
        exchange(("st2", slot), "row", lambda d: st_send.at[2 * slot + 1], lambda s: st_recv.at[2 * slot + 1, s])
        for j in range(N_ROW):
            f1_send[slot, j] = dot(normed, wf1[layer, :, j * WIDTH:(j + 1) * WIDTH]).astype(BF16)
        f1_recv[slot, row] = f1_send[slot, row]
        exchange(("f1", slot), "row", lambda d: f1_send.at[slot, d], lambda s: f1_recv.at[slot, s])

    def send_act(layer, stream):
        slot = layer * STREAMS + stream
        arrived(("st2", slot))
        cols = stat_columns(st_recv[2 * slot + 1])
        gains, const = affine_lines(layer, 1)
        arrived(("f1", slot))
        total = const
        for r in range(N_ROW):
            total = total + f1_recv[slot, r].astype(F32) * cols[r] + cols[4 + r] * gains[r]
        u_recv[slot, row] = jnp.maximum(total, 0.0).astype(BF16)
        exchange(("u", slot), "row", lambda d: u_recv.at[slot, row], lambda s: u_recv.at[slot, s])

    def send_out(layer, stream):
        slot = layer * STREAMS + stream
        need(("wf2", layer))
        arrived(("u", slot))
        acc = dot(u_recv[slot, 0], wf2[layer, 0:WIDTH, :])
        for r in range(1, N_ROW):
            acc = acc + dot(u_recv[slot, r], wf2[layer, r * WIDTH:(r + 1) * WIDTH, :])
        out_recv[slot, col] = acc.astype(BF16)
        exchange(("out", slot), "col", lambda d: out_recv.at[slot, col], lambda s: out_recv.at[slot, s])

    def finish(layer, stream):
        slot = layer * STREAMS + stream
        need("bf2")
        arrived(("out", slot))
        residual(slot, out_recv, bf2[layer:layer + 1, :].astype(F32), stream)

    stores = []

    def store(src, dst, index):
        copy = pltpu.make_async_copy(src, dst, store_sem.at[index])
        copy.start()
        stores.append(copy)

    for stream in range(STREAMS):
        send_qkv(0, stream)
    send_affine(0, 0)
    need("len")
    len_mat[...] = jnp.transpose(jnp.broadcast_to(len_buf[...].astype(F32), (128, 128)))
    for layer in range(LAYERS):
        for stream in range(STREAMS):
            attend(layer, stream)
        kv_turn[layer] = jnp.transpose(kv_mix[layer]).astype(BF16)
        store(kv_turn.at[layer, 0:HEAD], k_out.at[layer], 2 * layer)
        store(kv_turn.at[layer, HEAD:2 * HEAD], v_out.at[layer], 2 * layer + 1)
        if layer == 0:
            send_affine(0, 1)
        for stream in range(STREAMS):
            project(layer, stream)
        if layer == 0:
            for name in MAT_NAMES[:3]:
                need((name, 1))
            send_affine(1, 0)
            send_affine(1, 1)
        for stream in range(STREAMS):
            send_inner(layer, stream)
        for stream in range(STREAMS):
            send_act(layer, stream)
        for stream in range(STREAMS):
            send_out(layer, stream)
        for stream in range(STREAMS):
            finish(layer, stream)
            if layer + 1 < LAYERS:
                send_qkv(layer + 1, stream)
            else:
                span = pl.ds(stream * ROWS, ROWS)
                store(x_buf.at[span], h_out.at[span], 2 * LAYERS + stream)
    for copy in stores:
        copy.wait()
    for copy in sends:
        copy.wait_send()


N_SLOT = LAYERS * STREAMS
N_COPY = 3 * (8 * N_SLOT - 0 + 2 * LAYERS)


def emit_kernel(h_in, k_in, v_in, h_out, k_out, v_out, sem):
    copies = [pltpu.make_async_copy(src, dst, sem.at[i])
              for i, (src, dst) in enumerate(((h_in, h_out), (k_in, k_out), (v_in, v_out)))]
    for copy in copies:
        copy.start()
    for copy in copies:
        copy.wait()


def run_step(x, lens, k_cache, v_cache, g1, b1, wq, bq, wk, bk, wv, bv, wo, bo, g2, b2, wf1, bf1, wf2, bf2):
    any_spec = pl.BlockSpec(memory_space=pl.ANY)
    args = (x, lens.reshape(1, BATCH),
            jnp.swapaxes(k_cache, 3, 4).reshape(LAYERS, BATCH * HEAD, SEQ),
            jnp.swapaxes(v_cache, 3, 4).reshape(LAYERS, BATCH * HEAD, SEQ),
            g1, b1, wq, bq, wk, bk, wv, bv, wo, bo, g2, b2, wf1, bf1, wf2, bf2)
    vm = pltpu.VMEM
    in_scratch = [vm(a.shape, a.dtype) for a in args]
    scratch = in_scratch + [
        vm((BATCH, 128), F32),
        vm((LAYERS, BATCH, 128), F32),
        vm((LAYERS, BATCH, 128), BF16),
        vm((ROWS, SEQ), F32),
        vm((ROWS, SEQ), BF16),
        vm((ROWS, 128), F32),
        vm((2 * N_SLOT, 8, 128), F32),
        vm((2 * N_SLOT, N_ROW, 8, 128), F32),
        vm((2 * LAYERS, N_ROW, 8, WIDTH), F32),
        vm((2 * LAYERS, N_ROW, 8, WIDTH), F32),
        vm((N_SLOT, N_ROW, ROWS + HALF, 128), BF16),
        vm((N_SLOT, N_ROW, ROWS + HALF, 128), BF16),
        vm((N_SLOT, N_ROW, HALF, 128), BF16),
        vm((N_SLOT, N_COL, ROWS, WIDTH), BF16),
        vm((N_SLOT, N_ROW, ROWS, WIDTH), BF16),
        vm((N_SLOT, N_ROW, ROWS, WIDTH), BF16),
        vm((N_SLOT, N_ROW, ROWS, WIDTH), BF16),
        vm((N_SLOT, N_COL, ROWS, WIDTH), BF16),
        pltpu.SemaphoreType.DMA((32,)),
        pltpu.SemaphoreType.DMA((2 * N_SLOT,)),
        pltpu.SemaphoreType.DMA((2 * LAYERS + STREAMS,)),
        pltpu.SemaphoreType.DMA((N_COPY,)),
        pltpu.SemaphoreType.DMA((N_COPY,)),
    ]
    shapes = (jax.ShapeDtypeStruct((BATCH, WIDTH), BF16),
              jax.ShapeDtypeStruct((LAYERS, HEAD, BATCH), BF16),
              jax.ShapeDtypeStruct((LAYERS, HEAD, BATCH), BF16))
    results = pl.pallas_call(
        step_kernel,
        out_shape=shapes,
        in_specs=[pl.BlockSpec(memory_space=pltpu.HBM)] * len(args),
        out_specs=(any_spec,) * 3,
        scratch_shapes=scratch,
        compiler_params=pltpu.CompilerParams(
            collective_id=0, has_side_effects=True, vmem_limit_bytes=60 * 1024 * 1024),
        name="decode_step",
    )(*args)
    h_out, k_new, v_new = pl.pallas_call(
        emit_kernel,
        out_shape=shapes,
        in_specs=[pl.BlockSpec(memory_space=pltpu.VMEM)] * 3,
        out_specs=(pl.BlockSpec(memory_space=pltpu.HBM),) * 3,
        scratch_shapes=[pltpu.SemaphoreType.DMA((3,))],
        compiler_params=pltpu.CompilerParams(vmem_limit_bytes=1024 * 1024),
        name="emit",
    )(*results)

    def fresh(rows):
        return jnp.swapaxes(rows, 1, 2).reshape(LAYERS, BATCH, 1, HEAD)

    return h_out, fresh(k_new), fresh(v_new)


def solution(mesh):
    act_spec = P("dp", "row")
    cache_spec = P(None, "dp", ("col", "row"), None, None)
    fresh_spec = P(None, "dp", ("col", "row"), None)
    in_weight = P(None, "row", "col")
    out_weight = P(None, "col", "row")
    col_vec = P(None, "col")
    row_vec = P(None, "row")
    in_specs = (act_spec, P("dp"), cache_spec, cache_spec, row_vec, row_vec,
                in_weight, col_vec, in_weight, col_vec, in_weight, col_vec,
                out_weight, row_vec, row_vec, row_vec, in_weight, col_vec, out_weight, row_vec)
    return jax.shard_map(run_step, mesh=mesh, in_specs=in_specs,
                         out_specs=(act_spec, fresh_spec, fresh_spec), check_vma=False)
```

```python
import functools

import jax
import jax.numpy as jnp
from jax import lax
from jax.experimental import pallas as pl
from jax.experimental.pallas import tpu as pltpu
from jax.sharding import PartitionSpec as P

EPS_LN = 1e-5
MESH = pl.DeviceIdType.MESH
F32 = jnp.float32
BF16 = jnp.bfloat16

LAYERS = 2
BATCH = 128
STREAMS = 2
ROWS = BATCH // STREAMS
HALF = ROWS // 2
GROUP = 16
N_ROW = 4
N_COL = 4
HEAD = 64
SEQ = 512
WIDTH = 256
D_MODEL = 1024
FF_LOC = 1024
FF_HALF = FF_LOC // 2

VEC_NAMES = ("g1", "b1", "bq", "bk", "bv", "bo", "g2", "b2", "bf2")
MAT_NAMES = ("wq", "wk", "wv", "wo", "wf1", "wf2")


def lane_iota(shape):
    return lax.broadcasted_iota(jnp.int32, shape, len(shape) - 1)


def swap_halves(val):
    return pltpu.roll(val, HEAD, 1)


def low_half(shape):
    return lane_iota(shape) < HEAD


def step_kernel(*refs):
    (x_in, len_in, k_in, v_in, g1_in, b1_in, wq_in, bq_in, wk_in, bk_in, wv_in, bv_in,
     wo_in, bo_in, g2_in, b2_in, wf1_in, bf1_in, wf2_in, bf2_in,
     h_out, k_out, v_out,
     x_buf, len_buf, k_buf, v_buf, g1, b1, wq, bq, wk, bk, wv, bv, wo, bo, g2, b2, wf1, bf1, wf2, bf2,
     len_mat, kv_mix, kv_turn, s_buf, p_buf, o_mix,
     st_send, st_recv, gq_send, gq_recv, gf_send, gf_recv, qkv_send, qkv_recv, o_recv, o_all, wo_all,
     proj_recv, f1_mine, f1_send, f1_recv, pair_recv, u_recv, out_recv,
     load_sem, big_sem, store_sem, send_sem, recv_sem) = refs

    row = lax.axis_index("row")
    col = lax.axis_index("col")
    side = lax.rem(row, 2)
    chip = row // 2
    partner = chip * 2 + (1 - side)
    across = lax.rem(row + 2, N_ROW)

    loads = {}

    def load(name, src, dst, sem):
        copy = pltpu.make_async_copy(src, dst, sem)
        copy.start()
        loads[name] = copy

    n_load = [0]

    def small(name, src, dst):
        load(name, src, dst, load_sem.at[n_load[0]])
        n_load[0] += 1

    small("x", x_in, x_buf)
    small("g1", g1_in, g1)
    for layer in range(LAYERS):
        for name, src, dst in (("wq", wq_in, wq), ("wk", wk_in, wk), ("wv", wv_in, wv)):
            if layer == 0:
                small((name, layer), src.at[layer], dst.at[layer])
    small(("wo", 1), wo_in.at[1], wo_all.at[col])
    for name, src, dst in (("b1", b1_in, b1), ("bq", bq_in, bq), ("bk", bk_in, bk), ("bv", bv_in, bv),
                           ("len", len_in, len_buf), ("bo", bo_in, bo), ("g2", g2_in, g2), ("b2", b2_in, b2),
                           ("bf1", bf1_in, bf1), ("bf2", bf2_in, bf2)):
        small(name, src, dst)

    barrier = pltpu.get_barrier_semaphore()
    others = [{"col": lax.rem(col + a, N_COL), "row": lax.rem(row + b, N_ROW)}
              for a in (2, 3, 1, 0) for b in (2, 3, 1, 0) if a or b]
    for device in others:
        pl.semaphore_signal(barrier, inc=1, device_id=device, device_id_type=MESH)

    def big(layer, stream, which):
        src, dst = (k_in, k_buf) if which == 0 else (v_in, v_buf)
        span = pl.ds(stream * ROWS * HEAD, ROWS * HEAD)
        load(("kv", layer, stream, which), src.at[layer, span], dst.at[layer, span],
             big_sem.at[(layer * STREAMS + stream) * 2 + which])

    for stream in range(STREAMS):
        for which in range(2):
            big(0, stream, which)
    for name, src, dst in (("wo", wo_in, wo), ("wf1", wf1_in, wf1), ("wf2", wf2_in, wf2)):
        small((name, 0), src.at[0], dst.at[0])
    for name, src, dst in (("wq", wq_in, wq), ("wk", wk_in, wk), ("wv", wv_in, wv),
                           ("wf1", wf1_in, wf1), ("wf2", wf2_in, wf2)):
        small((name, 1), src.at[1], dst.at[1])
    for stream in range(STREAMS):
        for which in range(2):
            big(1, stream, which)

    waited = set()

    def need(name):
        if name not in waited:
            waited.add(name)
            loads[name].wait()

    drains = []
    recvs = {}
    n_sem = [0]

    def exchange(tag, copies, span):
        index = n_sem[0]
        n_sem[0] += 1
        for src, dst, device in copies:
            pltpu.make_async_remote_copy(
                src_ref=src, dst_ref=dst, send_sem=send_sem.at[index],
                recv_sem=recv_sem.at[index], device_id=device, device_id_type=MESH).start()
        drains.append(pltpu.make_async_copy(span, span, send_sem.at[index]))
        recvs[tag] = pltpu.make_async_copy(span, span, recv_sem.at[index])

    def to_axis(tag, axis, src_of, buf):
        me = row if axis == "row" else col
        dests = [lax.rem(me + off, 4) for off in (2, 3, 1)]
        exchange(tag, [(src_of(d), buf.at[me], {axis: d}) for d in dests], buf.at[0:3])

    def arrived(tag):
        recvs[tag].wait()

    def local_norm(state, gain):
        mean = jnp.sum(state, axis=-1, keepdims=True) * (1.0 / WIDTH)
        delta = state - mean
        var = jnp.sum(delta * delta, axis=-1, keepdims=True) * (1.0 / WIDTH)
        normed = (delta * lax.rsqrt(var + EPS_LN) * gain).astype(BF16)
        lanes = lane_iota((ROWS, 128))
        tile = jnp.where(lanes == 0, mean, jnp.where(lanes == 1, var, 0.0))
        if ROWS < 128:
            tile = jnp.concatenate([tile] * (128 // ROWS), axis=0)
        return normed, jnp.transpose(tile)[0:8]

    def merge_stats(blocks):
        share = 1.0 / len(blocks)
        mean = sum(m for m, _ in blocks) * share
        var = sum(v + (m - mean) * (m - mean) for m, v in blocks) * share
        return mean, var

    def stat_columns(blocks):
        mean, var = merge_stats(blocks)
        inv = lax.rsqrt(var + EPS_LN)
        lines = [jnp.sqrt(v + EPS_LN) * inv for _, v in blocks] + [(m - mean) * inv for m, _ in blocks]
        sub = lax.broadcasted_iota(jnp.int32, (8, 128), 0)
        tile = jnp.zeros((8, 128), F32)
        for i, line in enumerate(lines):
            tile = jnp.where(sub == i, line, tile)
        turned = jnp.transpose(jnp.concatenate([tile] * 16, axis=0))[0:ROWS]
        return [turned[:, i:i + 1] for i in range(len(lines))]

    def block_stats(index, r):
        tile = st_recv[index, r]
        return tile[0:1], tile[1:2]

    def pack_heads(q, k, v, j, rows):
        half = rows // 2
        lo = (j // 2) * 128
        q, k, v = q[:, lo:lo + 128], k[:, lo:lo + 128], v[:, lo:lo + 128]
        if j % 2 == 0:
            first = jnp.where(low_half((rows, 128)), q, swap_halves(k))
            second = jnp.where(low_half((half, 128)), v[:half], swap_halves(v[half:]))
        else:
            first = jnp.where(low_half((rows, 128)), swap_halves(q), k)
            second = jnp.where(low_half((half, 128)), swap_halves(v[:half]), v[half:])
        return first, second

    def dot(a, b):
        return jnp.dot(a, b, preferred_element_type=F32)

    def send_qkv(layer, stream):
        slot = layer * STREAMS + stream
        need("x")
        need("g1")
        state = x_buf[stream * ROWS:(stream + 1) * ROWS, :].astype(F32)
        normed, tile = local_norm(state, g1[layer:layer + 1, :].astype(F32))
        st_send[2 * slot] = tile
        st_recv[2 * slot, row] = tile
        for name in ("wq", "wk", "wv"):
            need((name, layer))
        q, k, v = dot(normed, wq[layer]), dot(normed, wk[layer]), dot(normed, wv[layer])
        for j in range(N_ROW):
            first, second = pack_heads(q, k, v, j, ROWS)
            qkv_send[slot, j, 0:ROWS] = first.astype(BF16)
            qkv_send[slot, j, ROWS:ROWS + HALF] = second.astype(BF16)
        qkv_recv[slot, row] = qkv_send[slot, row]
        if layer == 0 and stream == 0:
            pl.semaphore_wait(barrier, N_PEER)
        to_axis(("st1", slot), "row", lambda d: st_send.at[2 * slot], st_recv.at[2 * slot])
        to_axis(("qkv", slot), "row", lambda d: qkv_send.at[slot, d], qkv_recv.at[slot])
        if layer == 0 and stream == 0:
            need(("wo", 1))
            to_axis("wo", "col", lambda d: wo_all.at[col], wo_all)

    def affine_rows(gain, shift):
        sub = lax.broadcasted_iota(jnp.int32, (16, WIDTH), 0)
        return jnp.where(sub == 0, gain.astype(F32), jnp.where(sub == 1, shift.astype(F32), 0.0)).astype(BF16)

    def send_affine(layer, kind):
        bias_on = jnp.where(row == 0, 1.0, 0.0)
        if kind == 0:
            for name in ("b1", "bq", "bk", "bv"):
                need(name)
            rows = affine_rows(g1[layer:layer + 1, :], b1[layer:layer + 1, :])
            parts = []
            for w, b in ((wq, bq), (wk, bk), (wv, bv)):
                bias = b[layer:layer + 1, :].astype(F32) * bias_on
                part = dot(rows, w[layer])[0:8]
                sub_w = lax.broadcasted_iota(jnp.int32, (8, WIDTH), 0)
                parts.append(part + jnp.where(sub_w == 1, bias, 0.0))
            q, k, v = parts
            for j in range(N_ROW):
                lo = (j // 2) * 128
                qj, kj, vj = q[:, lo:lo + 128], k[:, lo:lo + 128], v[:, lo:lo + 128]
                if j % 2 == 0:
                    first = jnp.where(low_half((8, 128)), qj, swap_halves(kj))
                    second = jnp.where(low_half((8, 128)), vj, swap_halves(vj))
                else:
                    first = jnp.where(low_half((8, 128)), swap_halves(qj), kj)
                    second = jnp.where(low_half((8, 128)), swap_halves(vj), vj)
                gq_send[layer, j] = jnp.concatenate([first, second], axis=1)
            gq_recv[layer, row] = gq_send[layer, row]
            to_axis(("gb", layer, kind), "row", lambda d: gq_send.at[layer, d], gq_recv.at[layer])
        else:
            for name in ("g2", "b2", "bf1", ("wf1", layer)):
                need(name)
            rows = affine_rows(g2[layer:layer + 1, :], b2[layer:layer + 1, :])
            part = dot(rows, wf1[layer])[0:8]
            sub_w = lax.broadcasted_iota(jnp.int32, (8, FF_LOC), 0)
            part = part + jnp.where(sub_w == 1, bf1[layer:layer + 1, :].astype(F32) * bias_on, 0.0)
            for j in range(2):
                gf_send[layer, j] = part[:, j * FF_HALF:(j + 1) * FF_HALF]
            gf_recv[layer, row] = gf_send[layer, side]
            to_axis(("gb", layer, kind), "row", lambda d: gf_send.at[layer, lax.rem(d, 2)], gf_recv.at[layer])

    gb_done = set()

    def affine_lines(layer, kind):
        if (layer, kind) not in gb_done:
            gb_done.add((layer, kind))
            arrived(("gb", layer, kind))

    def gain_line(buf, layer, r):
        return buf[layer, r, 0:1]

    def const_line(buf, layer):
        return buf[layer, 0, 1:2] + buf[layer, 1, 1:2] + buf[layer, 2, 1:2] + buf[layer, 3, 1:2]

    def attend(layer, stream):
        slot = layer * STREAMS + stream
        span = slice(stream * ROWS, (stream + 1) * ROWS)
        arrived(("st1", slot))
        cols = stat_columns([block_stats(2 * slot, r) for r in range(N_ROW)])
        affine_lines(layer, 0)
        gains = [gain_line(gq_recv, layer, r) for r in range(N_ROW)]
        const = const_line(gq_recv, layer)
        arrived(("qkv", slot))
        low = low_half((HALF, 128))
        qk = const[:, 0:128]
        vv = const[:, 128:256]
        for r in range(N_ROW):
            part = qkv_recv[slot, r].astype(F32)
            scale, shift = cols[r], cols[4 + r]
            qk = qk + part[0:ROWS] * scale + shift * gains[r][:, 0:128]
            scale_v = jnp.where(low, scale[0:HALF], scale[HALF:ROWS])
            shift_v = jnp.where(low, shift[0:HALF], shift[HALF:ROWS])
            vv = vv + part[ROWS:ROWS + HALF] * scale_v + shift_v * gains[r][:, 128:256]
        full_low = low_half((ROWS, 128))
        qk_turn = swap_halves(qk)
        q2 = (jnp.where(full_low, qk, qk_turn) * (HEAD ** -0.5)).astype(BF16)
        k2 = jnp.where(full_low, qk_turn, qk).astype(BF16)
        vv_turn = swap_halves(vv)
        v2 = jnp.concatenate([jnp.where(low, vv, vv_turn), jnp.where(low, vv_turn, vv)], axis=0).astype(BF16)
        kv_mix[layer, span, :] = jnp.where(full_low, k2.astype(F32), v2.astype(F32))
        score_new = jnp.sum(jnp.where(full_low, q2.astype(F32) * k2.astype(F32), 0.0), axis=-1, keepdims=True)

        need(("kv", layer, stream, 0))
        q_row = lax.broadcasted_iota(jnp.int32, (GROUP, 128), 0)
        q_half = lane_iota((GROUP, 128)) // HEAD
        for g in range(ROWS // GROUP):
            base = (stream * ROWS + g * GROUP) * HEAD
            qg = q2[g * GROUP:(g + 1) * GROUP].astype(F32)
            spread = [jnp.where(q_row == 2 * j + q_half, qg, 0.0).astype(BF16) for j in range(GROUP // 2)]
            s_buf[g * GROUP:(g + 1) * GROUP, :] = dot(jnp.concatenate(spread, axis=1),
                                                      k_buf[layer, base:base + GROUP * HEAD, :])
        positions = lane_iota((ROWS, SEQ)).astype(F32)
        limit = len_mat[span, 0:1]
        scores = jnp.where(positions < limit, s_buf[...], -jnp.inf)
        peak = jnp.maximum(jnp.max(scores, axis=-1, keepdims=True), score_new)
        exp_cache = jnp.exp(scores - peak)
        exp_new = jnp.exp(score_new - peak)
        inv = 1.0 / (jnp.sum(exp_cache, axis=-1, keepdims=True) + exp_new)
        p_buf[...] = (exp_cache * inv).astype(BF16)
        prob_new = (exp_new * inv).astype(BF16).astype(F32)

        need(("kv", layer, stream, 1))
        for g in range(ROWS // GROUP):
            base = (stream * ROWS + g * GROUP) * HEAD
            wide = lax.dot_general(p_buf[g * GROUP:(g + 1) * GROUP, :], v_buf[layer, base:base + GROUP * HEAD, :],
                                   (((1,), (1,)), ((), ())), preferred_element_type=F32)
            acc = jnp.zeros((GROUP, 128), F32)
            for j in range(GROUP // 2):
                acc = acc + jnp.where(q_row == 2 * j + q_half, wide[:, j * 128:(j + 1) * 128], 0.0)
            o_mix[g * GROUP:(g + 1) * GROUP, :] = acc + swap_halves(acc)
        o2 = o_mix[...] + prob_new * v2.astype(F32)
        packed = jnp.where(low, o2[0:HALF], o2[HALF:ROWS]).astype(BF16)
        if layer == 0:
            o_recv[stream, row] = packed
            to_axis(("o", slot), "row", lambda d: o_recv.at[stream, row], o_recv.at[stream])
        else:
            head = col * N_ROW + row
            o_all[stream, head] = packed
            mine = o_all.at[stream, head]
            exchange(("o", slot), [(mine, mine, d) for d in others], o_all.at[stream, 0:N_PEER])

    def unpack_heads(buf, first):
        low = low_half((HALF, 128))
        parts = [buf[first + r].astype(F32) for r in range(N_ROW)]
        turns = [swap_halves(p) for p in parts]
        pairs = []
        for a, b in ((0, 1), (2, 3)):
            top = jnp.where(low, parts[a], turns[b])
            bottom = jnp.where(low, turns[a], parts[b])
            pairs.append(jnp.concatenate([top, bottom], axis=0).astype(BF16))
        return jnp.concatenate(pairs, axis=1)

    def project(stream):
        need(("wo", 0))
        arrived(("o", stream))
        proj_recv[stream, col] = dot(unpack_heads(o_recv.at[stream], 0), wo[0]).astype(BF16)
        to_axis(("proj", stream), "col", lambda d: proj_recv.at[stream, col], proj_recv.at[stream])

    def col_sum(buf):
        total = buf[0].astype(F32)
        for c in range(1, N_COL):
            total = total + buf[c].astype(F32)
        return total

    def residual(total, bias, stream):
        span = slice(stream * ROWS, (stream + 1) * ROWS)
        new = (x_buf[span, :].astype(F32) + (total + bias)).astype(BF16)
        x_buf[span, :] = new
        return new.astype(F32)

    def send_inner(layer, stream):
        slot = layer * STREAMS + stream
        need("bo")
        need("g2")
        need(("wf1", layer))
        if layer == 0:
            arrived(("proj", stream))
            total = col_sum(proj_recv.at[stream])
        else:
            if "wo" in recvs:
                recvs.pop("wo").wait()
            arrived(("o", slot))
            total = dot(unpack_heads(o_all.at[stream], 0), wo_all[0])
            for c in range(1, N_COL):
                total = total + dot(unpack_heads(o_all.at[stream], c * N_ROW), wo_all[c])
        state = residual(total, bo[layer:layer + 1, :].astype(F32), stream)
        normed, tile = local_norm(state, g2[layer:layer + 1, :].astype(F32))
        index = 2 * slot + 1
        st_send[index] = tile
        st_recv[index, row] = tile
        mine = st_send.at[index]
        spot = st_recv.at[index, row]
        exchange(("st2", slot), [(mine, spot, {"row": partner})], mine)
        far = lax.rem(partner + 2, N_ROW)
        exchange(("st3", slot), [(mine, spot, {"row": across}), (mine, spot, {"row": far})], st_recv.at[index, 0:2])
        theirs = pl.ds(pl.multiple_of((1 - side) * FF_HALF, FF_HALF), FF_HALF)
        f1_send[slot] = dot(normed, wf1[layer, :, theirs]).astype(BF16)
        exchange(("f1", slot), [(f1_send.at[slot], f1_recv.at[slot], {"row": partner})], f1_recv.at[slot])
        ours = pl.ds(pl.multiple_of(side * FF_HALF, FF_HALF), FF_HALF)
        f1_mine[stream] = dot(normed, wf1[layer, :, ours])

    def send_pair(layer, stream):
        slot = layer * STREAMS + stream
        arrived(("st2", slot))
        cols = stat_columns([block_stats(2 * slot + 1, r) for r in (row, partner)])
        affine_lines(layer, 1)
        arrived(("f1", slot))
        total = f1_mine[stream] * cols[0] + cols[2] * gain_line(gf_recv, layer, row)
        total = total + f1_recv[slot].astype(F32) * cols[1] + cols[3] * gain_line(gf_recv, layer, partner)
        pair_recv[slot, chip] = total.astype(BF16)
        mine = pair_recv.at[slot, chip]
        exchange(("pair", slot), [(mine, mine, {"row": across})], mine)

    def send_act(layer, stream):
        slot = layer * STREAMS + stream
        arrived(("st3", slot))
        pairs = [merge_stats([block_stats(2 * slot + 1, 2 * k + r) for r in range(2)]) for k in range(2)]
        cols = stat_columns(pairs)
        total = const_line(gf_recv, layer)
        arrived(("pair", slot))
        for k in range(2):
            gain = gain_line(gf_recv, layer, 2 * k) + gain_line(gf_recv, layer, 2 * k + 1)
            total = total + pair_recv[slot, k].astype(F32) * cols[k] + cols[2 + k] * gain
        u_recv[slot, side] = jnp.maximum(total, 0.0).astype(BF16)
        mine = u_recv.at[slot, side]
        exchange(("u", slot), [(mine, mine, {"row": partner})], mine)

    def send_out(layer, stream):
        slot = layer * STREAMS + stream
        need(("wf2", layer))
        arrived(("u", slot))
        acc = dot(u_recv[slot, 0], wf2[layer, 0:FF_HALF, :]) + dot(u_recv[slot, 1], wf2[layer, FF_HALF:, :])
        out_recv[slot, col] = acc.astype(BF16)
        to_axis(("out", slot), "col", lambda d: out_recv.at[slot, col], out_recv.at[slot])

    def finish(layer, stream):
        slot = layer * STREAMS + stream
        need("bf2")
        arrived(("out", slot))
        residual(col_sum(out_recv.at[slot]), bf2[layer:layer + 1, :].astype(F32), stream)

    stores = []

    def store(src, dst, index):
        copy = pltpu.make_async_copy(src, dst, store_sem.at[index])
        copy.start()
        stores.append(copy)

    for stream in range(STREAMS):
        send_qkv(0, stream)
    send_affine(0, 0)
    need("len")
    len_mat[...] = jnp.transpose(jnp.broadcast_to(len_buf[...].astype(F32), (128, 128)))
    for layer in range(LAYERS):
        for stream in range(STREAMS):
            attend(layer, stream)
        kv_turn[layer] = jnp.transpose(kv_mix[layer]).astype(BF16)
        store(kv_turn.at[layer, 0:HEAD], k_out.at[layer], 2 * layer)
        store(kv_turn.at[layer, HEAD:2 * HEAD], v_out.at[layer], 2 * layer + 1)
        if layer == 0:
            send_affine(0, 1)
        if layer == 0:
            for stream in range(STREAMS):
                project(stream)
            for name in MAT_NAMES[:3]:
                need((name, 1))
            send_affine(1, 0)
            send_affine(1, 1)
        for stream in range(STREAMS):
            send_inner(layer, stream)
        for stream in range(STREAMS):
            send_pair(layer, stream)
        for stream in range(STREAMS):
            send_act(layer, stream)
        for stream in range(STREAMS):
            send_out(layer, stream)
        for stream in range(STREAMS):
            finish(layer, stream)
            if layer + 1 < LAYERS:
                send_qkv(layer + 1, stream)
            else:
                span = pl.ds(stream * ROWS, ROWS)
                store(x_buf.at[span], h_out.at[span], 2 * LAYERS + stream)
    for copy in stores:
        copy.wait()
    for copy in drains:
        copy.wait()


N_SLOT = LAYERS * STREAMS
N_COPY = 9 * N_SLOT + STREAMS + 2 * LAYERS + 1
N_PEER = N_ROW * N_COL - 1


def emit_kernel(h_in, k_in, v_in, h_out, k_out, v_out, h_buf, k_buf, v_buf, sem):
    moves = ((h_in, h_buf, h_out), (k_in, k_buf, k_out), (v_in, v_buf, v_out))
    loads = [pltpu.make_async_copy(src, buf, sem.at[i]) for i, (src, buf, _) in enumerate(moves)]
    for copy in loads:
        copy.start()
    stores = []
    for i, (_, buf, dst) in enumerate(moves):
        loads[i].wait()
        copy = pltpu.make_async_copy(buf, dst, sem.at[i])
        copy.start()
        stores.append(copy)
    for copy in stores:
        copy.wait()


def run_step(x, lens, k_cache, v_cache, g1, b1, wq, bq, wk, bk, wv, bv, wo, bo, g2, b2, wf1, bf1, wf2, bf2):
    any_spec = pl.BlockSpec(memory_space=pl.ANY)
    args = (x, lens.reshape(1, BATCH),
            jnp.swapaxes(k_cache, 3, 4).reshape(LAYERS, BATCH * HEAD, SEQ),
            jnp.swapaxes(v_cache, 3, 4).reshape(LAYERS, BATCH * HEAD, SEQ),
            g1, b1, wq, bq, wk, bk, wv, bv, wo, bo, g2, b2, wf1, bf1, wf2, bf2)
    vm = pltpu.VMEM
    in_scratch = [vm(a.shape, a.dtype) for a in args]
    scratch = in_scratch + [
        vm((BATCH, 128), F32),
        vm((LAYERS, BATCH, 128), F32),
        vm((LAYERS, BATCH, 128), BF16),
        vm((ROWS, SEQ), F32),
        vm((ROWS, SEQ), BF16),
        vm((ROWS, 128), F32),
        vm((2 * N_SLOT, 8, 128), F32),
        vm((2 * N_SLOT, N_ROW, 8, 128), F32),
        vm((LAYERS, N_ROW, 8, WIDTH), F32),
        vm((LAYERS, N_ROW, 8, WIDTH), F32),
        vm((LAYERS, 2, 8, FF_HALF), F32),
        vm((LAYERS, N_ROW, 8, FF_HALF), F32),
        vm((N_SLOT, N_ROW, ROWS + HALF, 128), BF16),
        vm((N_SLOT, N_ROW, ROWS + HALF, 128), BF16),
        vm((STREAMS, N_ROW, HALF, 128), BF16),
        vm((STREAMS, N_ROW * N_COL, HALF, 128), BF16),
        vm((N_COL, WIDTH, WIDTH), BF16),
        vm((STREAMS, N_COL, ROWS, WIDTH), BF16),
        vm((STREAMS, ROWS, FF_HALF), F32),
        vm((N_SLOT, ROWS, FF_HALF), BF16),
        vm((N_SLOT, ROWS, FF_HALF), BF16),
        vm((N_SLOT, 2, ROWS, FF_HALF), BF16),
        vm((N_SLOT, 2, ROWS, FF_HALF), BF16),
        vm((N_SLOT, N_COL, ROWS, WIDTH), BF16),
        pltpu.SemaphoreType.DMA((32,)),
        pltpu.SemaphoreType.DMA((2 * N_SLOT,)),
        pltpu.SemaphoreType.DMA((2 * LAYERS + STREAMS,)),
        pltpu.SemaphoreType.DMA((N_COPY,)),
        pltpu.SemaphoreType.DMA((N_COPY,)),
    ]
    shapes = (jax.ShapeDtypeStruct((BATCH, WIDTH), BF16),
              jax.ShapeDtypeStruct((LAYERS, HEAD, BATCH), BF16),
              jax.ShapeDtypeStruct((LAYERS, HEAD, BATCH), BF16))
    results = pl.pallas_call(
        step_kernel,
        out_shape=shapes,
        in_specs=[pl.BlockSpec(memory_space=pltpu.HBM)] * len(args),
        out_specs=(any_spec,) * 3,
        scratch_shapes=scratch,
        compiler_params=pltpu.CompilerParams(
            collective_id=0, has_side_effects=True, vmem_limit_bytes=60 * 1024 * 1024),
        name="decode_step",
    )(*args)
    h_out, k_new, v_new = pl.pallas_call(
        emit_kernel,
        out_shape=shapes,
        in_specs=[any_spec] * 3,
        out_specs=(pl.BlockSpec(memory_space=pltpu.HBM),) * 3,
        scratch_shapes=[vm(a.shape, a.dtype) for a in shapes] + [pltpu.SemaphoreType.DMA((3,))],
        compiler_params=pltpu.CompilerParams(vmem_limit_bytes=60 * 1024 * 1024),
        name="emit",
    )(*results)

    def fresh(rows):
        return jnp.swapaxes(rows, 1, 2).reshape(LAYERS, BATCH, 1, HEAD)

    return h_out, fresh(k_new), fresh(v_new)


def solution(mesh):
    act_spec = P("dp", "row")
    cache_spec = P(None, "dp", ("col", "row"), None, None)
    fresh_spec = P(None, "dp", ("col", "row"), None)
    in_weight = P(None, "row", "col")
    out_weight = P(None, "col", "row")
    col_vec = P(None, "col")
    row_vec = P(None, "row")
    in_specs = (act_spec, P("dp"), cache_spec, cache_spec, row_vec, row_vec,
                in_weight, col_vec, in_weight, col_vec, in_weight, col_vec,
                out_weight, row_vec, row_vec, row_vec, in_weight, col_vec, out_weight, row_vec)
    return jax.shard_map(run_step, mesh=mesh, in_specs=in_specs,
                         out_specs=(act_spec, fresh_spec, fresh_spec), check_vma=False)
```

```python
import functools

import jax
import jax.numpy as jnp
from jax import lax
from jax.experimental import pallas as pl
from jax.experimental.pallas import tpu as pltpu
from jax.sharding import PartitionSpec as P

EPS_LN = 1e-5
MESH = pl.DeviceIdType.MESH
F32 = jnp.float32
BF16 = jnp.bfloat16

LAYERS = 2
BATCH = 128
STREAMS = 2
ROWS = BATCH // STREAMS
HALF = ROWS // 2
GROUP = 16
N_ROW = 4
N_COL = 4
HEAD = 64
SEQ = 512
WIDTH = 256
D_MODEL = 1024
FF_LOC = 1024
FF_HALF = FF_LOC // 2

VEC_NAMES = ("g1", "b1", "bq", "bk", "bv", "bo", "g2", "b2", "bf2")
MAT_NAMES = ("wq", "wk", "wv", "wo", "wf1", "wf2")


def lane_iota(shape):
    return lax.broadcasted_iota(jnp.int32, shape, len(shape) - 1)


def swap_halves(val):
    return pltpu.roll(val, HEAD, 1)


def low_half(shape):
    return lane_iota(shape) < HEAD


def step_kernel(*refs):
    (x_in, len_in, k_in, v_in, g1_in, b1_in, wq_in, bq_in, wk_in, bk_in, wv_in, bv_in,
     wo_in, bo_in, g2_in, b2_in, wf1_in, bf1_in, wf2_in, bf2_in,
     h_out, k_out, v_out,
     x_buf, len_buf, k_buf, v_buf, g1, b1, wq, bq, wk, bk, wv, bv, wo, bo, g2, b2, wf1, bf1, wf2, bf2,
     len_mat, kv_mix, kv_turn, s_buf, p_buf, o_mix,
     st_send, st_recv, gq_send, gq_recv, gf_send, gf_recv, qkv_send, qkv_recv, o_recv, o_all, wo_all,
     proj_recv, f1_mine, f1_send, f1_recv, pair_recv, u_recv, out_recv,
     load_sem, big_sem, store_sem, send_sem, recv_sem) = refs

    row = lax.axis_index("row")
    col = lax.axis_index("col")
    side = lax.rem(row, 2)
    chip = row // 2
    partner = chip * 2 + (1 - side)
    across = lax.rem(row + 2, N_ROW)

    loads = {}

    def load(name, src, dst, sem):
        copy = pltpu.make_async_copy(src, dst, sem)
        copy.start()
        loads[name] = copy

    n_load = [0]

    def small(name, src, dst):
        load(name, src, dst, load_sem.at[n_load[0]])
        n_load[0] += 1

    small("x", x_in, x_buf)
    small("g1", g1_in, g1)
    for layer in range(LAYERS):
        for name, src, dst in (("wq", wq_in, wq), ("wk", wk_in, wk), ("wv", wv_in, wv)):
            if layer == 0:
                small((name, layer), src.at[layer], dst.at[layer])
    small(("wo", 1), wo_in.at[1], wo_all.at[col])
    for name, src, dst in (("b1", b1_in, b1), ("bq", bq_in, bq), ("bk", bk_in, bk), ("bv", bv_in, bv),
                           ("len", len_in, len_buf), ("bo", bo_in, bo), ("g2", g2_in, g2), ("b2", b2_in, b2),
                           ("bf1", bf1_in, bf1), ("bf2", bf2_in, bf2)):
        small(name, src, dst)

    barrier = pltpu.get_barrier_semaphore()
    others = [{"col": lax.rem(col + a, N_COL), "row": lax.rem(row + b, N_ROW)}
              for a in (2, 3, 1, 0) for b in (2, 3, 1, 0) if a or b]
    for device in others:
        pl.semaphore_signal(barrier, inc=1, device_id=device, device_id_type=MESH)

    def big(layer, stream, which):
        src, dst = (k_in, k_buf) if which == 0 else (v_in, v_buf)
        span = pl.ds(stream * ROWS * HEAD, ROWS * HEAD)
        load(("kv", layer, stream, which), src.at[layer, span], dst.at[layer, span],
             big_sem.at[(layer * STREAMS + stream) * 2 + which])

    for stream in range(STREAMS):
        for which in range(2):
            big(0, stream, which)
    for name, src, dst in (("wo", wo_in, wo), ("wf1", wf1_in, wf1), ("wf2", wf2_in, wf2)):
        small((name, 0), src.at[0], dst.at[0])
    for name, src, dst in (("wq", wq_in, wq), ("wk", wk_in, wk), ("wv", wv_in, wv),
                           ("wf1", wf1_in, wf1), ("wf2", wf2_in, wf2)):
        small((name, 1), src.at[1], dst.at[1])
    for stream in range(STREAMS):
        for which in range(2):
            big(1, stream, which)

    waited = set()

    def need(name):
        if name not in waited:
            waited.add(name)
            loads[name].wait()

    drains = []
    recvs = {}
    n_sem = [0]

    def exchange(tag, copies, span):
        index = n_sem[0]
        n_sem[0] += 1
        for src, dst, device in copies:
            pltpu.make_async_remote_copy(
                src_ref=src, dst_ref=dst, send_sem=send_sem.at[index],
                recv_sem=recv_sem.at[index], device_id=device, device_id_type=MESH).start()
        drains.append(pltpu.make_async_copy(span, span, send_sem.at[index]))
        recvs[tag] = pltpu.make_async_copy(span, span, recv_sem.at[index])

    def to_axis(tag, axis, src_of, buf):
        me = row if axis == "row" else col
        dests = [lax.rem(me + off, 4) for off in (2, 3, 1)]
        exchange(tag, [(src_of(d), buf.at[me], {axis: d}) for d in dests], buf.at[0:3])

    def arrived(tag):
        recvs[tag].wait()

    def local_norm(state, gain):
        mean = jnp.sum(state, axis=-1, keepdims=True) * (1.0 / WIDTH)
        delta = state - mean
        var = jnp.sum(delta * delta, axis=-1, keepdims=True) * (1.0 / WIDTH)
        normed = (delta * lax.rsqrt(var + EPS_LN) * gain).astype(BF16)
        lanes = lane_iota((ROWS, 128))
        tile = jnp.where(lanes == 0, mean, jnp.where(lanes == 1, var, 0.0))
        if ROWS < 128:
            tile = jnp.concatenate([tile] * (128 // ROWS), axis=0)
        return normed, jnp.transpose(tile)[0:8]

    def merge_stats(blocks):
        share = 1.0 / len(blocks)
        mean = sum(m for m, _ in blocks) * share
        var = sum(v + (m - mean) * (m - mean) for m, v in blocks) * share
        return mean, var

    def stat_columns(blocks):
        mean, var = merge_stats(blocks)
        inv = lax.rsqrt(var + EPS_LN)
        lines = [jnp.sqrt(v + EPS_LN) * inv for _, v in blocks] + [(m - mean) * inv for m, _ in blocks]
        sub = lax.broadcasted_iota(jnp.int32, (8, 128), 0)
        tile = jnp.zeros((8, 128), F32)
        for i, line in enumerate(lines):
            tile = jnp.where(sub == i, line, tile)
        turned = jnp.transpose(jnp.concatenate([tile] * 16, axis=0))[0:ROWS]
        return [turned[:, i:i + 1] for i in range(len(lines))]

    def block_stats(index, r):
        tile = st_recv[index, r]
        return tile[0:1], tile[1:2]

    def pack_heads(q, k, v, j, rows):
        half = rows // 2
        lo = (j // 2) * 128
        q, k, v = q[:, lo:lo + 128], k[:, lo:lo + 128], v[:, lo:lo + 128]
        if j % 2 == 0:
            first = jnp.where(low_half((rows, 128)), q, swap_halves(k))
            second = jnp.where(low_half((half, 128)), v[:half], swap_halves(v[half:]))
        else:
            first = jnp.where(low_half((rows, 128)), swap_halves(q), k)
            second = jnp.where(low_half((half, 128)), swap_halves(v[:half]), v[half:])
        return first, second

    def dot(a, b):
        return jnp.dot(a, b, preferred_element_type=F32)

    def send_qkv(layer, stream):
        slot = layer * STREAMS + stream
        need("x")
        need("g1")
        state = x_buf[stream * ROWS:(stream + 1) * ROWS, :].astype(F32)
        normed, tile = local_norm(state, g1[layer:layer + 1, :].astype(F32))
        st_send[2 * slot] = tile
        st_recv[2 * slot, row] = tile
        for name in ("wq", "wk", "wv"):
            need((name, layer))
        q, k, v = dot(normed, wq[layer]), dot(normed, wk[layer]), dot(normed, wv[layer])
        for j in range(N_ROW):
            first, second = pack_heads(q, k, v, j, ROWS)
            qkv_send[slot, j, 0:ROWS] = first.astype(BF16)
            qkv_send[slot, j, ROWS:ROWS + HALF] = second.astype(BF16)
        qkv_recv[slot, row] = qkv_send[slot, row]
        if layer == 0 and stream == 0:
            pl.semaphore_wait(barrier, N_PEER)
        to_axis(("st1", slot), "row", lambda d: st_send.at[2 * slot], st_recv.at[2 * slot])
        to_axis(("qkv", slot), "row", lambda d: qkv_send.at[slot, d], qkv_recv.at[slot])

    def affine_rows(gain, shift):
        sub = lax.broadcasted_iota(jnp.int32, (16, WIDTH), 0)
        return jnp.where(sub == 0, gain.astype(F32), jnp.where(sub == 1, shift.astype(F32), 0.0)).astype(BF16)

    def send_affine(layer, kind):
        bias_on = jnp.where(row == 0, 1.0, 0.0)
        if kind == 0:
            for name in ("b1", "bq", "bk", "bv"):
                need(name)
            rows = affine_rows(g1[layer:layer + 1, :], b1[layer:layer + 1, :])
            parts = []
            for w, b in ((wq, bq), (wk, bk), (wv, bv)):
                bias = b[layer:layer + 1, :].astype(F32) * bias_on
                part = dot(rows, w[layer])[0:8]
                sub_w = lax.broadcasted_iota(jnp.int32, (8, WIDTH), 0)
                parts.append(part + jnp.where(sub_w == 1, bias, 0.0))
            q, k, v = parts
            for j in range(N_ROW):
                lo = (j // 2) * 128
                qj, kj, vj = q[:, lo:lo + 128], k[:, lo:lo + 128], v[:, lo:lo + 128]
                if j % 2 == 0:
                    first = jnp.where(low_half((8, 128)), qj, swap_halves(kj))
                    second = jnp.where(low_half((8, 128)), vj, swap_halves(vj))
                else:
                    first = jnp.where(low_half((8, 128)), swap_halves(qj), kj)
                    second = jnp.where(low_half((8, 128)), swap_halves(vj), vj)
                gq_send[layer, j] = jnp.concatenate([first, second], axis=1)
            gq_recv[layer, row] = gq_send[layer, row]
            to_axis(("gb", layer, kind), "row", lambda d: gq_send.at[layer, d], gq_recv.at[layer])
        else:
            for name in ("g2", "b2", "bf1", ("wf1", layer)):
                need(name)
            rows = affine_rows(g2[layer:layer + 1, :], b2[layer:layer + 1, :])
            part = dot(rows, wf1[layer])[0:8]
            sub_w = lax.broadcasted_iota(jnp.int32, (8, FF_LOC), 0)
            part = part + jnp.where(sub_w == 1, bf1[layer:layer + 1, :].astype(F32) * bias_on, 0.0)
            for j in range(2):
                gf_send[layer, j] = part[:, j * FF_HALF:(j + 1) * FF_HALF]
            gf_recv[layer, row] = gf_send[layer, side]
            to_axis(("gb", layer, kind), "row", lambda d: gf_send.at[layer, lax.rem(d, 2)], gf_recv.at[layer])

    gb_done = set()

    def affine_lines(layer, kind):
        if (layer, kind) not in gb_done:
            gb_done.add((layer, kind))
            arrived(("gb", layer, kind))

    def gain_line(buf, layer, r):
        return buf[layer, r, 0:1]

    def const_line(buf, layer):
        return buf[layer, 0, 1:2] + buf[layer, 1, 1:2] + buf[layer, 2, 1:2] + buf[layer, 3, 1:2]

    def attend(layer, stream):
        slot = layer * STREAMS + stream
        span = slice(stream * ROWS, (stream + 1) * ROWS)
        arrived(("st1", slot))
        cols = stat_columns([block_stats(2 * slot, r) for r in range(N_ROW)])
        affine_lines(layer, 0)
        gains = [gain_line(gq_recv, layer, r) for r in range(N_ROW)]
        const = const_line(gq_recv, layer)
        arrived(("qkv", slot))
        low = low_half((HALF, 128))
        qk = const[:, 0:128]
        vv = const[:, 128:256]
        for r in range(N_ROW):
            part = qkv_recv[slot, r].astype(F32)
            scale, shift = cols[r], cols[4 + r]
            qk = qk + part[0:ROWS] * scale + shift * gains[r][:, 0:128]
            scale_v = jnp.where(low, scale[0:HALF], scale[HALF:ROWS])
            shift_v = jnp.where(low, shift[0:HALF], shift[HALF:ROWS])
            vv = vv + part[ROWS:ROWS + HALF] * scale_v + shift_v * gains[r][:, 128:256]
        full_low = low_half((ROWS, 128))
        qk_turn = swap_halves(qk)
        q2 = (jnp.where(full_low, qk, qk_turn) * (HEAD ** -0.5)).astype(BF16)
        k2 = jnp.where(full_low, qk_turn, qk).astype(BF16)
        vv_turn = swap_halves(vv)
        v2 = jnp.concatenate([jnp.where(low, vv, vv_turn), jnp.where(low, vv_turn, vv)], axis=0).astype(BF16)
        kv_mix[layer, span, :] = jnp.where(full_low, k2.astype(F32), v2.astype(F32))
        score_new = jnp.sum(jnp.where(full_low, q2.astype(F32) * k2.astype(F32), 0.0), axis=-1, keepdims=True)

        need(("kv", layer, stream, 0))
        q_row = lax.broadcasted_iota(jnp.int32, (GROUP, 128), 0)
        q_half = lane_iota((GROUP, 128)) // HEAD
        for g in range(ROWS // GROUP):
            base = (stream * ROWS + g * GROUP) * HEAD
            qg = q2[g * GROUP:(g + 1) * GROUP].astype(F32)
            spread = [jnp.where(q_row == 2 * j + q_half, qg, 0.0).astype(BF16) for j in range(GROUP // 2)]
            s_buf[g * GROUP:(g + 1) * GROUP, :] = dot(jnp.concatenate(spread, axis=1),
                                                      k_buf[layer, base:base + GROUP * HEAD, :])
        positions = lane_iota((ROWS, SEQ)).astype(F32)
        limit = len_mat[span, 0:1]
        scores = jnp.where(positions < limit, s_buf[...], -jnp.inf)
        peak = jnp.maximum(jnp.max(scores, axis=-1, keepdims=True), score_new)
        exp_cache = jnp.exp(scores - peak)
        exp_new = jnp.exp(score_new - peak)
        inv = 1.0 / (jnp.sum(exp_cache, axis=-1, keepdims=True) + exp_new)
        p_buf[...] = (exp_cache * inv).astype(BF16)
        prob_new = (exp_new * inv).astype(BF16).astype(F32)

        need(("kv", layer, stream, 1))
        for g in range(ROWS // GROUP):
            base = (stream * ROWS + g * GROUP) * HEAD
            wide = lax.dot_general(p_buf[g * GROUP:(g + 1) * GROUP, :], v_buf[layer, base:base + GROUP * HEAD, :],
                                   (((1,), (1,)), ((), ())), preferred_element_type=F32)
            acc = jnp.zeros((GROUP, 128), F32)
            for j in range(GROUP // 2):
                acc = acc + jnp.where(q_row == 2 * j + q_half, wide[:, j * 128:(j + 1) * 128], 0.0)
            o_mix[g * GROUP:(g + 1) * GROUP, :] = acc + swap_halves(acc)
        o2 = o_mix[...] + prob_new * v2.astype(F32)
        packed = jnp.where(low, o2[0:HALF], o2[HALF:ROWS]).astype(BF16)
        if layer == 0:
            o_recv[stream, row] = packed
            to_axis(("o", slot), "row", lambda d: o_recv.at[stream, row], o_recv.at[stream])
        else:
            head = col * N_ROW + row
            o_all[stream, head] = packed
            mine = o_all.at[stream, head]
            exchange(("o", slot), [(mine, mine, d) for d in others], o_all.at[stream, 0:N_PEER])

    def unpack_heads(buf, first):
        low = low_half((HALF, 128))
        parts = [buf[first + r].astype(F32) for r in range(N_ROW)]
        turns = [swap_halves(p) for p in parts]
        pairs = []
        for a, b in ((0, 1), (2, 3)):
            top = jnp.where(low, parts[a], turns[b])
            bottom = jnp.where(low, turns[a], parts[b])
            pairs.append(jnp.concatenate([top, bottom], axis=0).astype(BF16))
        return jnp.concatenate(pairs, axis=1)

    def project(stream):
        need(("wo", 0))
        arrived(("o", stream))
        proj_recv[stream, col] = dot(unpack_heads(o_recv.at[stream], 0), wo[0]).astype(BF16)
        to_axis(("proj", stream), "col", lambda d: proj_recv.at[stream, col], proj_recv.at[stream])

    def col_sum(buf):
        total = buf[0].astype(F32)
        for c in range(1, N_COL):
            total = total + buf[c].astype(F32)
        return total

    def residual(total, bias, stream):
        span = slice(stream * ROWS, (stream + 1) * ROWS)
        new = (x_buf[span, :].astype(F32) + (total + bias)).astype(BF16)
        x_buf[span, :] = new
        return new.astype(F32)

    def send_inner(layer, stream):
        slot = layer * STREAMS + stream
        need("bo")
        need("g2")
        need(("wf1", layer))
        if layer == 0:
            arrived(("proj", stream))
            total = col_sum(proj_recv.at[stream])
        else:
            if "wo" in recvs:
                recvs.pop("wo").wait()
            arrived(("o", slot))
            total = dot(unpack_heads(o_all.at[stream], 0), wo_all[0])
            for c in range(1, N_COL):
                total = total + dot(unpack_heads(o_all.at[stream], c * N_ROW), wo_all[c])
        state = residual(total, bo[layer:layer + 1, :].astype(F32), stream)
        normed, tile = local_norm(state, g2[layer:layer + 1, :].astype(F32))
        index = 2 * slot + 1
        st_send[index] = tile
        st_recv[index, row] = tile
        mine = st_send.at[index]
        spot = st_recv.at[index, row]
        exchange(("st2", slot), [(mine, spot, {"row": partner})], mine)
        far = lax.rem(partner + 2, N_ROW)
        exchange(("st3", slot), [(mine, spot, {"row": across}), (mine, spot, {"row": far})], st_recv.at[index, 0:2])
        theirs = pl.ds(pl.multiple_of((1 - side) * FF_HALF, FF_HALF), FF_HALF)
        f1_send[slot] = dot(normed, wf1[layer, :, theirs]).astype(BF16)
        exchange(("f1", slot), [(f1_send.at[slot], f1_recv.at[slot], {"row": partner})], f1_recv.at[slot])
        ours = pl.ds(pl.multiple_of(side * FF_HALF, FF_HALF), FF_HALF)
        f1_mine[stream] = dot(normed, wf1[layer, :, ours])

    def send_pair(layer, stream):
        slot = layer * STREAMS + stream
        arrived(("st2", slot))
        cols = stat_columns([block_stats(2 * slot + 1, r) for r in (row, partner)])
        affine_lines(layer, 1)
        arrived(("f1", slot))
        total = f1_mine[stream] * cols[0] + cols[2] * gain_line(gf_recv, layer, row)
        total = total + f1_recv[slot].astype(F32) * cols[1] + cols[3] * gain_line(gf_recv, layer, partner)
        pair_recv[slot, chip] = total.astype(BF16)
        mine = pair_recv.at[slot, chip]
        exchange(("pair", slot), [(mine, mine, {"row": across})], mine)

    def send_act(layer, stream):
        slot = layer * STREAMS + stream
        arrived(("st3", slot))
        pairs = [merge_stats([block_stats(2 * slot + 1, 2 * k + r) for r in range(2)]) for k in range(2)]
        cols = stat_columns(pairs)
        total = const_line(gf_recv, layer)
        arrived(("pair", slot))
        for k in range(2):
            gain = gain_line(gf_recv, layer, 2 * k) + gain_line(gf_recv, layer, 2 * k + 1)
            total = total + pair_recv[slot, k].astype(F32) * cols[k] + cols[2 + k] * gain
        u_recv[slot, side] = jnp.maximum(total, 0.0).astype(BF16)
        mine = u_recv.at[slot, side]
        exchange(("u", slot), [(mine, mine, {"row": partner})], mine)

    def send_out(layer, stream):
        slot = layer * STREAMS + stream
        need(("wf2", layer))
        arrived(("u", slot))
        acc = dot(u_recv[slot, 0], wf2[layer, 0:FF_HALF, :]) + dot(u_recv[slot, 1], wf2[layer, FF_HALF:, :])
        out_recv[slot, col] = acc.astype(BF16)
        to_axis(("out", slot), "col", lambda d: out_recv.at[slot, col], out_recv.at[slot])

    def finish(layer, stream):
        slot = layer * STREAMS + stream
        need("bf2")
        arrived(("out", slot))
        residual(col_sum(out_recv.at[slot]), bf2[layer:layer + 1, :].astype(F32), stream)

    stores = []

    def store(src, dst, index):
        copy = pltpu.make_async_copy(src, dst, store_sem.at[index])
        copy.start()
        stores.append(copy)

    for stream in range(STREAMS):
        send_qkv(0, stream)
    send_affine(0, 0)
    need("len")
    len_mat[...] = jnp.transpose(jnp.broadcast_to(len_buf[...].astype(F32), (128, 128)))
    for layer in range(LAYERS):
        for stream in range(STREAMS):
            attend(layer, stream)
        kv_turn[layer] = jnp.transpose(kv_mix[layer]).astype(BF16)
        store(kv_turn.at[layer, 0:HEAD], k_out.at[layer], 2 * layer)
        store(kv_turn.at[layer, HEAD:2 * HEAD], v_out.at[layer], 2 * layer + 1)
        if layer == 0:
            send_affine(0, 1)
        if layer == 0:
            for stream in range(STREAMS):
                project(stream)
            for name in MAT_NAMES[:3]:
                need((name, 1))
            send_affine(1, 0)
            send_affine(1, 1)
        for stream in range(STREAMS):
            send_inner(layer, stream)
        if layer == 0:
            need(("wo", 1))
            to_axis("wo", "col", lambda d: wo_all.at[col], wo_all)
        for stream in range(STREAMS):
            send_pair(layer, stream)
        for stream in range(STREAMS):
            send_act(layer, stream)
        for stream in range(STREAMS):
            send_out(layer, stream)
        for stream in range(STREAMS):
            finish(layer, stream)
            if layer + 1 < LAYERS:
                send_qkv(layer + 1, stream)
            else:
                span = pl.ds(stream * ROWS, ROWS)
                store(x_buf.at[span], h_out.at[span], 2 * LAYERS + stream)
    for copy in stores:
        copy.wait()
    for copy in drains:
        copy.wait()


N_SLOT = LAYERS * STREAMS
N_COPY = 9 * N_SLOT + STREAMS + 2 * LAYERS + 1
N_PEER = N_ROW * N_COL - 1


def emit_kernel(h_in, k_in, v_in, h_out, k_out, v_out, h_buf, k_buf, v_buf, sem):
    moves = ((h_in, h_buf, h_out), (k_in, k_buf, k_out), (v_in, v_buf, v_out))
    loads = [pltpu.make_async_copy(src, buf, sem.at[i]) for i, (src, buf, _) in enumerate(moves)]
    for copy in loads:
        copy.start()
    stores = []
    for i, (_, buf, dst) in enumerate(moves):
        loads[i].wait()
        copy = pltpu.make_async_copy(buf, dst, sem.at[i])
        copy.start()
        stores.append(copy)
    for copy in stores:
        copy.wait()


def run_step(x, lens, k_cache, v_cache, g1, b1, wq, bq, wk, bk, wv, bv, wo, bo, g2, b2, wf1, bf1, wf2, bf2):
    any_spec = pl.BlockSpec(memory_space=pl.ANY)
    args = (x, lens.reshape(1, BATCH),
            jnp.swapaxes(k_cache, 3, 4).reshape(LAYERS, BATCH * HEAD, SEQ),
            jnp.swapaxes(v_cache, 3, 4).reshape(LAYERS, BATCH * HEAD, SEQ),
            g1, b1, wq, bq, wk, bk, wv, bv, wo, bo, g2, b2, wf1, bf1, wf2, bf2)
    vm = pltpu.VMEM
    in_scratch = [vm(a.shape, a.dtype) for a in args]
    scratch = in_scratch + [
        vm((BATCH, 128), F32),
        vm((LAYERS, BATCH, 128), F32),
        vm((LAYERS, BATCH, 128), BF16),
        vm((ROWS, SEQ), F32),
        vm((ROWS, SEQ), BF16),
        vm((ROWS, 128), F32),
        vm((2 * N_SLOT, 8, 128), F32),
        vm((2 * N_SLOT, N_ROW, 8, 128), F32),
        vm((LAYERS, N_ROW, 8, WIDTH), F32),
        vm((LAYERS, N_ROW, 8, WIDTH), F32),
        vm((LAYERS, 2, 8, FF_HALF), F32),
        vm((LAYERS, N_ROW, 8, FF_HALF), F32),
        vm((N_SLOT, N_ROW, ROWS + HALF, 128), BF16),
        vm((N_SLOT, N_ROW, ROWS + HALF, 128), BF16),
        vm((STREAMS, N_ROW, HALF, 128), BF16),
        vm((STREAMS, N_ROW * N_COL, HALF, 128), BF16),
        vm((N_COL, WIDTH, WIDTH), BF16),
        vm((STREAMS, N_COL, ROWS, WIDTH), BF16),
        vm((STREAMS, ROWS, FF_HALF), F32),
        vm((N_SLOT, ROWS, FF_HALF), BF16),
        vm((N_SLOT, ROWS, FF_HALF), BF16),
        vm((N_SLOT, 2, ROWS, FF_HALF), BF16),
        vm((N_SLOT, 2, ROWS, FF_HALF), BF16),
        vm((N_SLOT, N_COL, ROWS, WIDTH), BF16),
        pltpu.SemaphoreType.DMA((32,)),
        pltpu.SemaphoreType.DMA((2 * N_SLOT,)),
        pltpu.SemaphoreType.DMA((2 * LAYERS + STREAMS,)),
        pltpu.SemaphoreType.DMA((N_COPY,)),
        pltpu.SemaphoreType.DMA((N_COPY,)),
    ]
    shapes = (jax.ShapeDtypeStruct((BATCH, WIDTH), BF16),
              jax.ShapeDtypeStruct((LAYERS, HEAD, BATCH), BF16),
              jax.ShapeDtypeStruct((LAYERS, HEAD, BATCH), BF16))
    results = pl.pallas_call(
        step_kernel,
        out_shape=shapes,
        in_specs=[pl.BlockSpec(memory_space=pltpu.HBM)] * len(args),
        out_specs=(any_spec,) * 3,
        scratch_shapes=scratch,
        compiler_params=pltpu.CompilerParams(
            collective_id=0, has_side_effects=True, vmem_limit_bytes=60 * 1024 * 1024),
        name="decode_step",
    )(*args)
    h_out, k_new, v_new = pl.pallas_call(
        emit_kernel,
        out_shape=shapes,
        in_specs=[any_spec] * 3,
        out_specs=(pl.BlockSpec(memory_space=pltpu.HBM),) * 3,
        scratch_shapes=[vm(a.shape, a.dtype) for a in shapes] + [pltpu.SemaphoreType.DMA((3,))],
        compiler_params=pltpu.CompilerParams(vmem_limit_bytes=60 * 1024 * 1024),
        name="emit",
    )(*results)

    def fresh(rows):
        return jnp.swapaxes(rows, 1, 2).reshape(LAYERS, BATCH, 1, HEAD)

    return h_out, fresh(k_new), fresh(v_new)


def solution(mesh):
    act_spec = P("dp", "row")
    cache_spec = P(None, "dp", ("col", "row"), None, None)
    fresh_spec = P(None, "dp", ("col", "row"), None)
    in_weight = P(None, "row", "col")
    out_weight = P(None, "col", "row")
    col_vec = P(None, "col")
    row_vec = P(None, "row")
    in_specs = (act_spec, P("dp"), cache_spec, cache_spec, row_vec, row_vec,
                in_weight, col_vec, in_weight, col_vec, in_weight, col_vec,
                out_weight, row_vec, row_vec, row_vec, in_weight, col_vec, out_weight, row_vec)
    return jax.shard_map(run_step, mesh=mesh, in_specs=in_specs,
                         out_specs=(act_spec, fresh_spec, fresh_spec), check_vma=False)
```

```python
import functools

import jax
import jax.numpy as jnp
from jax import lax
from jax.experimental import pallas as pl
from jax.experimental.pallas import tpu as pltpu
from jax.sharding import PartitionSpec as P

EPS_LN = 1e-5
MESH = pl.DeviceIdType.MESH
F32 = jnp.float32
BF16 = jnp.bfloat16

LAYERS = 2
BATCH = 128
STREAMS = 2
ROWS = BATCH // STREAMS
HALF = ROWS // 2
GROUP = 16
N_ROW = 4
N_COL = 4
HEAD = 64
SEQ = 512
WIDTH = 256
D_MODEL = 1024
FF_LOC = 1024
FF_HALF = FF_LOC // 2

VEC_NAMES = ("g1", "b1", "bq", "bk", "bv", "bo", "g2", "b2", "bf2")
MAT_NAMES = ("wq", "wk", "wv", "wo", "wf1", "wf2")


def lane_iota(shape):
    return lax.broadcasted_iota(jnp.int32, shape, len(shape) - 1)


def swap_halves(val):
    return pltpu.roll(val, HEAD, 1)


def low_half(shape):
    return lane_iota(shape) < HEAD


def step_kernel(*refs):
    (x_in, len_in, k_in, v_in, g1_in, b1_in, wq_in, bq_in, wk_in, bk_in, wv_in, bv_in,
     wo_in, bo_in, g2_in, b2_in, wf1_in, bf1_in, wf2_in, bf2_in,
     h_out, k_out, v_out,
     x_buf, len_buf, k_buf, v_buf, g1, b1, wq, bq, wk, bk, wv, bv, wo, bo, g2, b2, wf1, bf1, wf2, bf2,
     len_mat, kv_mix, kv_turn, s_buf, p_buf, o_mix,
     st_send, st_recv, gq_send, gq_recv, gf_send, gf_recv, qkv_send, qkv_recv, o_recv,
     proj_recv, f1_mine, f1_send, f1_recv, pair_recv, u_recv, out_recv,
     load_sem, big_sem, store_sem, send_sem, recv_sem) = refs

    row = lax.axis_index("row")
    col = lax.axis_index("col")
    side = lax.rem(row, 2)
    chip = row // 2
    partner = chip * 2 + (1 - side)
    across = lax.rem(row + 2, N_ROW)

    loads = {}

    def load(name, src, dst, sem):
        copy = pltpu.make_async_copy(src, dst, sem)
        copy.start()
        loads[name] = copy

    n_load = [0]

    def small(name, src, dst):
        load(name, src, dst, load_sem.at[n_load[0]])
        n_load[0] += 1

    small("x", x_in, x_buf)
    small("g1", g1_in, g1)
    for layer in range(LAYERS):
        for name, src, dst in (("wq", wq_in, wq), ("wk", wk_in, wk), ("wv", wv_in, wv)):
            if layer == 0:
                small((name, layer), src.at[layer], dst.at[layer])
    for name, src, dst in (("b1", b1_in, b1), ("bq", bq_in, bq), ("bk", bk_in, bk), ("bv", bv_in, bv),
                           ("len", len_in, len_buf), ("bo", bo_in, bo), ("g2", g2_in, g2), ("b2", b2_in, b2),
                           ("bf1", bf1_in, bf1), ("bf2", bf2_in, bf2)):
        small(name, src, dst)

    barrier = pltpu.get_barrier_semaphore()
    for off in range(1, 4):
        pl.semaphore_signal(barrier, inc=1, device_id={"row": lax.rem(row + off, N_ROW)}, device_id_type=MESH)
        pl.semaphore_signal(barrier, inc=1, device_id={"col": lax.rem(col + off, N_COL)}, device_id_type=MESH)

    def big(layer, stream, which):
        src, dst = (k_in, k_buf) if which == 0 else (v_in, v_buf)
        span = pl.ds(stream * ROWS * HEAD, ROWS * HEAD)
        load(("kv", layer, stream, which), src.at[layer, span], dst.at[layer, span],
             big_sem.at[(layer * STREAMS + stream) * 2 + which])

    for stream in range(STREAMS):
        for which in range(2):
            big(0, stream, which)
    for name, src, dst in (("wo", wo_in, wo), ("wf1", wf1_in, wf1), ("wf2", wf2_in, wf2)):
        small((name, 0), src.at[0], dst.at[0])
    for name, src, dst in (("wq", wq_in, wq), ("wk", wk_in, wk), ("wv", wv_in, wv), ("wo", wo_in, wo),
                           ("wf1", wf1_in, wf1), ("wf2", wf2_in, wf2)):
        small((name, 1), src.at[1], dst.at[1])
    for stream in range(STREAMS):
        for which in range(2):
            big(1, stream, which)

    waited = set()

    def need(name):
        if name not in waited:
            waited.add(name)
            loads[name].wait()

    drains = []
    recvs = {}
    n_sem = [0]

    def exchange(tag, copies, span):
        index = n_sem[0]
        n_sem[0] += 1
        for src, dst, device in copies:
            pltpu.make_async_remote_copy(
                src_ref=src, dst_ref=dst, send_sem=send_sem.at[index],
                recv_sem=recv_sem.at[index], device_id=device, device_id_type=MESH).start()
        drains.append(pltpu.make_async_copy(span, span, send_sem.at[index]))
        recvs[tag] = pltpu.make_async_copy(span, span, recv_sem.at[index])

    def to_axis(tag, axis, src_of, buf):
        me = row if axis == "row" else col
        dests = [lax.rem(me + off, 4) for off in (2, 3, 1)]
        exchange(tag, [(src_of(d), buf.at[me], {axis: d}) for d in dests], buf.at[0:3])

    def arrived(tag):
        recvs[tag].wait()

    def local_norm(state, gain):
        mean = jnp.sum(state, axis=-1, keepdims=True) * (1.0 / WIDTH)
        delta = state - mean
        var = jnp.sum(delta * delta, axis=-1, keepdims=True) * (1.0 / WIDTH)
        normed = (delta * lax.rsqrt(var + EPS_LN) * gain).astype(BF16)
        lanes = lane_iota((ROWS, 128))
        tile = jnp.where(lanes == 0, mean, jnp.where(lanes == 1, var, 0.0))
        if ROWS < 128:
            tile = jnp.concatenate([tile] * (128 // ROWS), axis=0)
        return normed, jnp.transpose(tile)[0:8]

    def merge_stats(blocks):
        share = 1.0 / len(blocks)
        mean = sum(m for m, _ in blocks) * share
        var = sum(v + (m - mean) * (m - mean) for m, v in blocks) * share
        return mean, var

    def stat_columns(blocks):
        mean, var = merge_stats(blocks)
        inv = lax.rsqrt(var + EPS_LN)
        lines = [jnp.sqrt(v + EPS_LN) * inv for _, v in blocks] + [(m - mean) * inv for m, _ in blocks]
        sub = lax.broadcasted_iota(jnp.int32, (8, 128), 0)
        tile = jnp.zeros((8, 128), F32)
        for i, line in enumerate(lines):
            tile = jnp.where(sub == i, line, tile)
        turned = jnp.transpose(jnp.concatenate([tile] * 16, axis=0))[0:ROWS]
        return [turned[:, i:i + 1] for i in range(len(lines))]

    def block_stats(index, r):
        tile = st_recv[index, r]
        return tile[0:1], tile[1:2]

    def pack_heads(q, k, v, j, rows):
        half = rows // 2
        lo = (j // 2) * 128
        q, k, v = q[:, lo:lo + 128], k[:, lo:lo + 128], v[:, lo:lo + 128]
        if j % 2 == 0:
            first = jnp.where(low_half((rows, 128)), q, swap_halves(k))
            second = jnp.where(low_half((half, 128)), v[:half], swap_halves(v[half:]))
        else:
            first = jnp.where(low_half((rows, 128)), swap_halves(q), k)
            second = jnp.where(low_half((half, 128)), swap_halves(v[:half]), v[half:])
        return first, second

    def dot(a, b):
        return jnp.dot(a, b, preferred_element_type=F32)

    def send_qkv(layer, stream):
        slot = layer * STREAMS + stream
        need("x")
        need("g1")
        state = x_buf[stream * ROWS:(stream + 1) * ROWS, :].astype(F32)
        normed, tile = local_norm(state, g1[layer:layer + 1, :].astype(F32))
        st_send[2 * slot] = tile
        st_recv[2 * slot, row] = tile
        for name in ("wq", "wk", "wv"):
            need((name, layer))
        q, k, v = dot(normed, wq[layer]), dot(normed, wk[layer]), dot(normed, wv[layer])
        for j in range(N_ROW):
            first, second = pack_heads(q, k, v, j, ROWS)
            qkv_send[slot, j, 0:ROWS] = first.astype(BF16)
            qkv_send[slot, j, ROWS:ROWS + HALF] = second.astype(BF16)
        qkv_recv[slot, row] = qkv_send[slot, row]
        if layer == 0 and stream == 0:
            pl.semaphore_wait(barrier, N_PEER)
        to_axis(("st1", slot), "row", lambda d: st_send.at[2 * slot], st_recv.at[2 * slot])
        to_axis(("qkv", slot), "row", lambda d: qkv_send.at[slot, d], qkv_recv.at[slot])

    def affine_rows(gain, shift):
        sub = lax.broadcasted_iota(jnp.int32, (16, WIDTH), 0)
        return jnp.where(sub == 0, gain.astype(F32), jnp.where(sub == 1, shift.astype(F32), 0.0)).astype(BF16)

    def send_affine(layer, kind):
        bias_on = jnp.where(row == 0, 1.0, 0.0)
        if kind == 0:
            for name in ("b1", "bq", "bk", "bv"):
                need(name)
            rows = affine_rows(g1[layer:layer + 1, :], b1[layer:layer + 1, :])
            parts = []
            for w, b in ((wq, bq), (wk, bk), (wv, bv)):
                bias = b[layer:layer + 1, :].astype(F32) * bias_on
                part = dot(rows, w[layer])[0:8]
                sub_w = lax.broadcasted_iota(jnp.int32, (8, WIDTH), 0)
                parts.append(part + jnp.where(sub_w == 1, bias, 0.0))
            q, k, v = parts
            for j in range(N_ROW):
                lo = (j // 2) * 128
                qj, kj, vj = q[:, lo:lo + 128], k[:, lo:lo + 128], v[:, lo:lo + 128]
                if j % 2 == 0:
                    first = jnp.where(low_half((8, 128)), qj, swap_halves(kj))
                    second = jnp.where(low_half((8, 128)), vj, swap_halves(vj))
                else:
                    first = jnp.where(low_half((8, 128)), swap_halves(qj), kj)
                    second = jnp.where(low_half((8, 128)), swap_halves(vj), vj)
                gq_send[layer, j] = jnp.concatenate([first, second], axis=1)
            gq_recv[layer, row] = gq_send[layer, row]
            to_axis(("gb", layer, kind), "row", lambda d: gq_send.at[layer, d], gq_recv.at[layer])
        else:
            for name in ("g2", "b2", "bf1", ("wf1", layer)):
                need(name)
            rows = affine_rows(g2[layer:layer + 1, :], b2[layer:layer + 1, :])
            part = dot(rows, wf1[layer])[0:8]
            sub_w = lax.broadcasted_iota(jnp.int32, (8, FF_LOC), 0)
            part = part + jnp.where(sub_w == 1, bf1[layer:layer + 1, :].astype(F32) * bias_on, 0.0)
            for j in range(2):
                gf_send[layer, j] = part[:, j * FF_HALF:(j + 1) * FF_HALF]
            gf_recv[layer, row] = gf_send[layer, side]
            to_axis(("gb", layer, kind), "row", lambda d: gf_send.at[layer, lax.rem(d, 2)], gf_recv.at[layer])

    gb_done = set()

    def affine_lines(layer, kind):
        if (layer, kind) not in gb_done:
            gb_done.add((layer, kind))
            arrived(("gb", layer, kind))

    def gain_line(buf, layer, r):
        return buf[layer, r, 0:1]

    def const_line(buf, layer):
        return buf[layer, 0, 1:2] + buf[layer, 1, 1:2] + buf[layer, 2, 1:2] + buf[layer, 3, 1:2]

    def attend(layer, stream):
        slot = layer * STREAMS + stream
        span = slice(stream * ROWS, (stream + 1) * ROWS)
        arrived(("st1", slot))
        cols = stat_columns([block_stats(2 * slot, r) for r in range(N_ROW)])
        affine_lines(layer, 0)
        gains = [gain_line(gq_recv, layer, r) for r in range(N_ROW)]
        const = const_line(gq_recv, layer)
        arrived(("qkv", slot))
        low = low_half((HALF, 128))
        qk = const[:, 0:128]
        vv = const[:, 128:256]
        for r in range(N_ROW):
            part = qkv_recv[slot, r].astype(F32)
            scale, shift = cols[r], cols[4 + r]
            qk = qk + part[0:ROWS] * scale + shift * gains[r][:, 0:128]
            scale_v = jnp.where(low, scale[0:HALF], scale[HALF:ROWS])
            shift_v = jnp.where(low, shift[0:HALF], shift[HALF:ROWS])
            vv = vv + part[ROWS:ROWS + HALF] * scale_v + shift_v * gains[r][:, 128:256]
        full_low = low_half((ROWS, 128))
        qk_turn = swap_halves(qk)
        q2 = (jnp.where(full_low, qk, qk_turn) * (HEAD ** -0.5)).astype(BF16)
        k2 = jnp.where(full_low, qk_turn, qk).astype(BF16)
        vv_turn = swap_halves(vv)
        v2 = jnp.concatenate([jnp.where(low, vv, vv_turn), jnp.where(low, vv_turn, vv)], axis=0).astype(BF16)
        kv_mix[layer, span, :] = jnp.where(full_low, k2.astype(F32), v2.astype(F32))
        score_new = jnp.sum(jnp.where(full_low, q2.astype(F32) * k2.astype(F32), 0.0), axis=-1, keepdims=True)

        need(("kv", layer, stream, 0))
        q_row = lax.broadcasted_iota(jnp.int32, (GROUP, 128), 0)
        q_half = lane_iota((GROUP, 128)) // HEAD
        for g in range(ROWS // GROUP):
            base = (stream * ROWS + g * GROUP) * HEAD
            qg = q2[g * GROUP:(g + 1) * GROUP].astype(F32)
            spread = [jnp.where(q_row == 2 * j + q_half, qg, 0.0).astype(BF16) for j in range(GROUP // 2)]
            s_buf[g * GROUP:(g + 1) * GROUP, :] = dot(jnp.concatenate(spread, axis=1),
                                                      k_buf[layer, base:base + GROUP * HEAD, :])
        positions = lane_iota((ROWS, SEQ)).astype(F32)
        limit = len_mat[span, 0:1]
        scores = jnp.where(positions < limit, s_buf[...], -jnp.inf)
        peak = jnp.maximum(jnp.max(scores, axis=-1, keepdims=True), score_new)
        exp_cache = jnp.exp(scores - peak)
        exp_new = jnp.exp(score_new - peak)
        inv = 1.0 / (jnp.sum(exp_cache, axis=-1, keepdims=True) + exp_new)
        p_buf[...] = (exp_cache * inv).astype(BF16)
        prob_new = (exp_new * inv).astype(BF16).astype(F32)

        need(("kv", layer, stream, 1))
        for g in range(ROWS // GROUP):
            base = (stream * ROWS + g * GROUP) * HEAD
            wide = lax.dot_general(p_buf[g * GROUP:(g + 1) * GROUP, :], v_buf[layer, base:base + GROUP * HEAD, :],
                                   (((1,), (1,)), ((), ())), preferred_element_type=F32)
            acc = jnp.zeros((GROUP, 128), F32)
            for j in range(GROUP // 2):
                acc = acc + jnp.where(q_row == 2 * j + q_half, wide[:, j * 128:(j + 1) * 128], 0.0)
            o_mix[g * GROUP:(g + 1) * GROUP, :] = acc + swap_halves(acc)
        o2 = o_mix[...] + prob_new * v2.astype(F32)
        packed = jnp.where(low, o2[0:HALF], o2[HALF:ROWS]).astype(BF16)
        o_recv[slot, row] = packed
        to_axis(("o", slot), "row", lambda d: o_recv.at[slot, row], o_recv.at[slot])

    def unpack_heads(buf, first):
        low = low_half((HALF, 128))
        parts = [buf[first + r].astype(F32) for r in range(N_ROW)]
        turns = [swap_halves(p) for p in parts]
        pairs = []
        for a, b in ((0, 1), (2, 3)):
            top = jnp.where(low, parts[a], turns[b])
            bottom = jnp.where(low, turns[a], parts[b])
            pairs.append(jnp.concatenate([top, bottom], axis=0).astype(BF16))
        return jnp.concatenate(pairs, axis=1)

    def project(layer, stream):
        slot = layer * STREAMS + stream
        need(("wo", layer))
        arrived(("o", slot))
        proj_recv[slot, col] = dot(unpack_heads(o_recv.at[slot], 0), wo[layer]).astype(BF16)
        to_axis(("proj", slot), "col", lambda d: proj_recv.at[slot, col], proj_recv.at[slot])

    def col_sum(buf):
        total = buf[0].astype(F32)
        for c in range(1, N_COL):
            total = total + buf[c].astype(F32)
        return total

    def residual(total, bias, stream):
        span = slice(stream * ROWS, (stream + 1) * ROWS)
        new = (x_buf[span, :].astype(F32) + (total + bias)).astype(BF16)
        x_buf[span, :] = new
        return new.astype(F32)

    def send_inner(layer, stream):
        slot = layer * STREAMS + stream
        need("bo")
        need("g2")
        need(("wf1", layer))
        arrived(("proj", slot))
        total = col_sum(proj_recv.at[slot])
        state = residual(total, bo[layer:layer + 1, :].astype(F32), stream)
        normed, tile = local_norm(state, g2[layer:layer + 1, :].astype(F32))
        index = 2 * slot + 1
        st_send[index] = tile
        st_recv[index, row] = tile
        mine = st_send.at[index]
        spot = st_recv.at[index, row]
        exchange(("st2", slot), [(mine, spot, {"row": partner})], mine)
        far = lax.rem(partner + 2, N_ROW)
        exchange(("st3", slot), [(mine, spot, {"row": across}), (mine, spot, {"row": far})], st_recv.at[index, 0:2])
        theirs = pl.ds(pl.multiple_of((1 - side) * FF_HALF, FF_HALF), FF_HALF)
        f1_send[slot] = dot(normed, wf1[layer, :, theirs]).astype(BF16)
        exchange(("f1", slot), [(f1_send.at[slot], f1_recv.at[slot], {"row": partner})], f1_recv.at[slot])
        ours = pl.ds(pl.multiple_of(side * FF_HALF, FF_HALF), FF_HALF)
        f1_mine[stream] = dot(normed, wf1[layer, :, ours])

    def send_pair(layer, stream):
        slot = layer * STREAMS + stream
        arrived(("st2", slot))
        cols = stat_columns([block_stats(2 * slot + 1, r) for r in (row, partner)])
        affine_lines(layer, 1)
        arrived(("f1", slot))
        total = f1_mine[stream] * cols[0] + cols[2] * gain_line(gf_recv, layer, row)
        total = total + f1_recv[slot].astype(F32) * cols[1] + cols[3] * gain_line(gf_recv, layer, partner)
        pair_recv[slot, chip] = total.astype(BF16)
        mine = pair_recv.at[slot, chip]
        exchange(("pair", slot), [(mine, mine, {"row": across})], mine)

    def send_act(layer, stream):
        slot = layer * STREAMS + stream
        arrived(("st3", slot))
        pairs = [merge_stats([block_stats(2 * slot + 1, 2 * k + r) for r in range(2)]) for k in range(2)]
        cols = stat_columns(pairs)
        total = const_line(gf_recv, layer)
        arrived(("pair", slot))
        for k in range(2):
            gain = gain_line(gf_recv, layer, 2 * k) + gain_line(gf_recv, layer, 2 * k + 1)
            total = total + pair_recv[slot, k].astype(F32) * cols[k] + cols[2 + k] * gain
        u_recv[slot, side] = jnp.maximum(total, 0.0).astype(BF16)
        mine = u_recv.at[slot, side]
        exchange(("u", slot), [(mine, mine, {"row": partner})], mine)

    def send_out(layer, stream):
        slot = layer * STREAMS + stream
        need(("wf2", layer))
        arrived(("u", slot))
        acc = dot(u_recv[slot, 0], wf2[layer, 0:FF_HALF, :]) + dot(u_recv[slot, 1], wf2[layer, FF_HALF:, :])
        out_recv[slot, col] = acc.astype(BF16)
        to_axis(("out", slot), "col", lambda d: out_recv.at[slot, col], out_recv.at[slot])

    def finish(layer, stream):
        slot = layer * STREAMS + stream
        need("bf2")
        arrived(("out", slot))
        residual(col_sum(out_recv.at[slot]), bf2[layer:layer + 1, :].astype(F32), stream)

    stores = []

    def store(src, dst, index):
        copy = pltpu.make_async_copy(src, dst, store_sem.at[index])
        copy.start()
        stores.append(copy)

    for stream in range(STREAMS):
        send_qkv(0, stream)
    send_affine(0, 0)
    need("len")
    len_mat[...] = jnp.transpose(jnp.broadcast_to(len_buf[...].astype(F32), (128, 128)))
    for layer in range(LAYERS):
        for stream in range(STREAMS):
            attend(layer, stream)
        kv_turn[layer] = jnp.transpose(kv_mix[layer]).astype(BF16)
        store(kv_turn.at[layer, 0:HEAD], k_out.at[layer], 2 * layer)
        store(kv_turn.at[layer, HEAD:2 * HEAD], v_out.at[layer], 2 * layer + 1)
        if layer == 0:
            send_affine(0, 1)
        for stream in range(STREAMS):
            project(layer, stream)
        if layer == 0:
            for name in MAT_NAMES[:3]:
                need((name, 1))
            send_affine(1, 0)
            send_affine(1, 1)
        for stream in range(STREAMS):
            send_inner(layer, stream)
        for stream in range(STREAMS):
            send_pair(layer, stream)
        for stream in range(STREAMS):
            send_act(layer, stream)
        for stream in range(STREAMS):
            send_out(layer, stream)
        for stream in range(STREAMS):
            finish(layer, stream)
            if layer + 1 < LAYERS:
                send_qkv(layer + 1, stream)
            else:
                span = pl.ds(stream * ROWS, ROWS)
                store(x_buf.at[span], h_out.at[span], 2 * LAYERS + stream)
    for copy in stores:
        copy.wait()
    for copy in drains:
        copy.wait()


N_SLOT = LAYERS * STREAMS
N_COPY = 10 * N_SLOT + 2 * LAYERS
N_PEER = N_ROW + N_COL - 2


def emit_kernel(h_in, k_in, v_in, h_out, k_out, v_out, h_buf, k_buf, v_buf, sem):
    moves = ((h_in, h_buf, h_out), (k_in, k_buf, k_out), (v_in, v_buf, v_out))
    loads = [pltpu.make_async_copy(src, buf, sem.at[i]) for i, (src, buf, _) in enumerate(moves)]
    for copy in loads:
        copy.start()
    stores = []
    for i, (_, buf, dst) in enumerate(moves):
        loads[i].wait()
        copy = pltpu.make_async_copy(buf, dst, sem.at[i])
        copy.start()
        stores.append(copy)
    for copy in stores:
        copy.wait()


def run_step(x, lens, k_cache, v_cache, g1, b1, wq, bq, wk, bk, wv, bv, wo, bo, g2, b2, wf1, bf1, wf2, bf2):
    any_spec = pl.BlockSpec(memory_space=pl.ANY)
    args = (x, lens.reshape(1, BATCH),
            jnp.swapaxes(k_cache, 3, 4).reshape(LAYERS, BATCH * HEAD, SEQ),
            jnp.swapaxes(v_cache, 3, 4).reshape(LAYERS, BATCH * HEAD, SEQ),
            g1, b1, wq, bq, wk, bk, wv, bv, wo, bo, g2, b2, wf1, bf1, wf2, bf2)
    vm = pltpu.VMEM
    in_scratch = [vm(a.shape, a.dtype) for a in args]
    scratch = in_scratch + [
        vm((BATCH, 128), F32),
        vm((LAYERS, BATCH, 128), F32),
        vm((LAYERS, BATCH, 128), BF16),
        vm((ROWS, SEQ), F32),
        vm((ROWS, SEQ), BF16),
        vm((ROWS, 128), F32),
        vm((2 * N_SLOT, 8, 128), F32),
        vm((2 * N_SLOT, N_ROW, 8, 128), F32),
        vm((LAYERS, N_ROW, 8, WIDTH), F32),
        vm((LAYERS, N_ROW, 8, WIDTH), F32),
        vm((LAYERS, 2, 8, FF_HALF), F32),
        vm((LAYERS, N_ROW, 8, FF_HALF), F32),
        vm((N_SLOT, N_ROW, ROWS + HALF, 128), BF16),
        vm((N_SLOT, N_ROW, ROWS + HALF, 128), BF16),
        vm((N_SLOT, N_ROW, HALF, 128), BF16),
        vm((N_SLOT, N_COL, ROWS, WIDTH), BF16),
        vm((STREAMS, ROWS, FF_HALF), F32),
        vm((N_SLOT, ROWS, FF_HALF), BF16),
        vm((N_SLOT, ROWS, FF_HALF), BF16),
        vm((N_SLOT, 2, ROWS, FF_HALF), BF16),
        vm((N_SLOT, 2, ROWS, FF_HALF), BF16),
        vm((N_SLOT, N_COL, ROWS, WIDTH), BF16),
        pltpu.SemaphoreType.DMA((32,)),
        pltpu.SemaphoreType.DMA((2 * N_SLOT,)),
        pltpu.SemaphoreType.DMA((2 * LAYERS + STREAMS,)),
        pltpu.SemaphoreType.DMA((N_COPY,)),
        pltpu.SemaphoreType.DMA((N_COPY,)),
    ]
    shapes = (jax.ShapeDtypeStruct((BATCH, WIDTH), BF16),
              jax.ShapeDtypeStruct((LAYERS, HEAD, BATCH), BF16),
              jax.ShapeDtypeStruct((LAYERS, HEAD, BATCH), BF16))
    results = pl.pallas_call(
        step_kernel,
        out_shape=shapes,
        in_specs=[pl.BlockSpec(memory_space=pltpu.HBM)] * len(args),
        out_specs=(any_spec,) * 3,
        scratch_shapes=scratch,
        compiler_params=pltpu.CompilerParams(
            collective_id=0, has_side_effects=True, vmem_limit_bytes=60 * 1024 * 1024),
        name="decode_step",
    )(*args)
    h_out, k_new, v_new = pl.pallas_call(
        emit_kernel,
        out_shape=shapes,
        in_specs=[any_spec] * 3,
        out_specs=(pl.BlockSpec(memory_space=pltpu.HBM),) * 3,
        scratch_shapes=[vm(a.shape, a.dtype) for a in shapes] + [pltpu.SemaphoreType.DMA((3,))],
        compiler_params=pltpu.CompilerParams(vmem_limit_bytes=60 * 1024 * 1024),
        name="emit",
    )(*results)

    def fresh(rows):
        return jnp.swapaxes(rows, 1, 2).reshape(LAYERS, BATCH, 1, HEAD)

    return h_out, fresh(k_new), fresh(v_new)


def solution(mesh):
    act_spec = P("dp", "row")
    cache_spec = P(None, "dp", ("col", "row"), None, None)
    fresh_spec = P(None, "dp", ("col", "row"), None)
    in_weight = P(None, "row", "col")
    out_weight = P(None, "col", "row")
    col_vec = P(None, "col")
    row_vec = P(None, "row")
    in_specs = (act_spec, P("dp"), cache_spec, cache_spec, row_vec, row_vec,
                in_weight, col_vec, in_weight, col_vec, in_weight, col_vec,
                out_weight, row_vec, row_vec, row_vec, in_weight, col_vec, out_weight, row_vec)
    return jax.shard_map(run_step, mesh=mesh, in_specs=in_specs,
                         out_specs=(act_spec, fresh_spec, fresh_spec), check_vma=False)
```

```python
import functools

import jax
import jax.numpy as jnp
from jax import lax
from jax.experimental import pallas as pl
from jax.experimental.pallas import tpu as pltpu
from jax.sharding import PartitionSpec as P

EPS_LN = 1e-5
MESH = pl.DeviceIdType.MESH
F32 = jnp.float32
BF16 = jnp.bfloat16

LAYERS = 2
BATCH = 128
STREAMS = 4
ROWS = BATCH // STREAMS
HALF = ROWS // 2
GROUP = 16
N_ROW = 4
N_COL = 4
HEAD = 64
SEQ = 512
WIDTH = 256
D_MODEL = 1024
FF_LOC = 1024
FF_HALF = FF_LOC // 2

VEC_NAMES = ("g1", "b1", "bq", "bk", "bv", "bo", "g2", "b2", "bf2")
MAT_NAMES = ("wq", "wk", "wv", "wo", "wf1", "wf2")


def lane_iota(shape):
    return lax.broadcasted_iota(jnp.int32, shape, len(shape) - 1)


def swap_halves(val):
    return pltpu.roll(val, HEAD, 1)


def low_half(shape):
    return lane_iota(shape) < HEAD


def step_kernel(*refs):
    (x_in, len_in, k_in, v_in, g1_in, b1_in, wq_in, bq_in, wk_in, bk_in, wv_in, bv_in,
     wo_in, bo_in, g2_in, b2_in, wf1_in, bf1_in, wf2_in, bf2_in,
     h_out, k_out, v_out,
     x_buf, len_buf, k_buf, v_buf, g1, b1, wq, bq, wk, bk, wv, bv, wo, bo, g2, b2, wf1, bf1, wf2, bf2,
     len_mat, kv_mix, kv_turn, s_buf, p_buf, o_mix,
     st_send, st_recv, gq_send, gq_recv, gf_send, gf_recv, qkv_send, qkv_recv, o_recv,
     proj_recv, f1_mine, f1_send, f1_recv, pair_recv, u_recv, out_recv,
     load_sem, big_sem, store_sem, send_sem, recv_sem) = refs

    row = lax.axis_index("row")
    col = lax.axis_index("col")
    side = lax.rem(row, 2)
    chip = row // 2
    partner = chip * 2 + (1 - side)
    across = lax.rem(row + 2, N_ROW)

    loads = {}

    def load(name, src, dst, sem):
        copy = pltpu.make_async_copy(src, dst, sem)
        copy.start()
        loads[name] = copy

    n_load = [0]

    def small(name, src, dst):
        load(name, src, dst, load_sem.at[n_load[0]])
        n_load[0] += 1

    small("x", x_in, x_buf)
    small("g1", g1_in, g1)
    for layer in range(LAYERS):
        for name, src, dst in (("wq", wq_in, wq), ("wk", wk_in, wk), ("wv", wv_in, wv)):
            if layer == 0:
                small((name, layer), src.at[layer], dst.at[layer])
    for name, src, dst in (("b1", b1_in, b1), ("bq", bq_in, bq), ("bk", bk_in, bk), ("bv", bv_in, bv),
                           ("len", len_in, len_buf), ("bo", bo_in, bo), ("g2", g2_in, g2), ("b2", b2_in, b2),
                           ("bf1", bf1_in, bf1), ("bf2", bf2_in, bf2)):
        small(name, src, dst)

    barrier = pltpu.get_barrier_semaphore()
    for off in range(1, 4):
        pl.semaphore_signal(barrier, inc=1, device_id={"row": lax.rem(row + off, N_ROW)}, device_id_type=MESH)
        pl.semaphore_signal(barrier, inc=1, device_id={"col": lax.rem(col + off, N_COL)}, device_id_type=MESH)

    def big(layer, stream, which):
        src, dst = (k_in, k_buf) if which == 0 else (v_in, v_buf)
        span = pl.ds(stream * ROWS * HEAD, ROWS * HEAD)
        load(("kv", layer, stream, which), src.at[layer, span], dst.at[layer, span],
             big_sem.at[(layer * STREAMS + stream) * 2 + which])

    for stream in range(STREAMS):
        for which in range(2):
            big(0, stream, which)
    for name, src, dst in (("wo", wo_in, wo), ("wf1", wf1_in, wf1), ("wf2", wf2_in, wf2)):
        small((name, 0), src.at[0], dst.at[0])
    for name, src, dst in (("wq", wq_in, wq), ("wk", wk_in, wk), ("wv", wv_in, wv), ("wo", wo_in, wo),
                           ("wf1", wf1_in, wf1), ("wf2", wf2_in, wf2)):
        small((name, 1), src.at[1], dst.at[1])
    for stream in range(STREAMS):
        for which in range(2):
            big(1, stream, which)

    waited = set()

    def need(name):
        if name not in waited:
            waited.add(name)
            loads[name].wait()

    drains = []
    recvs = {}
    n_sem = [0]

    def exchange(tag, copies, span):
        index = n_sem[0]
        n_sem[0] += 1
        for src, dst, device in copies:
            pltpu.make_async_remote_copy(
                src_ref=src, dst_ref=dst, send_sem=send_sem.at[index],
                recv_sem=recv_sem.at[index], device_id=device, device_id_type=MESH).start()
        drains.append(pltpu.make_async_copy(span, span, send_sem.at[index]))
        recvs[tag] = pltpu.make_async_copy(span, span, recv_sem.at[index])

    def to_axis(tag, axis, src_of, buf):
        me = row if axis == "row" else col
        dests = [lax.rem(me + off, 4) for off in (2, 3, 1)]
        exchange(tag, [(src_of(d), buf.at[me], {axis: d}) for d in dests], buf.at[0:3])

    def arrived(tag):
        recvs[tag].wait()

    def local_norm(state, gain):
        mean = jnp.sum(state, axis=-1, keepdims=True) * (1.0 / WIDTH)
        delta = state - mean
        var = jnp.sum(delta * delta, axis=-1, keepdims=True) * (1.0 / WIDTH)
        normed = (delta * lax.rsqrt(var + EPS_LN) * gain).astype(BF16)
        lanes = lane_iota((ROWS, 128))
        tile = jnp.where(lanes == 0, mean, jnp.where(lanes == 1, var, 0.0))
        if ROWS < 128:
            tile = jnp.concatenate([tile] * (128 // ROWS), axis=0)
        return normed, jnp.transpose(tile)[0:8]

    def merge_stats(blocks):
        share = 1.0 / len(blocks)
        mean = sum(m for m, _ in blocks) * share
        var = sum(v + (m - mean) * (m - mean) for m, v in blocks) * share
        return mean, var

    def stat_columns(blocks):
        mean, var = merge_stats(blocks)
        inv = lax.rsqrt(var + EPS_LN)
        lines = [jnp.sqrt(v + EPS_LN) * inv for _, v in blocks] + [(m - mean) * inv for m, _ in blocks]
        sub = lax.broadcasted_iota(jnp.int32, (8, 128), 0)
        tile = jnp.zeros((8, 128), F32)
        for i, line in enumerate(lines):
            tile = jnp.where(sub == i, line, tile)
        turned = jnp.transpose(jnp.concatenate([tile] * 16, axis=0))[0:ROWS]
        return [turned[:, i:i + 1] for i in range(len(lines))]

    def block_stats(index, r):
        tile = st_recv[index, r]
        return tile[0:1], tile[1:2]

    def pack_heads(q, k, v, j, rows):
        half = rows // 2
        lo = (j // 2) * 128
        q, k, v = q[:, lo:lo + 128], k[:, lo:lo + 128], v[:, lo:lo + 128]
        if j % 2 == 0:
            first = jnp.where(low_half((rows, 128)), q, swap_halves(k))
            second = jnp.where(low_half((half, 128)), v[:half], swap_halves(v[half:]))
        else:
            first = jnp.where(low_half((rows, 128)), swap_halves(q), k)
            second = jnp.where(low_half((half, 128)), swap_halves(v[:half]), v[half:])
        return first, second

    def dot(a, b):
        return jnp.dot(a, b, preferred_element_type=F32)

    def send_qkv(layer, stream):
        slot = layer * STREAMS + stream
        need("x")
        need("g1")
        state = x_buf[stream * ROWS:(stream + 1) * ROWS, :].astype(F32)
        normed, tile = local_norm(state, g1[layer:layer + 1, :].astype(F32))
        st_send[2 * slot] = tile
        st_recv[2 * slot, row] = tile
        for name in ("wq", "wk", "wv"):
            need((name, layer))
        q, k, v = dot(normed, wq[layer]), dot(normed, wk[layer]), dot(normed, wv[layer])
        for j in range(N_ROW):
            first, second = pack_heads(q, k, v, j, ROWS)
            qkv_send[slot, j, 0:ROWS] = first.astype(BF16)
            qkv_send[slot, j, ROWS:ROWS + HALF] = second.astype(BF16)
        qkv_recv[slot, row] = qkv_send[slot, row]
        if layer == 0 and stream == 0:
            pl.semaphore_wait(barrier, N_PEER)
        to_axis(("st1", slot), "row", lambda d: st_send.at[2 * slot], st_recv.at[2 * slot])
        to_axis(("qkv", slot), "row", lambda d: qkv_send.at[slot, d], qkv_recv.at[slot])

    def affine_rows(gain, shift):
        sub = lax.broadcasted_iota(jnp.int32, (16, WIDTH), 0)
        return jnp.where(sub == 0, gain.astype(F32), jnp.where(sub == 1, shift.astype(F32), 0.0)).astype(BF16)

    def send_affine(layer, kind):
        bias_on = jnp.where(row == 0, 1.0, 0.0)
        if kind == 0:
            for name in ("b1", "bq", "bk", "bv"):
                need(name)
            rows = affine_rows(g1[layer:layer + 1, :], b1[layer:layer + 1, :])
            parts = []
            for w, b in ((wq, bq), (wk, bk), (wv, bv)):
                bias = b[layer:layer + 1, :].astype(F32) * bias_on
                part = dot(rows, w[layer])[0:8]
                sub_w = lax.broadcasted_iota(jnp.int32, (8, WIDTH), 0)
                parts.append(part + jnp.where(sub_w == 1, bias, 0.0))
            q, k, v = parts
            for j in range(N_ROW):
                lo = (j // 2) * 128
                qj, kj, vj = q[:, lo:lo + 128], k[:, lo:lo + 128], v[:, lo:lo + 128]
                if j % 2 == 0:
                    first = jnp.where(low_half((8, 128)), qj, swap_halves(kj))
                    second = jnp.where(low_half((8, 128)), vj, swap_halves(vj))
                else:
                    first = jnp.where(low_half((8, 128)), swap_halves(qj), kj)
                    second = jnp.where(low_half((8, 128)), swap_halves(vj), vj)
                gq_send[layer, j] = jnp.concatenate([first, second], axis=1)
            gq_recv[layer, row] = gq_send[layer, row]
            to_axis(("gb", layer, kind), "row", lambda d: gq_send.at[layer, d], gq_recv.at[layer])
        else:
            for name in ("g2", "b2", "bf1", ("wf1", layer)):
                need(name)
            rows = affine_rows(g2[layer:layer + 1, :], b2[layer:layer + 1, :])
            part = dot(rows, wf1[layer])[0:8]
            sub_w = lax.broadcasted_iota(jnp.int32, (8, FF_LOC), 0)
            part = part + jnp.where(sub_w == 1, bf1[layer:layer + 1, :].astype(F32) * bias_on, 0.0)
            for j in range(2):
                gf_send[layer, j] = part[:, j * FF_HALF:(j + 1) * FF_HALF]
            gf_recv[layer, row] = gf_send[layer, side]
            to_axis(("gb", layer, kind), "row", lambda d: gf_send.at[layer, lax.rem(d, 2)], gf_recv.at[layer])

    gb_done = set()

    def affine_lines(layer, kind):
        if (layer, kind) not in gb_done:
            gb_done.add((layer, kind))
            arrived(("gb", layer, kind))

    def gain_line(buf, layer, r):
        return buf[layer, r, 0:1]

    def const_line(buf, layer):
        return buf[layer, 0, 1:2] + buf[layer, 1, 1:2] + buf[layer, 2, 1:2] + buf[layer, 3, 1:2]

    def attend(layer, stream):
        slot = layer * STREAMS + stream
        span = slice(stream * ROWS, (stream + 1) * ROWS)
        arrived(("st1", slot))
        cols = stat_columns([block_stats(2 * slot, r) for r in range(N_ROW)])
        affine_lines(layer, 0)
        gains = [gain_line(gq_recv, layer, r) for r in range(N_ROW)]
        const = const_line(gq_recv, layer)
        arrived(("qkv", slot))
        low = low_half((HALF, 128))
        qk = const[:, 0:128]
        vv = const[:, 128:256]
        for r in range(N_ROW):
            part = qkv_recv[slot, r].astype(F32)
            scale, shift = cols[r], cols[4 + r]
            qk = qk + part[0:ROWS] * scale + shift * gains[r][:, 0:128]
            scale_v = jnp.where(low, scale[0:HALF], scale[HALF:ROWS])
            shift_v = jnp.where(low, shift[0:HALF], shift[HALF:ROWS])
            vv = vv + part[ROWS:ROWS + HALF] * scale_v + shift_v * gains[r][:, 128:256]
        full_low = low_half((ROWS, 128))
        qk_turn = swap_halves(qk)
        q2 = (jnp.where(full_low, qk, qk_turn) * (HEAD ** -0.5)).astype(BF16)
        k2 = jnp.where(full_low, qk_turn, qk).astype(BF16)
        vv_turn = swap_halves(vv)
        v2 = jnp.concatenate([jnp.where(low, vv, vv_turn), jnp.where(low, vv_turn, vv)], axis=0).astype(BF16)
        kv_mix[layer, span, :] = jnp.where(full_low, k2.astype(F32), v2.astype(F32))
        score_new = jnp.sum(jnp.where(full_low, q2.astype(F32) * k2.astype(F32), 0.0), axis=-1, keepdims=True)

        need(("kv", layer, stream, 0))
        q_row = lax.broadcasted_iota(jnp.int32, (GROUP, 128), 0)
        q_half = lane_iota((GROUP, 128)) // HEAD
        for g in range(ROWS // GROUP):
            base = (stream * ROWS + g * GROUP) * HEAD
            qg = q2[g * GROUP:(g + 1) * GROUP].astype(F32)
            spread = [jnp.where(q_row == 2 * j + q_half, qg, 0.0).astype(BF16) for j in range(GROUP // 2)]
            s_buf[g * GROUP:(g + 1) * GROUP, :] = dot(jnp.concatenate(spread, axis=1),
                                                      k_buf[layer, base:base + GROUP * HEAD, :])
        positions = lane_iota((ROWS, SEQ)).astype(F32)
        limit = len_mat[span, 0:1]
        scores = jnp.where(positions < limit, s_buf[...], -jnp.inf)
        peak = jnp.maximum(jnp.max(scores, axis=-1, keepdims=True), score_new)
        exp_cache = jnp.exp(scores - peak)
        exp_new = jnp.exp(score_new - peak)
        inv = 1.0 / (jnp.sum(exp_cache, axis=-1, keepdims=True) + exp_new)
        p_buf[...] = (exp_cache * inv).astype(BF16)
        prob_new = (exp_new * inv).astype(BF16).astype(F32)

        need(("kv", layer, stream, 1))
        for g in range(ROWS // GROUP):
            base = (stream * ROWS + g * GROUP) * HEAD
            wide = lax.dot_general(p_buf[g * GROUP:(g + 1) * GROUP, :], v_buf[layer, base:base + GROUP * HEAD, :],
                                   (((1,), (1,)), ((), ())), preferred_element_type=F32)
            acc = jnp.zeros((GROUP, 128), F32)
            for j in range(GROUP // 2):
                acc = acc + jnp.where(q_row == 2 * j + q_half, wide[:, j * 128:(j + 1) * 128], 0.0)
            o_mix[g * GROUP:(g + 1) * GROUP, :] = acc + swap_halves(acc)
        o2 = o_mix[...] + prob_new * v2.astype(F32)
        packed = jnp.where(low, o2[0:HALF], o2[HALF:ROWS]).astype(BF16)
        o_recv[slot, row] = packed
        to_axis(("o", slot), "row", lambda d: o_recv.at[slot, row], o_recv.at[slot])

    def unpack_heads(buf, first):
        low = low_half((HALF, 128))
        parts = [buf[first + r].astype(F32) for r in range(N_ROW)]
        turns = [swap_halves(p) for p in parts]
        pairs = []
        for a, b in ((0, 1), (2, 3)):
            top = jnp.where(low, parts[a], turns[b])
            bottom = jnp.where(low, turns[a], parts[b])
            pairs.append(jnp.concatenate([top, bottom], axis=0).astype(BF16))
        return jnp.concatenate(pairs, axis=1)

    def project(layer, stream):
        slot = layer * STREAMS + stream
        need(("wo", layer))
        arrived(("o", slot))
        proj_recv[slot, col] = dot(unpack_heads(o_recv.at[slot], 0), wo[layer]).astype(BF16)
        to_axis(("proj", slot), "col", lambda d: proj_recv.at[slot, col], proj_recv.at[slot])

    def col_sum(buf):
        total = buf[0].astype(F32)
        for c in range(1, N_COL):
            total = total + buf[c].astype(F32)
        return total

    def residual(total, bias, stream):
        span = slice(stream * ROWS, (stream + 1) * ROWS)
        new = (x_buf[span, :].astype(F32) + (total + bias)).astype(BF16)
        x_buf[span, :] = new
        return new.astype(F32)

    def send_inner(layer, stream):
        slot = layer * STREAMS + stream
        need("bo")
        need("g2")
        need(("wf1", layer))
        arrived(("proj", slot))
        total = col_sum(proj_recv.at[slot])
        state = residual(total, bo[layer:layer + 1, :].astype(F32), stream)
        normed, tile = local_norm(state, g2[layer:layer + 1, :].astype(F32))
        index = 2 * slot + 1
        st_send[index] = tile
        st_recv[index, row] = tile
        mine = st_send.at[index]
        spot = st_recv.at[index, row]
        exchange(("st2", slot), [(mine, spot, {"row": partner})], mine)
        far = lax.rem(partner + 2, N_ROW)
        exchange(("st3", slot), [(mine, spot, {"row": across}), (mine, spot, {"row": far})], st_recv.at[index, 0:2])
        theirs = pl.ds(pl.multiple_of((1 - side) * FF_HALF, FF_HALF), FF_HALF)
        f1_send[slot] = dot(normed, wf1[layer, :, theirs]).astype(BF16)
        exchange(("f1", slot), [(f1_send.at[slot], f1_recv.at[slot], {"row": partner})], f1_recv.at[slot])
        ours = pl.ds(pl.multiple_of(side * FF_HALF, FF_HALF), FF_HALF)
        f1_mine[stream] = dot(normed, wf1[layer, :, ours])

    def send_pair(layer, stream):
        slot = layer * STREAMS + stream
        arrived(("st2", slot))
        cols = stat_columns([block_stats(2 * slot + 1, r) for r in (row, partner)])
        affine_lines(layer, 1)
        arrived(("f1", slot))
        total = f1_mine[stream] * cols[0] + cols[2] * gain_line(gf_recv, layer, row)
        total = total + f1_recv[slot].astype(F32) * cols[1] + cols[3] * gain_line(gf_recv, layer, partner)
        pair_recv[slot, chip] = total.astype(BF16)
        mine = pair_recv.at[slot, chip]
        exchange(("pair", slot), [(mine, mine, {"row": across})], mine)

    def send_act(layer, stream):
        slot = layer * STREAMS + stream
        arrived(("st3", slot))
        pairs = [merge_stats([block_stats(2 * slot + 1, 2 * k + r) for r in range(2)]) for k in range(2)]
        cols = stat_columns(pairs)
        total = const_line(gf_recv, layer)
        arrived(("pair", slot))
        for k in range(2):
            gain = gain_line(gf_recv, layer, 2 * k) + gain_line(gf_recv, layer, 2 * k + 1)
            total = total + pair_recv[slot, k].astype(F32) * cols[k] + cols[2 + k] * gain
        u_recv[slot, side] = jnp.maximum(total, 0.0).astype(BF16)
        mine = u_recv.at[slot, side]
        exchange(("u", slot), [(mine, mine, {"row": partner})], mine)

    def send_out(layer, stream):
        slot = layer * STREAMS + stream
        need(("wf2", layer))
        arrived(("u", slot))
        acc = dot(u_recv[slot, 0], wf2[layer, 0:FF_HALF, :]) + dot(u_recv[slot, 1], wf2[layer, FF_HALF:, :])
        out_recv[slot, col] = acc.astype(BF16)
        to_axis(("out", slot), "col", lambda d: out_recv.at[slot, col], out_recv.at[slot])

    def finish(layer, stream):
        slot = layer * STREAMS + stream
        need("bf2")
        arrived(("out", slot))
        residual(col_sum(out_recv.at[slot]), bf2[layer:layer + 1, :].astype(F32), stream)

    stores = []

    def store(src, dst, index):
        copy = pltpu.make_async_copy(src, dst, store_sem.at[index])
        copy.start()
        stores.append(copy)

    for stream in range(STREAMS):
        send_qkv(0, stream)
    send_affine(0, 0)
    need("len")
    len_mat[...] = jnp.transpose(jnp.broadcast_to(len_buf[...].astype(F32), (128, 128)))
    for layer in range(LAYERS):
        for stream in range(STREAMS):
            attend(layer, stream)
        kv_turn[layer] = jnp.transpose(kv_mix[layer]).astype(BF16)
        store(kv_turn.at[layer, 0:HEAD], k_out.at[layer], 2 * layer)
        store(kv_turn.at[layer, HEAD:2 * HEAD], v_out.at[layer], 2 * layer + 1)
        if layer == 0:
            send_affine(0, 1)
        for stream in range(STREAMS):
            project(layer, stream)
        if layer == 0:
            for name in MAT_NAMES[:3]:
                need((name, 1))
            send_affine(1, 0)
            send_affine(1, 1)
        for stream in range(STREAMS):
            send_inner(layer, stream)
        for stream in range(STREAMS):
            send_pair(layer, stream)
        for stream in range(STREAMS):
            send_act(layer, stream)
        for stream in range(STREAMS):
            send_out(layer, stream)
        for stream in range(STREAMS):
            finish(layer, stream)
            if layer + 1 < LAYERS:
                send_qkv(layer + 1, stream)
            else:
                span = pl.ds(stream * ROWS, ROWS)
                store(x_buf.at[span], h_out.at[span], 2 * LAYERS + stream)
    for copy in stores:
        copy.wait()
    for copy in drains:
        copy.wait()


N_SLOT = LAYERS * STREAMS
N_COPY = 10 * N_SLOT + 2 * LAYERS
N_PEER = N_ROW + N_COL - 2


def emit_kernel(h_in, k_in, v_in, h_out, k_out, v_out, h_buf, k_buf, v_buf, sem):
    moves = ((h_in, h_buf, h_out), (k_in, k_buf, k_out), (v_in, v_buf, v_out))
    loads = [pltpu.make_async_copy(src, buf, sem.at[i]) for i, (src, buf, _) in enumerate(moves)]
    for copy in loads:
        copy.start()
    stores = []
    for i, (_, buf, dst) in enumerate(moves):
        loads[i].wait()
        copy = pltpu.make_async_copy(buf, dst, sem.at[i])
        copy.start()
        stores.append(copy)
    for copy in stores:
        copy.wait()


def run_step(x, lens, k_cache, v_cache, g1, b1, wq, bq, wk, bk, wv, bv, wo, bo, g2, b2, wf1, bf1, wf2, bf2):
    any_spec = pl.BlockSpec(memory_space=pl.ANY)
    args = (x, lens.reshape(1, BATCH),
            jnp.swapaxes(k_cache, 3, 4).reshape(LAYERS, BATCH * HEAD, SEQ),
            jnp.swapaxes(v_cache, 3, 4).reshape(LAYERS, BATCH * HEAD, SEQ),
            g1, b1, wq, bq, wk, bk, wv, bv, wo, bo, g2, b2, wf1, bf1, wf2, bf2)
    vm = pltpu.VMEM
    in_scratch = [vm(a.shape, a.dtype) for a in args]
    scratch = in_scratch + [
        vm((BATCH, 128), F32),
        vm((LAYERS, BATCH, 128), F32),
        vm((LAYERS, BATCH, 128), BF16),
        vm((ROWS, SEQ), F32),
        vm((ROWS, SEQ), BF16),
        vm((ROWS, 128), F32),
        vm((2 * N_SLOT, 8, 128), F32),
        vm((2 * N_SLOT, N_ROW, 8, 128), F32),
        vm((LAYERS, N_ROW, 8, WIDTH), F32),
        vm((LAYERS, N_ROW, 8, WIDTH), F32),
        vm((LAYERS, 2, 8, FF_HALF), F32),
        vm((LAYERS, N_ROW, 8, FF_HALF), F32),
        vm((N_SLOT, N_ROW, ROWS + HALF, 128), BF16),
        vm((N_SLOT, N_ROW, ROWS + HALF, 128), BF16),
        vm((N_SLOT, N_ROW, HALF, 128), BF16),
        vm((N_SLOT, N_COL, ROWS, WIDTH), BF16),
        vm((STREAMS, ROWS, FF_HALF), F32),
        vm((N_SLOT, ROWS, FF_HALF), BF16),
        vm((N_SLOT, ROWS, FF_HALF), BF16),
        vm((N_SLOT, 2, ROWS, FF_HALF), BF16),
        vm((N_SLOT, 2, ROWS, FF_HALF), BF16),
        vm((N_SLOT, N_COL, ROWS, WIDTH), BF16),
        pltpu.SemaphoreType.DMA((32,)),
        pltpu.SemaphoreType.DMA((2 * N_SLOT,)),
        pltpu.SemaphoreType.DMA((2 * LAYERS + STREAMS,)),
        pltpu.SemaphoreType.DMA((N_COPY,)),
        pltpu.SemaphoreType.DMA((N_COPY,)),
    ]
    shapes = (jax.ShapeDtypeStruct((BATCH, WIDTH), BF16),
              jax.ShapeDtypeStruct((LAYERS, HEAD, BATCH), BF16),
              jax.ShapeDtypeStruct((LAYERS, HEAD, BATCH), BF16))
    results = pl.pallas_call(
        step_kernel,
        out_shape=shapes,
        in_specs=[pl.BlockSpec(memory_space=pltpu.HBM)] * len(args),
        out_specs=(any_spec,) * 3,
        scratch_shapes=scratch,
        compiler_params=pltpu.CompilerParams(
            collective_id=0, has_side_effects=True, vmem_limit_bytes=60 * 1024 * 1024),
        name="decode_step",
    )(*args)
    h_out, k_new, v_new = pl.pallas_call(
        emit_kernel,
        out_shape=shapes,
        in_specs=[any_spec] * 3,
        out_specs=(pl.BlockSpec(memory_space=pltpu.HBM),) * 3,
        scratch_shapes=[vm(a.shape, a.dtype) for a in shapes] + [pltpu.SemaphoreType.DMA((3,))],
        compiler_params=pltpu.CompilerParams(vmem_limit_bytes=60 * 1024 * 1024),
        name="emit",
    )(*results)

    def fresh(rows):
        return jnp.swapaxes(rows, 1, 2).reshape(LAYERS, BATCH, 1, HEAD)

    return h_out, fresh(k_new), fresh(v_new)


def solution(mesh):
    act_spec = P("dp", "row")
    cache_spec = P(None, "dp", ("col", "row"), None, None)
    fresh_spec = P(None, "dp", ("col", "row"), None)
    in_weight = P(None, "row", "col")
    out_weight = P(None, "col", "row")
    col_vec = P(None, "col")
    row_vec = P(None, "row")
    in_specs = (act_spec, P("dp"), cache_spec, cache_spec, row_vec, row_vec,
                in_weight, col_vec, in_weight, col_vec, in_weight, col_vec,
                out_weight, row_vec, row_vec, row_vec, in_weight, col_vec, out_weight, row_vec)
    return jax.shard_map(run_step, mesh=mesh, in_specs=in_specs,
                         out_specs=(act_spec, fresh_spec, fresh_spec), check_vma=False)
```

```python
import functools

import jax
import jax.numpy as jnp
from jax import lax
from jax.experimental import pallas as pl
from jax.experimental.pallas import tpu as pltpu
from jax.sharding import PartitionSpec as P

EPS_LN = 1e-5
MESH = pl.DeviceIdType.MESH
F32 = jnp.float32
BF16 = jnp.bfloat16

LAYERS = 2
BATCH = 128
STREAMS = 2
ROWS = BATCH // STREAMS
HALF = ROWS // 2
GROUP = 16
COL_PIECES = 4
N_ROW = 4
N_COL = 4
HEAD = 64
SEQ = 512
WIDTH = 256
D_MODEL = 1024
FF_LOC = 1024
FF_HALF = FF_LOC // 2

VEC_NAMES = ("g1", "b1", "bq", "bk", "bv", "bo", "g2", "b2", "bf2")
MAT_NAMES = ("wq", "wk", "wv", "wo", "wf1", "wf2")


def lane_iota(shape):
    return lax.broadcasted_iota(jnp.int32, shape, len(shape) - 1)


def swap_halves(val):
    return pltpu.roll(val, HEAD, 1)


def low_half(shape):
    return lane_iota(shape) < HEAD


def step_kernel(*refs):
    (x_in, len_in, k_in, v_in, g1_in, b1_in, wq_in, bq_in, wk_in, bk_in, wv_in, bv_in,
     wo_in, bo_in, g2_in, b2_in, wf1_in, bf1_in, wf2_in, bf2_in,
     h_out, k_out, v_out,
     x_buf, len_buf, k_buf, v_buf, g1, b1, wq, bq, wk, bk, wv, bv, wo, bo, g2, b2, wf1, bf1, wf2, bf2,
     len_mat, kv_mix, kv_turn, s_buf, p_buf, o_mix,
     st_send, st_recv, gq_send, gq_recv, gf_send, gf_recv, qkv_send, qkv_recv, o_recv,
     proj_recv, f1_mine, f1_send, f1_recv, pair_recv, u_recv, out_recv,
     load_sem, big_sem, store_sem, send_sem, recv_sem) = refs

    row = lax.axis_index("row")
    col = lax.axis_index("col")
    side = lax.rem(row, 2)
    chip = row // 2
    partner = chip * 2 + (1 - side)
    across = lax.rem(row + 2, N_ROW)

    loads = {}

    def load(name, src, dst, sem):
        copy = pltpu.make_async_copy(src, dst, sem)
        copy.start()
        loads[name] = copy

    n_load = [0]

    def small(name, src, dst):
        load(name, src, dst, load_sem.at[n_load[0]])
        n_load[0] += 1

    small("x", x_in, x_buf)
    small("g1", g1_in, g1)
    for layer in range(LAYERS):
        for name, src, dst in (("wq", wq_in, wq), ("wk", wk_in, wk), ("wv", wv_in, wv)):
            if layer == 0:
                small((name, layer), src.at[layer], dst.at[layer])
    for name, src, dst in (("b1", b1_in, b1), ("bq", bq_in, bq), ("bk", bk_in, bk), ("bv", bv_in, bv),
                           ("len", len_in, len_buf), ("bo", bo_in, bo), ("g2", g2_in, g2), ("b2", b2_in, b2),
                           ("bf1", bf1_in, bf1), ("bf2", bf2_in, bf2)):
        small(name, src, dst)

    barrier = pltpu.get_barrier_semaphore()
    for off in range(1, 4):
        pl.semaphore_signal(barrier, inc=1, device_id={"row": lax.rem(row + off, N_ROW)}, device_id_type=MESH)
        pl.semaphore_signal(barrier, inc=1, device_id={"col": lax.rem(col + off, N_COL)}, device_id_type=MESH)

    def big(layer, stream, which):
        src, dst = (k_in, k_buf) if which == 0 else (v_in, v_buf)
        span = pl.ds(stream * ROWS * HEAD, ROWS * HEAD)
        load(("kv", layer, stream, which), src.at[layer, span], dst.at[layer, span],
             big_sem.at[(layer * STREAMS + stream) * 2 + which])

    for stream in range(STREAMS):
        for which in range(2):
            big(0, stream, which)
    for name, src, dst in (("wo", wo_in, wo), ("wf1", wf1_in, wf1), ("wf2", wf2_in, wf2)):
        small((name, 0), src.at[0], dst.at[0])
    for name, src, dst in (("wq", wq_in, wq), ("wk", wk_in, wk), ("wv", wv_in, wv), ("wo", wo_in, wo),
                           ("wf1", wf1_in, wf1), ("wf2", wf2_in, wf2)):
        small((name, 1), src.at[1], dst.at[1])
    for stream in range(STREAMS):
        for which in range(2):
            big(1, stream, which)

    waited = set()

    def need(name):
        if name not in waited:
            waited.add(name)
            loads[name].wait()

    drains = []
    recvs = {}
    n_sem = [0]

    def exchange(tag, copies, span):
        index = n_sem[0]
        n_sem[0] += 1
        for src, dst, device in copies:
            pltpu.make_async_remote_copy(
                src_ref=src, dst_ref=dst, send_sem=send_sem.at[index],
                recv_sem=recv_sem.at[index], device_id=device, device_id_type=MESH).start()
        drains.append(pltpu.make_async_copy(span, span, send_sem.at[index]))
        recvs[tag] = pltpu.make_async_copy(span, span, recv_sem.at[index])

    def to_col(tag, buf):
        peers = (3 - col, lax.rem(col + 2, N_COL), col + 1 - 2 * lax.rem(col, 2))
        rows = ROWS // COL_PIECES
        copies = []
        for piece in range(COL_PIECES):
            mine = buf.at[col, piece * rows:(piece + 1) * rows]
            copies += [(mine, mine, {"col": peer}) for peer in peers]
        exchange(tag, copies, buf.at[0:3])

    def to_axis(tag, axis, src_of, buf):
        me = row if axis == "row" else col
        dests = [lax.rem(me + off, 4) for off in (2, 3, 1)]
        exchange(tag, [(src_of(d), buf.at[me], {axis: d}) for d in dests], buf.at[0:3])

    def arrived(tag):
        recvs[tag].wait()

    def local_norm(state, gain):
        mean = jnp.sum(state, axis=-1, keepdims=True) * (1.0 / WIDTH)
        delta = state - mean
        var = jnp.sum(delta * delta, axis=-1, keepdims=True) * (1.0 / WIDTH)
        normed = (delta * lax.rsqrt(var + EPS_LN) * gain).astype(BF16)
        lanes = lane_iota((ROWS, 128))
        tile = jnp.where(lanes == 0, mean, jnp.where(lanes == 1, var, 0.0))
        if ROWS < 128:
            tile = jnp.concatenate([tile] * (128 // ROWS), axis=0)
        return normed, jnp.transpose(tile)[0:8]

    def merge_stats(blocks):
        share = 1.0 / len(blocks)
        mean = sum(m for m, _ in blocks) * share
        var = sum(v + (m - mean) * (m - mean) for m, v in blocks) * share
        return mean, var

    def stat_columns(blocks):
        mean, var = merge_stats(blocks)
        inv = lax.rsqrt(var + EPS_LN)
        lines = [jnp.sqrt(v + EPS_LN) * inv for _, v in blocks] + [(m - mean) * inv for m, _ in blocks]
        sub = lax.broadcasted_iota(jnp.int32, (8, 128), 0)
        tile = jnp.zeros((8, 128), F32)
        for i, line in enumerate(lines):
            tile = jnp.where(sub == i, line, tile)
        turned = jnp.transpose(jnp.concatenate([tile] * 16, axis=0))[0:ROWS]
        return [turned[:, i:i + 1] for i in range(len(lines))]

    def block_stats(index, r):
        tile = st_recv[index, r]
        return tile[0:1], tile[1:2]

    def pack_heads(q, k, v, j, rows):
        half = rows // 2
        lo = (j // 2) * 128
        q, k, v = q[:, lo:lo + 128], k[:, lo:lo + 128], v[:, lo:lo + 128]
        if j % 2 == 0:
            first = jnp.where(low_half((rows, 128)), q, swap_halves(k))
            second = jnp.where(low_half((half, 128)), v[:half], swap_halves(v[half:]))
        else:
            first = jnp.where(low_half((rows, 128)), swap_halves(q), k)
            second = jnp.where(low_half((half, 128)), swap_halves(v[:half]), v[half:])
        return first, second

    def dot(a, b):
        return jnp.dot(a, b, preferred_element_type=F32)

    def send_qkv(layer, stream):
        slot = layer * STREAMS + stream
        need("x")
        need("g1")
        state = x_buf[stream * ROWS:(stream + 1) * ROWS, :].astype(F32)
        normed, tile = local_norm(state, g1[layer:layer + 1, :].astype(F32))
        st_send[2 * slot] = tile
        st_recv[2 * slot, row] = tile
        for name in ("wq", "wk", "wv"):
            need((name, layer))
        q, k, v = dot(normed, wq[layer]), dot(normed, wk[layer]), dot(normed, wv[layer])
        for j in range(N_ROW):
            first, second = pack_heads(q, k, v, j, ROWS)
            qkv_send[slot, j, 0:ROWS] = first.astype(BF16)
            qkv_send[slot, j, ROWS:ROWS + HALF] = second.astype(BF16)
        qkv_recv[slot, row] = qkv_send[slot, row]
        if layer == 0 and stream == 0:
            pl.semaphore_wait(barrier, N_PEER)
        to_axis(("st1", slot), "row", lambda d: st_send.at[2 * slot], st_recv.at[2 * slot])
        to_axis(("qkv", slot), "row", lambda d: qkv_send.at[slot, d], qkv_recv.at[slot])

    def affine_rows(gain, shift):
        sub = lax.broadcasted_iota(jnp.int32, (16, WIDTH), 0)
        return jnp.where(sub == 0, gain.astype(F32), jnp.where(sub == 1, shift.astype(F32), 0.0)).astype(BF16)

    def send_affine(layer, kind):
        bias_on = jnp.where(row == 0, 1.0, 0.0)
        if kind == 0:
            for name in ("b1", "bq", "bk", "bv"):
                need(name)
            rows = affine_rows(g1[layer:layer + 1, :], b1[layer:layer + 1, :])
            parts = []
            for w, b in ((wq, bq), (wk, bk), (wv, bv)):
                bias = b[layer:layer + 1, :].astype(F32) * bias_on
                part = dot(rows, w[layer])[0:8]
                sub_w = lax.broadcasted_iota(jnp.int32, (8, WIDTH), 0)
                parts.append(part + jnp.where(sub_w == 1, bias, 0.0))
            q, k, v = parts
            for j in range(N_ROW):
                lo = (j // 2) * 128
                qj, kj, vj = q[:, lo:lo + 128], k[:, lo:lo + 128], v[:, lo:lo + 128]
                if j % 2 == 0:
                    first = jnp.where(low_half((8, 128)), qj, swap_halves(kj))
                    second = jnp.where(low_half((8, 128)), vj, swap_halves(vj))
                else:
                    first = jnp.where(low_half((8, 128)), swap_halves(qj), kj)
                    second = jnp.where(low_half((8, 128)), swap_halves(vj), vj)
                gq_send[layer, j] = jnp.concatenate([first, second], axis=1)
            gq_recv[layer, row] = gq_send[layer, row]
            to_axis(("gb", layer, kind), "row", lambda d: gq_send.at[layer, d], gq_recv.at[layer])
        else:
            for name in ("g2", "b2", "bf1", ("wf1", layer)):
                need(name)
            rows = affine_rows(g2[layer:layer + 1, :], b2[layer:layer + 1, :])
            part = dot(rows, wf1[layer])[0:8]
            sub_w = lax.broadcasted_iota(jnp.int32, (8, FF_LOC), 0)
            part = part + jnp.where(sub_w == 1, bf1[layer:layer + 1, :].astype(F32) * bias_on, 0.0)
            for j in range(2):
                gf_send[layer, j] = part[:, j * FF_HALF:(j + 1) * FF_HALF]
            gf_recv[layer, row] = gf_send[layer, side]
            to_axis(("gb", layer, kind), "row", lambda d: gf_send.at[layer, lax.rem(d, 2)], gf_recv.at[layer])

    gb_done = set()

    def affine_lines(layer, kind):
        if (layer, kind) not in gb_done:
            gb_done.add((layer, kind))
            arrived(("gb", layer, kind))

    def gain_line(buf, layer, r):
        return buf[layer, r, 0:1]

    def const_line(buf, layer):
        return buf[layer, 0, 1:2] + buf[layer, 1, 1:2] + buf[layer, 2, 1:2] + buf[layer, 3, 1:2]

    def attend(layer, stream):
        slot = layer * STREAMS + stream
        span = slice(stream * ROWS, (stream + 1) * ROWS)
        arrived(("st1", slot))
        cols = stat_columns([block_stats(2 * slot, r) for r in range(N_ROW)])
        affine_lines(layer, 0)
        gains = [gain_line(gq_recv, layer, r) for r in range(N_ROW)]
        const = const_line(gq_recv, layer)
        arrived(("qkv", slot))
        low = low_half((HALF, 128))
        qk = const[:, 0:128]
        vv = const[:, 128:256]
        for r in range(N_ROW):
            part = qkv_recv[slot, r].astype(F32)
            scale, shift = cols[r], cols[4 + r]
            qk = qk + part[0:ROWS] * scale + shift * gains[r][:, 0:128]
            scale_v = jnp.where(low, scale[0:HALF], scale[HALF:ROWS])
            shift_v = jnp.where(low, shift[0:HALF], shift[HALF:ROWS])
            vv = vv + part[ROWS:ROWS + HALF] * scale_v + shift_v * gains[r][:, 128:256]
        full_low = low_half((ROWS, 128))
        qk_turn = swap_halves(qk)
        q2 = (jnp.where(full_low, qk, qk_turn) * (HEAD ** -0.5)).astype(BF16)
        k2 = jnp.where(full_low, qk_turn, qk).astype(BF16)
        vv_turn = swap_halves(vv)
        v2 = jnp.concatenate([jnp.where(low, vv, vv_turn), jnp.where(low, vv_turn, vv)], axis=0).astype(BF16)
        kv_mix[layer, span, :] = jnp.where(full_low, k2.astype(F32), v2.astype(F32))
        score_new = jnp.sum(jnp.where(full_low, q2.astype(F32) * k2.astype(F32), 0.0), axis=-1, keepdims=True)

        need(("kv", layer, stream, 0))
        q_row = lax.broadcasted_iota(jnp.int32, (GROUP, 128), 0)
        q_half = lane_iota((GROUP, 128)) // HEAD
        for g in range(ROWS // GROUP):
            base = (stream * ROWS + g * GROUP) * HEAD
            qg = q2[g * GROUP:(g + 1) * GROUP].astype(F32)
            spread = [jnp.where(q_row == 2 * j + q_half, qg, 0.0).astype(BF16) for j in range(GROUP // 2)]
            s_buf[g * GROUP:(g + 1) * GROUP, :] = dot(jnp.concatenate(spread, axis=1),
                                                      k_buf[layer, base:base + GROUP * HEAD, :])
        positions = lane_iota((ROWS, SEQ)).astype(F32)
        limit = len_mat[span, 0:1]
        scores = jnp.where(positions < limit, s_buf[...], -jnp.inf)
        peak = jnp.maximum(jnp.max(scores, axis=-1, keepdims=True), score_new)
        exp_cache = jnp.exp(scores - peak)
        exp_new = jnp.exp(score_new - peak)
        inv = 1.0 / (jnp.sum(exp_cache, axis=-1, keepdims=True) + exp_new)
        p_buf[...] = (exp_cache * inv).astype(BF16)
        prob_new = (exp_new * inv).astype(BF16).astype(F32)

        need(("kv", layer, stream, 1))
        for g in range(ROWS // GROUP):
            base = (stream * ROWS + g * GROUP) * HEAD
            wide = lax.dot_general(p_buf[g * GROUP:(g + 1) * GROUP, :], v_buf[layer, base:base + GROUP * HEAD, :],
                                   (((1,), (1,)), ((), ())), preferred_element_type=F32)
            acc = jnp.zeros((GROUP, 128), F32)
            for j in range(GROUP // 2):
                acc = acc + jnp.where(q_row == 2 * j + q_half, wide[:, j * 128:(j + 1) * 128], 0.0)
            o_mix[g * GROUP:(g + 1) * GROUP, :] = acc + swap_halves(acc)
        o2 = o_mix[...] + prob_new * v2.astype(F32)
        packed = jnp.where(low, o2[0:HALF], o2[HALF:ROWS]).astype(BF16)
        o_recv[slot, row] = packed
        to_axis(("o", slot), "row", lambda d: o_recv.at[slot, row], o_recv.at[slot])

    def unpack_heads(buf, first):
        low = low_half((HALF, 128))
        parts = [buf[first + r].astype(F32) for r in range(N_ROW)]
        turns = [swap_halves(p) for p in parts]
        pairs = []
        for a, b in ((0, 1), (2, 3)):
            top = jnp.where(low, parts[a], turns[b])
            bottom = jnp.where(low, turns[a], parts[b])
            pairs.append(jnp.concatenate([top, bottom], axis=0).astype(BF16))
        return jnp.concatenate(pairs, axis=1)

    def project(layer, stream):
        slot = layer * STREAMS + stream
        need(("wo", layer))
        arrived(("o", slot))
        proj_recv[slot, col] = dot(unpack_heads(o_recv.at[slot], 0), wo[layer]).astype(BF16)
        to_col(("proj", slot), proj_recv.at[slot])

    def col_sum(buf):
        total = buf[0].astype(F32)
        for c in range(1, N_COL):
            total = total + buf[c].astype(F32)
        return total

    def residual(total, bias, stream):
        span = slice(stream * ROWS, (stream + 1) * ROWS)
        new = (x_buf[span, :].astype(F32) + (total + bias)).astype(BF16)
        x_buf[span, :] = new
        return new.astype(F32)

    def send_inner(layer, stream):
        slot = layer * STREAMS + stream
        need("bo")
        need("g2")
        need(("wf1", layer))
        arrived(("proj", slot))
        total = col_sum(proj_recv.at[slot])
        state = residual(total, bo[layer:layer + 1, :].astype(F32), stream)
        normed, tile = local_norm(state, g2[layer:layer + 1, :].astype(F32))
        index = 2 * slot + 1
        st_send[index] = tile
        st_recv[index, row] = tile
        mine = st_send.at[index]
        spot = st_recv.at[index, row]
        exchange(("st2", slot), [(mine, spot, {"row": partner})], mine)
        far = lax.rem(partner + 2, N_ROW)
        exchange(("st3", slot), [(mine, spot, {"row": across}), (mine, spot, {"row": far})], st_recv.at[index, 0:2])
        theirs = pl.ds(pl.multiple_of((1 - side) * FF_HALF, FF_HALF), FF_HALF)
        f1_send[slot] = dot(normed, wf1[layer, :, theirs]).astype(BF16)
        exchange(("f1", slot), [(f1_send.at[slot], f1_recv.at[slot], {"row": partner})], f1_recv.at[slot])
        ours = pl.ds(pl.multiple_of(side * FF_HALF, FF_HALF), FF_HALF)
        f1_mine[stream] = dot(normed, wf1[layer, :, ours])

    def send_pair(layer, stream):
        slot = layer * STREAMS + stream
        arrived(("st2", slot))
        cols = stat_columns([block_stats(2 * slot + 1, r) for r in (row, partner)])
        affine_lines(layer, 1)
        arrived(("f1", slot))
        total = f1_mine[stream] * cols[0] + cols[2] * gain_line(gf_recv, layer, row)
        total = total + f1_recv[slot].astype(F32) * cols[1] + cols[3] * gain_line(gf_recv, layer, partner)
        pair_recv[slot, chip] = total.astype(BF16)
        mine = pair_recv.at[slot, chip]
        exchange(("pair", slot), [(mine, mine, {"row": across})], mine)

    def send_act(layer, stream):
        slot = layer * STREAMS + stream
        arrived(("st3", slot))
        pairs = [merge_stats([block_stats(2 * slot + 1, 2 * k + r) for r in range(2)]) for k in range(2)]
        cols = stat_columns(pairs)
        total = const_line(gf_recv, layer)
        arrived(("pair", slot))
        for k in range(2):
            gain = gain_line(gf_recv, layer, 2 * k) + gain_line(gf_recv, layer, 2 * k + 1)
            total = total + pair_recv[slot, k].astype(F32) * cols[k] + cols[2 + k] * gain
        u_recv[slot, side] = jnp.maximum(total, 0.0).astype(BF16)
        mine = u_recv.at[slot, side]
        exchange(("u", slot), [(mine, mine, {"row": partner})], mine)

    def send_out(layer, stream):
        slot = layer * STREAMS + stream
        need(("wf2", layer))
        arrived(("u", slot))
        acc = dot(u_recv[slot, 0], wf2[layer, 0:FF_HALF, :]) + dot(u_recv[slot, 1], wf2[layer, FF_HALF:, :])
        out_recv[slot, col] = acc.astype(BF16)
        to_col(("out", slot), out_recv.at[slot])

    def finish(layer, stream):
        slot = layer * STREAMS + stream
        need("bf2")
        arrived(("out", slot))
        residual(col_sum(out_recv.at[slot]), bf2[layer:layer + 1, :].astype(F32), stream)

    stores = []

    def store(src, dst, index):
        copy = pltpu.make_async_copy(src, dst, store_sem.at[index])
        copy.start()
        stores.append(copy)

    for stream in range(STREAMS):
        send_qkv(0, stream)
    send_affine(0, 0)
    need("len")
    len_mat[...] = jnp.transpose(jnp.broadcast_to(len_buf[...].astype(F32), (128, 128)))
    for layer in range(LAYERS):
        for stream in range(STREAMS):
            attend(layer, stream)
        kv_turn[layer] = jnp.transpose(kv_mix[layer]).astype(BF16)
        store(kv_turn.at[layer, 0:HEAD], k_out.at[layer], 2 * layer)
        store(kv_turn.at[layer, HEAD:2 * HEAD], v_out.at[layer], 2 * layer + 1)
        if layer == 0:
            send_affine(0, 1)
        for stream in range(STREAMS):
            project(layer, stream)
        if layer == 0:
            for name in MAT_NAMES[:3]:
                need((name, 1))
            send_affine(1, 0)
            send_affine(1, 1)
        for stream in range(STREAMS):
            send_inner(layer, stream)
        for stream in range(STREAMS):
            send_pair(layer, stream)
        for stream in range(STREAMS):
            send_act(layer, stream)
        for stream in range(STREAMS):
            send_out(layer, stream)
        for stream in range(STREAMS):
            finish(layer, stream)
            if layer + 1 < LAYERS:
                send_qkv(layer + 1, stream)
            else:
                span = pl.ds(stream * ROWS, ROWS)
                store(x_buf.at[span], h_out.at[span], 2 * LAYERS + stream)
    for copy in stores:
        copy.wait()
    for copy in drains:
        copy.wait()


N_SLOT = LAYERS * STREAMS
N_COPY = 10 * N_SLOT + 2 * LAYERS
N_PEER = N_ROW + N_COL - 2


def emit_kernel(h_in, k_in, v_in, h_out, k_out, v_out, h_buf, k_buf, v_buf, sem):
    moves = ((h_in, h_buf, h_out), (k_in, k_buf, k_out), (v_in, v_buf, v_out))
    loads = [pltpu.make_async_copy(src, buf, sem.at[i]) for i, (src, buf, _) in enumerate(moves)]
    for copy in loads:
        copy.start()
    stores = []
    for i, (_, buf, dst) in enumerate(moves):
        loads[i].wait()
        copy = pltpu.make_async_copy(buf, dst, sem.at[i])
        copy.start()
        stores.append(copy)
    for copy in stores:
        copy.wait()


def run_step(x, lens, k_cache, v_cache, g1, b1, wq, bq, wk, bk, wv, bv, wo, bo, g2, b2, wf1, bf1, wf2, bf2):
    any_spec = pl.BlockSpec(memory_space=pl.ANY)
    args = (x, lens.reshape(1, BATCH),
            jnp.swapaxes(k_cache, 3, 4).reshape(LAYERS, BATCH * HEAD, SEQ),
            jnp.swapaxes(v_cache, 3, 4).reshape(LAYERS, BATCH * HEAD, SEQ),
            g1, b1, wq, bq, wk, bk, wv, bv, wo, bo, g2, b2, wf1, bf1, wf2, bf2)
    vm = pltpu.VMEM
    in_scratch = [vm(a.shape, a.dtype) for a in args]
    scratch = in_scratch + [
        vm((BATCH, 128), F32),
        vm((LAYERS, BATCH, 128), F32),
        vm((LAYERS, BATCH, 128), BF16),
        vm((ROWS, SEQ), F32),
        vm((ROWS, SEQ), BF16),
        vm((ROWS, 128), F32),
        vm((2 * N_SLOT, 8, 128), F32),
        vm((2 * N_SLOT, N_ROW, 8, 128), F32),
        vm((LAYERS, N_ROW, 8, WIDTH), F32),
        vm((LAYERS, N_ROW, 8, WIDTH), F32),
        vm((LAYERS, 2, 8, FF_HALF), F32),
        vm((LAYERS, N_ROW, 8, FF_HALF), F32),
        vm((N_SLOT, N_ROW, ROWS + HALF, 128), BF16),
        vm((N_SLOT, N_ROW, ROWS + HALF, 128), BF16),
        vm((N_SLOT, N_ROW, HALF, 128), BF16),
        vm((N_SLOT, N_COL, ROWS, WIDTH), BF16),
        vm((STREAMS, ROWS, FF_HALF), F32),
        vm((N_SLOT, ROWS, FF_HALF), BF16),
        vm((N_SLOT, ROWS, FF_HALF), BF16),
        vm((N_SLOT, 2, ROWS, FF_HALF), BF16),
        vm((N_SLOT, 2, ROWS, FF_HALF), BF16),
        vm((N_SLOT, N_COL, ROWS, WIDTH), BF16),
        pltpu.SemaphoreType.DMA((32,)),
        pltpu.SemaphoreType.DMA((2 * N_SLOT,)),
        pltpu.SemaphoreType.DMA((2 * LAYERS + STREAMS,)),
        pltpu.SemaphoreType.DMA((N_COPY,)),
        pltpu.SemaphoreType.DMA((N_COPY,)),
    ]
    shapes = (jax.ShapeDtypeStruct((BATCH, WIDTH), BF16),
              jax.ShapeDtypeStruct((LAYERS, HEAD, BATCH), BF16),
              jax.ShapeDtypeStruct((LAYERS, HEAD, BATCH), BF16))
    results = pl.pallas_call(
        step_kernel,
        out_shape=shapes,
        in_specs=[pl.BlockSpec(memory_space=pltpu.HBM)] * len(args),
        out_specs=(any_spec,) * 3,
        scratch_shapes=scratch,
        compiler_params=pltpu.CompilerParams(
            collective_id=0, has_side_effects=True, vmem_limit_bytes=60 * 1024 * 1024),
        name="decode_step",
    )(*args)
    h_out, k_new, v_new = pl.pallas_call(
        emit_kernel,
        out_shape=shapes,
        in_specs=[any_spec] * 3,
        out_specs=(pl.BlockSpec(memory_space=pltpu.HBM),) * 3,
        scratch_shapes=[vm(a.shape, a.dtype) for a in shapes] + [pltpu.SemaphoreType.DMA((3,))],
        compiler_params=pltpu.CompilerParams(vmem_limit_bytes=60 * 1024 * 1024),
        name="emit",
    )(*results)

    def fresh(rows):
        return jnp.swapaxes(rows, 1, 2).reshape(LAYERS, BATCH, 1, HEAD)

    return h_out, fresh(k_new), fresh(v_new)


def solution(mesh):
    act_spec = P("dp", "row")
    cache_spec = P(None, "dp", ("col", "row"), None, None)
    fresh_spec = P(None, "dp", ("col", "row"), None)
    in_weight = P(None, "row", "col")
    out_weight = P(None, "col", "row")
    col_vec = P(None, "col")
    row_vec = P(None, "row")
    in_specs = (act_spec, P("dp"), cache_spec, cache_spec, row_vec, row_vec,
                in_weight, col_vec, in_weight, col_vec, in_weight, col_vec,
                out_weight, row_vec, row_vec, row_vec, in_weight, col_vec, out_weight, row_vec)
    return jax.shard_map(run_step, mesh=mesh, in_specs=in_specs,
                         out_specs=(act_spec, fresh_spec, fresh_spec), check_vma=False)
```

```python
import functools

import jax
import jax.numpy as jnp
from jax import lax
from jax.experimental import pallas as pl
from jax.experimental.pallas import tpu as pltpu
from jax.sharding import PartitionSpec as P

EPS_LN = 1e-5
MESH = pl.DeviceIdType.MESH
F32 = jnp.float32
BF16 = jnp.bfloat16

LAYERS = 2
BATCH = 128
STREAMS = 2
ROWS = BATCH // STREAMS
HALF = ROWS // 2
GROUP = 16
COL_PIECES = 2
N_ROW = 4
N_COL = 4
HEAD = 64
SEQ = 512
WIDTH = 256
D_MODEL = 1024
FF_LOC = 1024
FF_HALF = FF_LOC // 2

VEC_NAMES = ("g1", "b1", "bq", "bk", "bv", "bo", "g2", "b2", "bf2")
MAT_NAMES = ("wq", "wk", "wv", "wo", "wf1", "wf2")


def lane_iota(shape):
    return lax.broadcasted_iota(jnp.int32, shape, len(shape) - 1)


def swap_halves(val):
    return pltpu.roll(val, HEAD, 1)


def low_half(shape):
    return lane_iota(shape) < HEAD


def step_kernel(*refs):
    (x_in, len_in, k_in, v_in, g1_in, b1_in, wq_in, bq_in, wk_in, bk_in, wv_in, bv_in,
     wo_in, bo_in, g2_in, b2_in, wf1_in, bf1_in, wf2_in, bf2_in,
     h_out, k_out, v_out,
     x_buf, len_buf, k_buf, v_buf, g1, b1, wq, bq, wk, bk, wv, bv, wo, bo, g2, b2, wf1, bf1, wf2, bf2,
     len_mat, kv_mix, kv_turn, s_buf, p_buf, o_mix,
     st_send, st_recv, gq_send, gq_recv, gf_send, gf_recv, qkv_send, qkv_recv, o_recv,
     proj_recv, f1_mine, f1_send, f1_recv, pair_recv, u_recv, out_recv,
     load_sem, big_sem, store_sem, send_sem, recv_sem) = refs

    row = lax.axis_index("row")
    col = lax.axis_index("col")
    side = lax.rem(row, 2)
    chip = row // 2
    partner = chip * 2 + (1 - side)
    across = lax.rem(row + 2, N_ROW)

    loads = {}

    def load(name, src, dst, sem):
        copy = pltpu.make_async_copy(src, dst, sem)
        copy.start()
        loads[name] = copy

    n_load = [0]

    def small(name, src, dst):
        load(name, src, dst, load_sem.at[n_load[0]])
        n_load[0] += 1

    small("x", x_in, x_buf)
    small("g1", g1_in, g1)
    for layer in range(LAYERS):
        for name, src, dst in (("wq", wq_in, wq), ("wk", wk_in, wk), ("wv", wv_in, wv)):
            if layer == 0:
                small((name, layer), src.at[layer], dst.at[layer])
    for name, src, dst in (("b1", b1_in, b1), ("bq", bq_in, bq), ("bk", bk_in, bk), ("bv", bv_in, bv),
                           ("len", len_in, len_buf), ("bo", bo_in, bo), ("g2", g2_in, g2), ("b2", b2_in, b2),
                           ("bf1", bf1_in, bf1), ("bf2", bf2_in, bf2)):
        small(name, src, dst)

    barrier = pltpu.get_barrier_semaphore()
    for off in range(1, 4):
        pl.semaphore_signal(barrier, inc=1, device_id={"row": lax.rem(row + off, N_ROW)}, device_id_type=MESH)
        pl.semaphore_signal(barrier, inc=1, device_id={"col": lax.rem(col + off, N_COL)}, device_id_type=MESH)

    def big(layer, stream, which):
        src, dst = (k_in, k_buf) if which == 0 else (v_in, v_buf)
        span = pl.ds(stream * ROWS * HEAD, ROWS * HEAD)
        load(("kv", layer, stream, which), src.at[layer, span], dst.at[layer, span],
             big_sem.at[(layer * STREAMS + stream) * 2 + which])

    def late_loads(layer):
        for stream in range(STREAMS):
            for which in range(2):
                big(layer, stream, which)
        names = (("wo", wo_in, wo), ("wf1", wf1_in, wf1), ("wf2", wf2_in, wf2))
        if layer:
            names += (("wq", wq_in, wq), ("wk", wk_in, wk), ("wv", wv_in, wv))
        for name, src, dst in names:
            small((name, layer), src.at[layer], dst.at[layer])

    waited = set()

    def need(name):
        if name not in waited:
            waited.add(name)
            loads[name].wait()

    drains = []
    recvs = {}
    n_sem = [0]

    def exchange(tag, copies, span):
        index = n_sem[0]
        n_sem[0] += 1
        for src, dst, device in copies:
            pltpu.make_async_remote_copy(
                src_ref=src, dst_ref=dst, send_sem=send_sem.at[index],
                recv_sem=recv_sem.at[index], device_id=device, device_id_type=MESH).start()
        drains.append(pltpu.make_async_copy(span, span, send_sem.at[index]))
        recvs[tag] = pltpu.make_async_copy(span, span, recv_sem.at[index])

    def to_col(tag, buf):
        peers = [lax.rem(col + off, N_COL) for off in (2, 3, 1)]
        rows = ROWS // COL_PIECES
        copies = []
        for piece in range(COL_PIECES):
            mine = buf.at[col, piece * rows:(piece + 1) * rows]
            copies += [(mine, mine, {"col": peer}) for peer in peers]
        exchange(tag, copies, buf.at[0:3])

    def to_axis(tag, axis, src_of, buf):
        me = row if axis == "row" else col
        dests = [lax.rem(me + off, 4) for off in (2, 3, 1)]
        exchange(tag, [(src_of(d), buf.at[me], {axis: d}) for d in dests], buf.at[0:3])

    def arrived(tag):
        recvs[tag].wait()

    def local_norm(state, gain):
        mean = jnp.sum(state, axis=-1, keepdims=True) * (1.0 / WIDTH)
        delta = state - mean
        var = jnp.sum(delta * delta, axis=-1, keepdims=True) * (1.0 / WIDTH)
        normed = (delta * lax.rsqrt(var + EPS_LN) * gain).astype(BF16)
        lanes = lane_iota((ROWS, 128))
        tile = jnp.where(lanes == 0, mean, jnp.where(lanes == 1, var, 0.0))
        if ROWS < 128:
            tile = jnp.concatenate([tile] * (128 // ROWS), axis=0)
        return normed, jnp.transpose(tile)[0:8]

    def merge_stats(blocks):
        share = 1.0 / len(blocks)
        mean = sum(m for m, _ in blocks) * share
        var = sum(v + (m - mean) * (m - mean) for m, v in blocks) * share
        return mean, var

    def stat_columns(blocks):
        mean, var = merge_stats(blocks)
        inv = lax.rsqrt(var + EPS_LN)
        lines = [jnp.sqrt(v + EPS_LN) * inv for _, v in blocks] + [(m - mean) * inv for m, _ in blocks]
        sub = lax.broadcasted_iota(jnp.int32, (8, 128), 0)
        tile = jnp.zeros((8, 128), F32)
        for i, line in enumerate(lines):
            tile = jnp.where(sub == i, line, tile)
        turned = jnp.transpose(jnp.concatenate([tile] * 16, axis=0))[0:ROWS]
        return [turned[:, i:i + 1] for i in range(len(lines))]

    def block_stats(index, r):
        tile = st_recv[index, r]
        return tile[0:1], tile[1:2]

    def pack_heads(q, k, v, j, rows):
        half = rows // 2
        lo = (j // 2) * 128
        q, k, v = q[:, lo:lo + 128], k[:, lo:lo + 128], v[:, lo:lo + 128]
        if j % 2 == 0:
            first = jnp.where(low_half((rows, 128)), q, swap_halves(k))
            second = jnp.where(low_half((half, 128)), v[:half], swap_halves(v[half:]))
        else:
            first = jnp.where(low_half((rows, 128)), swap_halves(q), k)
            second = jnp.where(low_half((half, 128)), swap_halves(v[:half]), v[half:])
        return first, second

    def dot(a, b):
        return jnp.dot(a, b, preferred_element_type=F32)

    def send_qkv(layer, stream):
        slot = layer * STREAMS + stream
        need("x")
        need("g1")
        state = x_buf[stream * ROWS:(stream + 1) * ROWS, :].astype(F32)
        normed, tile = local_norm(state, g1[layer:layer + 1, :].astype(F32))
        st_send[2 * slot] = tile
        st_recv[2 * slot, row] = tile
        for name in ("wq", "wk", "wv"):
            need((name, layer))
        q, k, v = dot(normed, wq[layer]), dot(normed, wk[layer]), dot(normed, wv[layer])
        for j in range(N_ROW):
            first, second = pack_heads(q, k, v, j, ROWS)
            qkv_send[slot, j, 0:ROWS] = first.astype(BF16)
            qkv_send[slot, j, ROWS:ROWS + HALF] = second.astype(BF16)
        qkv_recv[slot, row] = qkv_send[slot, row]
        if layer == 0 and stream == 0:
            pl.semaphore_wait(barrier, N_PEER)
        to_axis(("st1", slot), "row", lambda d: st_send.at[2 * slot], st_recv.at[2 * slot])
        to_axis(("qkv", slot), "row", lambda d: qkv_send.at[slot, d], qkv_recv.at[slot])

    def affine_rows(gain, shift):
        sub = lax.broadcasted_iota(jnp.int32, (16, WIDTH), 0)
        return jnp.where(sub == 0, gain.astype(F32), jnp.where(sub == 1, shift.astype(F32), 0.0)).astype(BF16)

    def send_affine(layer, kind):
        bias_on = jnp.where(row == 0, 1.0, 0.0)
        if kind == 0:
            for name in ("b1", "bq", "bk", "bv"):
                need(name)
            rows = affine_rows(g1[layer:layer + 1, :], b1[layer:layer + 1, :])
            parts = []
            for w, b in ((wq, bq), (wk, bk), (wv, bv)):
                bias = b[layer:layer + 1, :].astype(F32) * bias_on
                part = dot(rows, w[layer])[0:8]
                sub_w = lax.broadcasted_iota(jnp.int32, (8, WIDTH), 0)
                parts.append(part + jnp.where(sub_w == 1, bias, 0.0))
            q, k, v = parts
            for j in range(N_ROW):
                lo = (j // 2) * 128
                qj, kj, vj = q[:, lo:lo + 128], k[:, lo:lo + 128], v[:, lo:lo + 128]
                if j % 2 == 0:
                    first = jnp.where(low_half((8, 128)), qj, swap_halves(kj))
                    second = jnp.where(low_half((8, 128)), vj, swap_halves(vj))
                else:
                    first = jnp.where(low_half((8, 128)), swap_halves(qj), kj)
                    second = jnp.where(low_half((8, 128)), swap_halves(vj), vj)
                gq_send[layer, j] = jnp.concatenate([first, second], axis=1)
            gq_recv[layer, row] = gq_send[layer, row]
            to_axis(("gb", layer, kind), "row", lambda d: gq_send.at[layer, d], gq_recv.at[layer])
        else:
            for name in ("g2", "b2", "bf1", ("wf1", layer)):
                need(name)
            rows = affine_rows(g2[layer:layer + 1, :], b2[layer:layer + 1, :])
            part = dot(rows, wf1[layer])[0:8]
            sub_w = lax.broadcasted_iota(jnp.int32, (8, FF_LOC), 0)
            part = part + jnp.where(sub_w == 1, bf1[layer:layer + 1, :].astype(F32) * bias_on, 0.0)
            for j in range(2):
                gf_send[layer, j] = part[:, j * FF_HALF:(j + 1) * FF_HALF]
            gf_recv[layer, row] = gf_send[layer, side]
            to_axis(("gb", layer, kind), "row", lambda d: gf_send.at[layer, lax.rem(d, 2)], gf_recv.at[layer])

    gb_done = set()

    def affine_lines(layer, kind):
        if (layer, kind) not in gb_done:
            gb_done.add((layer, kind))
            arrived(("gb", layer, kind))

    def gain_line(buf, layer, r):
        return buf[layer, r, 0:1]

    def const_line(buf, layer):
        return buf[layer, 0, 1:2] + buf[layer, 1, 1:2] + buf[layer, 2, 1:2] + buf[layer, 3, 1:2]

    def attend(layer, stream):
        slot = layer * STREAMS + stream
        span = slice(stream * ROWS, (stream + 1) * ROWS)
        arrived(("st1", slot))
        cols = stat_columns([block_stats(2 * slot, r) for r in range(N_ROW)])
        affine_lines(layer, 0)
        gains = [gain_line(gq_recv, layer, r) for r in range(N_ROW)]
        const = const_line(gq_recv, layer)
        arrived(("qkv", slot))
        low = low_half((HALF, 128))
        qk = const[:, 0:128]
        vv = const[:, 128:256]
        for r in range(N_ROW):
            part = qkv_recv[slot, r].astype(F32)
            scale, shift = cols[r], cols[4 + r]
            qk = qk + part[0:ROWS] * scale + shift * gains[r][:, 0:128]
            scale_v = jnp.where(low, scale[0:HALF], scale[HALF:ROWS])
            shift_v = jnp.where(low, shift[0:HALF], shift[HALF:ROWS])
            vv = vv + part[ROWS:ROWS + HALF] * scale_v + shift_v * gains[r][:, 128:256]
        full_low = low_half((ROWS, 128))
        qk_turn = swap_halves(qk)
        q2 = (jnp.where(full_low, qk, qk_turn) * (HEAD ** -0.5)).astype(BF16)
        k2 = jnp.where(full_low, qk_turn, qk).astype(BF16)
        vv_turn = swap_halves(vv)
        v2 = jnp.concatenate([jnp.where(low, vv, vv_turn), jnp.where(low, vv_turn, vv)], axis=0).astype(BF16)
        kv_mix[layer, span, :] = jnp.where(full_low, k2.astype(F32), v2.astype(F32))
        score_new = jnp.sum(jnp.where(full_low, q2.astype(F32) * k2.astype(F32), 0.0), axis=-1, keepdims=True)

        need(("kv", layer, stream, 0))
        q_row = lax.broadcasted_iota(jnp.int32, (GROUP, 128), 0)
        q_half = lane_iota((GROUP, 128)) // HEAD
        for g in range(ROWS // GROUP):
            base = (stream * ROWS + g * GROUP) * HEAD
            qg = q2[g * GROUP:(g + 1) * GROUP].astype(F32)
            spread = [jnp.where(q_row == 2 * j + q_half, qg, 0.0).astype(BF16) for j in range(GROUP // 2)]
            s_buf[g * GROUP:(g + 1) * GROUP, :] = dot(jnp.concatenate(spread, axis=1),
                                                      k_buf[layer, base:base + GROUP * HEAD, :])
        positions = lane_iota((ROWS, SEQ)).astype(F32)
        limit = len_mat[span, 0:1]
        scores = jnp.where(positions < limit, s_buf[...], -jnp.inf)
        peak = jnp.maximum(jnp.max(scores, axis=-1, keepdims=True), score_new)
        exp_cache = jnp.exp(scores - peak)
        exp_new = jnp.exp(score_new - peak)
        inv = 1.0 / (jnp.sum(exp_cache, axis=-1, keepdims=True) + exp_new)
        p_buf[...] = (exp_cache * inv).astype(BF16)
        prob_new = (exp_new * inv).astype(BF16).astype(F32)

        need(("kv", layer, stream, 1))
        for g in range(ROWS // GROUP):
            base = (stream * ROWS + g * GROUP) * HEAD
            wide = lax.dot_general(p_buf[g * GROUP:(g + 1) * GROUP, :], v_buf[layer, base:base + GROUP * HEAD, :],
                                   (((1,), (1,)), ((), ())), preferred_element_type=F32)
            acc = jnp.zeros((GROUP, 128), F32)
            for j in range(GROUP // 2):
                acc = acc + jnp.where(q_row == 2 * j + q_half, wide[:, j * 128:(j + 1) * 128], 0.0)
            o_mix[g * GROUP:(g + 1) * GROUP, :] = acc + swap_halves(acc)
        o2 = o_mix[...] + prob_new * v2.astype(F32)
        packed = jnp.where(low, o2[0:HALF], o2[HALF:ROWS]).astype(BF16)
        o_recv[slot, row] = packed
        to_axis(("o", slot), "row", lambda d: o_recv.at[slot, row], o_recv.at[slot])

    def unpack_heads(buf, first):
        low = low_half((HALF, 128))
        parts = [buf[first + r].astype(F32) for r in range(N_ROW)]
        turns = [swap_halves(p) for p in parts]
        pairs = []
        for a, b in ((0, 1), (2, 3)):
            top = jnp.where(low, parts[a], turns[b])
            bottom = jnp.where(low, turns[a], parts[b])
            pairs.append(jnp.concatenate([top, bottom], axis=0).astype(BF16))
        return jnp.concatenate(pairs, axis=1)

    def project(layer, stream):
        slot = layer * STREAMS + stream
        need(("wo", layer))
        arrived(("o", slot))
        proj_recv[slot, col] = dot(unpack_heads(o_recv.at[slot], 0), wo[layer]).astype(BF16)
        to_col(("proj", slot), proj_recv.at[slot])

    def col_sum(buf):
        total = buf[0].astype(F32)
        for c in range(1, N_COL):
            total = total + buf[c].astype(F32)
        return total

    def residual(total, bias, stream):
        span = slice(stream * ROWS, (stream + 1) * ROWS)
        new = (x_buf[span, :].astype(F32) + (total + bias)).astype(BF16)
        x_buf[span, :] = new
        return new.astype(F32)

    def send_inner(layer, stream):
        slot = layer * STREAMS + stream
        need("bo")
        need("g2")
        need(("wf1", layer))
        arrived(("proj", slot))
        total = col_sum(proj_recv.at[slot])
        state = residual(total, bo[layer:layer + 1, :].astype(F32), stream)
        normed, tile = local_norm(state, g2[layer:layer + 1, :].astype(F32))
        index = 2 * slot + 1
        st_send[index] = tile
        st_recv[index, row] = tile
        mine = st_send.at[index]
        spot = st_recv.at[index, row]
        exchange(("st2", slot), [(mine, spot, {"row": partner})], mine)
        far = lax.rem(partner + 2, N_ROW)
        exchange(("st3", slot), [(mine, spot, {"row": across}), (mine, spot, {"row": far})], st_recv.at[index, 0:2])
        theirs = pl.ds(pl.multiple_of((1 - side) * FF_HALF, FF_HALF), FF_HALF)
        f1_send[slot] = dot(normed, wf1[layer, :, theirs]).astype(BF16)
        exchange(("f1", slot), [(f1_send.at[slot], f1_recv.at[slot], {"row": partner})], f1_recv.at[slot])
        ours = pl.ds(pl.multiple_of(side * FF_HALF, FF_HALF), FF_HALF)
        f1_mine[stream] = dot(normed, wf1[layer, :, ours])

    def send_pair(layer, stream):
        slot = layer * STREAMS + stream
        arrived(("st2", slot))
        cols = stat_columns([block_stats(2 * slot + 1, r) for r in (row, partner)])
        affine_lines(layer, 1)
        arrived(("f1", slot))
        total = f1_mine[stream] * cols[0] + cols[2] * gain_line(gf_recv, layer, row)
        total = total + f1_recv[slot].astype(F32) * cols[1] + cols[3] * gain_line(gf_recv, layer, partner)
        pair_recv[slot, chip] = total.astype(BF16)
        mine = pair_recv.at[slot, chip]
        exchange(("pair", slot), [(mine, mine, {"row": across})], mine)

    def send_act(layer, stream):
        slot = layer * STREAMS + stream
        arrived(("st3", slot))
        pairs = [merge_stats([block_stats(2 * slot + 1, 2 * k + r) for r in range(2)]) for k in range(2)]
        cols = stat_columns(pairs)
        total = const_line(gf_recv, layer)
        arrived(("pair", slot))
        for k in range(2):
            gain = gain_line(gf_recv, layer, 2 * k) + gain_line(gf_recv, layer, 2 * k + 1)
            total = total + pair_recv[slot, k].astype(F32) * cols[k] + cols[2 + k] * gain
        u_recv[slot, side] = jnp.maximum(total, 0.0).astype(BF16)
        mine = u_recv.at[slot, side]
        exchange(("u", slot), [(mine, mine, {"row": partner})], mine)

    def send_out(layer, stream):
        slot = layer * STREAMS + stream
        need(("wf2", layer))
        arrived(("u", slot))
        acc = dot(u_recv[slot, 0], wf2[layer, 0:FF_HALF, :]) + dot(u_recv[slot, 1], wf2[layer, FF_HALF:, :])
        out_recv[slot, col] = acc.astype(BF16)
        to_col(("out", slot), out_recv.at[slot])

    def finish(layer, stream):
        slot = layer * STREAMS + stream
        need("bf2")
        arrived(("out", slot))
        residual(col_sum(out_recv.at[slot]), bf2[layer:layer + 1, :].astype(F32), stream)

    stores = []

    def store(src, dst, index):
        copy = pltpu.make_async_copy(src, dst, store_sem.at[index])
        copy.start()
        stores.append(copy)

    for stream in range(STREAMS):
        send_qkv(0, stream)
    send_affine(0, 0)
    late_loads(0)
    need("len")
    len_mat[...] = jnp.transpose(jnp.broadcast_to(len_buf[...].astype(F32), (128, 128)))
    for layer in range(LAYERS):
        for stream in range(STREAMS):
            attend(layer, stream)
        kv_turn[layer] = jnp.transpose(kv_mix[layer]).astype(BF16)
        store(kv_turn.at[layer, 0:HEAD], k_out.at[layer], 2 * layer)
        store(kv_turn.at[layer, HEAD:2 * HEAD], v_out.at[layer], 2 * layer + 1)
        if layer == 0:
            send_affine(0, 1)
        for stream in range(STREAMS):
            project(layer, stream)
        if layer == 0:
            late_loads(1)
        for stream in range(STREAMS):
            send_inner(layer, stream)
        for stream in range(STREAMS):
            send_pair(layer, stream)
        if layer == 0:
            for name in MAT_NAMES[:3]:
                need((name, 1))
            send_affine(1, 0)
            send_affine(1, 1)
        for stream in range(STREAMS):
            send_act(layer, stream)
        for stream in range(STREAMS):
            send_out(layer, stream)
        for stream in range(STREAMS):
            finish(layer, stream)
            if layer + 1 < LAYERS:
                send_qkv(layer + 1, stream)
            else:
                span = pl.ds(stream * ROWS, ROWS)
                store(x_buf.at[span], h_out.at[span], 2 * LAYERS + stream)
    for copy in stores:
        copy.wait()
    for copy in drains:
        copy.wait()


N_SLOT = LAYERS * STREAMS
N_COPY = 10 * N_SLOT + 2 * LAYERS
N_PEER = N_ROW + N_COL - 2


def emit_kernel(h_in, k_in, v_in, h_out, k_out, v_out, h_buf, k_buf, v_buf, sem):
    moves = ((h_in, h_buf, h_out), (k_in, k_buf, k_out), (v_in, v_buf, v_out))
    loads = [pltpu.make_async_copy(src, buf, sem.at[i]) for i, (src, buf, _) in enumerate(moves)]
    for copy in loads:
        copy.start()
    stores = []
    for i, (_, buf, dst) in enumerate(moves):
        loads[i].wait()
        copy = pltpu.make_async_copy(buf, dst, sem.at[i])
        copy.start()
        stores.append(copy)
    for copy in stores:
        copy.wait()


def run_step(x, lens, k_cache, v_cache, g1, b1, wq, bq, wk, bk, wv, bv, wo, bo, g2, b2, wf1, bf1, wf2, bf2):
    any_spec = pl.BlockSpec(memory_space=pl.ANY)
    args = (x, lens.reshape(1, BATCH),
            jnp.swapaxes(k_cache, 3, 4).reshape(LAYERS, BATCH * HEAD, SEQ),
            jnp.swapaxes(v_cache, 3, 4).reshape(LAYERS, BATCH * HEAD, SEQ),
            g1, b1, wq, bq, wk, bk, wv, bv, wo, bo, g2, b2, wf1, bf1, wf2, bf2)
    vm = pltpu.VMEM
    in_scratch = [vm(a.shape, a.dtype) for a in args]
    scratch = in_scratch + [
        vm((BATCH, 128), F32),
        vm((LAYERS, BATCH, 128), F32),
        vm((LAYERS, BATCH, 128), BF16),
        vm((ROWS, SEQ), F32),
        vm((ROWS, SEQ), BF16),
        vm((ROWS, 128), F32),
        vm((2 * N_SLOT, 8, 128), F32),
        vm((2 * N_SLOT, N_ROW, 8, 128), F32),
        vm((LAYERS, N_ROW, 8, WIDTH), F32),
        vm((LAYERS, N_ROW, 8, WIDTH), F32),
        vm((LAYERS, 2, 8, FF_HALF), F32),
        vm((LAYERS, N_ROW, 8, FF_HALF), F32),
        vm((N_SLOT, N_ROW, ROWS + HALF, 128), BF16),
        vm((N_SLOT, N_ROW, ROWS + HALF, 128), BF16),
        vm((N_SLOT, N_ROW, HALF, 128), BF16),
        vm((N_SLOT, N_COL, ROWS, WIDTH), BF16),
        vm((STREAMS, ROWS, FF_HALF), F32),
        vm((N_SLOT, ROWS, FF_HALF), BF16),
        vm((N_SLOT, ROWS, FF_HALF), BF16),
        vm((N_SLOT, 2, ROWS, FF_HALF), BF16),
        vm((N_SLOT, 2, ROWS, FF_HALF), BF16),
        vm((N_SLOT, N_COL, ROWS, WIDTH), BF16),
        pltpu.SemaphoreType.DMA((32,)),
        pltpu.SemaphoreType.DMA((2 * N_SLOT,)),
        pltpu.SemaphoreType.DMA((2 * LAYERS + STREAMS,)),
        pltpu.SemaphoreType.DMA((N_COPY,)),
        pltpu.SemaphoreType.DMA((N_COPY,)),
    ]
    shapes = (jax.ShapeDtypeStruct((BATCH, WIDTH), BF16),
              jax.ShapeDtypeStruct((LAYERS, HEAD, BATCH), BF16),
              jax.ShapeDtypeStruct((LAYERS, HEAD, BATCH), BF16))
    results = pl.pallas_call(
        step_kernel,
        out_shape=shapes,
        in_specs=[pl.BlockSpec(memory_space=pltpu.HBM)] * len(args),
        out_specs=(any_spec,) * 3,
        scratch_shapes=scratch,
        compiler_params=pltpu.CompilerParams(
            collective_id=0, has_side_effects=True, vmem_limit_bytes=60 * 1024 * 1024),
        name="decode_step",
    )(*args)
    h_out, k_new, v_new = pl.pallas_call(
        emit_kernel,
        out_shape=shapes,
        in_specs=[any_spec] * 3,
        out_specs=(pl.BlockSpec(memory_space=pltpu.HBM),) * 3,
        scratch_shapes=[vm(a.shape, a.dtype) for a in shapes] + [pltpu.SemaphoreType.DMA((3,))],
        compiler_params=pltpu.CompilerParams(vmem_limit_bytes=60 * 1024 * 1024),
        name="emit",
    )(*results)

    def fresh(rows):
        return jnp.swapaxes(rows, 1, 2).reshape(LAYERS, BATCH, 1, HEAD)

    return h_out, fresh(k_new), fresh(v_new)


def solution(mesh):
    act_spec = P("dp", "row")
    cache_spec = P(None, "dp", ("col", "row"), None, None)
    fresh_spec = P(None, "dp", ("col", "row"), None)
    in_weight = P(None, "row", "col")
    out_weight = P(None, "col", "row")
    col_vec = P(None, "col")
    row_vec = P(None, "row")
    in_specs = (act_spec, P("dp"), cache_spec, cache_spec, row_vec, row_vec,
                in_weight, col_vec, in_weight, col_vec, in_weight, col_vec,
                out_weight, row_vec, row_vec, row_vec, in_weight, col_vec, out_weight, row_vec)
    return jax.shard_map(run_step, mesh=mesh, in_specs=in_specs,
                         out_specs=(act_spec, fresh_spec, fresh_spec), check_vma=False)
```

```python
import functools

import jax
import jax.numpy as jnp
from jax import lax
from jax.experimental import pallas as pl
from jax.experimental.pallas import tpu as pltpu
from jax.sharding import PartitionSpec as P

EPS_LN = 1e-5
MESH = pl.DeviceIdType.MESH
F32 = jnp.float32
BF16 = jnp.bfloat16

LAYERS = 2
BATCH = 128
STREAMS = 2
ROWS = BATCH // STREAMS
HALF = ROWS // 2
GROUP = 16
COL_PIECES = 4
N_ROW = 4
N_COL = 4
HEAD = 64
SEQ = 512
WIDTH = 256
D_MODEL = 1024
FF_LOC = 1024
FF_HALF = FF_LOC // 2

VEC_NAMES = ("g1", "b1", "bq", "bk", "bv", "bo", "g2", "b2", "bf2")
MAT_NAMES = ("wq", "wk", "wv", "wo", "wf1", "wf2")


def lane_iota(shape):
    return lax.broadcasted_iota(jnp.int32, shape, len(shape) - 1)


def swap_halves(val):
    return pltpu.roll(val, HEAD, 1)


def low_half(shape):
    return lane_iota(shape) < HEAD


def step_kernel(*refs):
    (x_in, len_in, k_in, v_in, g1_in, b1_in, wq_in, bq_in, wk_in, bk_in, wv_in, bv_in,
     wo_in, bo_in, g2_in, b2_in, wf1_in, bf1_in, wf2_in, bf2_in,
     h_out, k_out, v_out,
     x_buf, len_buf, k_buf, v_buf, g1, b1, wq, bq, wk, bk, wv, bv, wo, bo, g2, b2, wf1, bf1, wf2, bf2,
     len_mat, kv_mix, kv_turn, s_buf, p_buf, o_mix,
     st_send, st_recv, gq_send, gq_recv, gf_send, gf_recv, qkv_send, qkv_recv, o_recv,
     proj_recv, f1_mine, f1_send, f1_recv, pair_recv, u_recv, out_recv,
     load_sem, big_sem, store_sem, send_sem, recv_sem) = refs

    row = lax.axis_index("row")
    col = lax.axis_index("col")
    side = lax.rem(row, 2)
    chip = row // 2
    partner = chip * 2 + (1 - side)
    across = lax.rem(row + 2, N_ROW)

    loads = {}

    def load(name, src, dst, sem):
        copy = pltpu.make_async_copy(src, dst, sem)
        copy.start()
        loads[name] = copy

    n_load = [0]

    def small(name, src, dst):
        load(name, src, dst, load_sem.at[n_load[0]])
        n_load[0] += 1

    small("x", x_in, x_buf)
    small("g1", g1_in, g1)
    for layer in range(LAYERS):
        for name, src, dst in (("wq", wq_in, wq), ("wk", wk_in, wk), ("wv", wv_in, wv)):
            if layer == 0:
                small((name, layer), src.at[layer], dst.at[layer])
    for name, src, dst in (("wq", wq_in, wq), ("wk", wk_in, wk), ("wv", wv_in, wv)):
        small((name, 1), src.at[1], dst.at[1])
    for name, src, dst in (("b1", b1_in, b1), ("bq", bq_in, bq), ("bk", bk_in, bk), ("bv", bv_in, bv),
                           ("len", len_in, len_buf), ("bo", bo_in, bo), ("g2", g2_in, g2), ("b2", b2_in, b2),
                           ("bf1", bf1_in, bf1), ("bf2", bf2_in, bf2)):
        small(name, src, dst)
    for layer in range(LAYERS):
        small(("wf1", layer), wf1_in.at[layer], wf1.at[layer])

    barrier = pltpu.get_barrier_semaphore()
    for off in range(1, 4):
        pl.semaphore_signal(barrier, inc=1, device_id={"row": lax.rem(row + off, N_ROW)}, device_id_type=MESH)
        pl.semaphore_signal(barrier, inc=1, device_id={"col": lax.rem(col + off, N_COL)}, device_id_type=MESH)

    def big(layer, stream, which):
        src, dst = (k_in, k_buf) if which == 0 else (v_in, v_buf)
        span = pl.ds(stream * ROWS * HEAD, ROWS * HEAD)
        load(("kv", layer, stream, which), src.at[layer, span], dst.at[layer, span],
             big_sem.at[(layer * STREAMS + stream) * 2 + which])

    for stream in range(STREAMS):
        for which in range(2):
            big(0, stream, which)
    for name, src, dst in (("wo", wo_in, wo), ("wf2", wf2_in, wf2)):
        small((name, 0), src.at[0], dst.at[0])
    for name, src, dst in (("wo", wo_in, wo), ("wf2", wf2_in, wf2)):
        small((name, 1), src.at[1], dst.at[1])
    for stream in range(STREAMS):
        for which in range(2):
            big(1, stream, which)

    waited = set()

    def need(name):
        if name not in waited:
            waited.add(name)
            loads[name].wait()

    drains = []
    recvs = {}
    n_sem = [0]

    def exchange(tag, copies, span):
        index = n_sem[0]
        n_sem[0] += 1
        for src, dst, device in copies:
            pltpu.make_async_remote_copy(
                src_ref=src, dst_ref=dst, send_sem=send_sem.at[index],
                recv_sem=recv_sem.at[index], device_id=device, device_id_type=MESH).start()
        drains.append(pltpu.make_async_copy(span, span, send_sem.at[index]))
        recvs[tag] = pltpu.make_async_copy(span, span, recv_sem.at[index])

    def to_col(tag, buf):
        peers = (3 - col, lax.rem(col + 2, N_COL), col + 1 - 2 * lax.rem(col, 2))
        rows = ROWS // COL_PIECES
        copies = []
        for piece in range(COL_PIECES):
            mine = buf.at[col, piece * rows:(piece + 1) * rows]
            copies += [(mine, mine, {"col": peer}) for peer in peers]
        exchange(tag, copies, buf.at[0:3])

    def to_axis(tag, axis, src_of, buf):
        me = row if axis == "row" else col
        dests = [lax.rem(me + off, 4) for off in (2, 3, 1)]
        exchange(tag, [(src_of(d), buf.at[me], {axis: d}) for d in dests], buf.at[0:3])

    def arrived(tag):
        recvs[tag].wait()

    def local_norm(state, gain):
        mean = jnp.sum(state, axis=-1, keepdims=True) * (1.0 / WIDTH)
        delta = state - mean
        var = jnp.sum(delta * delta, axis=-1, keepdims=True) * (1.0 / WIDTH)
        normed = (delta * lax.rsqrt(var + EPS_LN) * gain).astype(BF16)
        lanes = lane_iota((ROWS, 128))
        tile = jnp.where(lanes == 0, mean, jnp.where(lanes == 1, var, 0.0))
        if ROWS < 128:
            tile = jnp.concatenate([tile] * (128 // ROWS), axis=0)
        return normed, jnp.transpose(tile)[0:8]

    def merge_stats(blocks):
        share = 1.0 / len(blocks)
        mean = sum(m for m, _ in blocks) * share
        var = sum(v + (m - mean) * (m - mean) for m, v in blocks) * share
        return mean, var

    def stat_columns(blocks):
        mean, var = merge_stats(blocks)
        inv = lax.rsqrt(var + EPS_LN)
        lines = [jnp.sqrt(v + EPS_LN) * inv for _, v in blocks] + [(m - mean) * inv for m, _ in blocks]
        sub = lax.broadcasted_iota(jnp.int32, (8, 128), 0)
        tile = jnp.zeros((8, 128), F32)
        for i, line in enumerate(lines):
            tile = jnp.where(sub == i, line, tile)
        turned = jnp.transpose(jnp.concatenate([tile] * 16, axis=0))[0:ROWS]
        return [turned[:, i:i + 1] for i in range(len(lines))]

    def block_stats(index, r):
        tile = st_recv[index, r]
        return tile[0:1], tile[1:2]

    def pack_heads(q, k, v, j, rows):
        half = rows // 2
        lo = (j // 2) * 128
        q, k, v = q[:, lo:lo + 128], k[:, lo:lo + 128], v[:, lo:lo + 128]
        if j % 2 == 0:
            first = jnp.where(low_half((rows, 128)), q, swap_halves(k))
            second = jnp.where(low_half((half, 128)), v[:half], swap_halves(v[half:]))
        else:
            first = jnp.where(low_half((rows, 128)), swap_halves(q), k)
            second = jnp.where(low_half((half, 128)), swap_halves(v[:half]), v[half:])
        return first, second

    def dot(a, b):
        return jnp.dot(a, b, preferred_element_type=F32)

    def send_qkv(layer, stream):
        slot = layer * STREAMS + stream
        need("x")
        need("g1")
        state = x_buf[stream * ROWS:(stream + 1) * ROWS, :].astype(F32)
        normed, tile = local_norm(state, g1[layer:layer + 1, :].astype(F32))
        st_send[2 * slot] = tile
        st_recv[2 * slot, row] = tile
        for name in ("wq", "wk", "wv"):
            need((name, layer))
        q, k, v = dot(normed, wq[layer]), dot(normed, wk[layer]), dot(normed, wv[layer])
        for j in range(N_ROW):
            first, second = pack_heads(q, k, v, j, ROWS)
            qkv_send[slot, j, 0:ROWS] = first.astype(BF16)
            qkv_send[slot, j, ROWS:ROWS + HALF] = second.astype(BF16)
        qkv_recv[slot, row] = qkv_send[slot, row]
        if layer == 0 and stream == 0:
            pl.semaphore_wait(barrier, N_PEER)
        to_axis(("st1", slot), "row", lambda d: st_send.at[2 * slot], st_recv.at[2 * slot])
        to_axis(("qkv", slot), "row", lambda d: qkv_send.at[slot, d], qkv_recv.at[slot])

    def affine_rows(gains, shifts, layer):
        gain, shift = gains[layer:layer + 1, :].astype(F32), shifts[layer:layer + 1, :].astype(F32)
        sub = lax.broadcasted_iota(jnp.int32, (16, WIDTH), 0)
        return jnp.where(sub == 2 * layer, gain, jnp.where(sub == 2 * layer + 1, shift, 0.0)).astype(BF16)

    def send_affine(kind):
        bias_on = jnp.where(row == 0, 1.0, 0.0)

        def product(gains, shifts, w, b):
            total = None
            for layer in range(LAYERS):
                part = dot(affine_rows(gains, shifts, layer), w[layer])[0:8]
                sub = lax.broadcasted_iota(jnp.int32, part.shape, 0)
                part = part + jnp.where(sub == 2 * layer + 1, b[layer:layer + 1, :].astype(F32) * bias_on, 0.0)
                total = part if total is None else total + part
            return total

        if kind == 0:
            for name in ("b1", "bq", "bk", "bv", ("wq", 1), ("wk", 1), ("wv", 1)):
                need(name)
            q, k, v = product(g1, b1, wq, bq), product(g1, b1, wk, bk), product(g1, b1, wv, bv)
            for j in range(N_ROW):
                lo = (j // 2) * 128
                qj, kj, vj = q[:, lo:lo + 128], k[:, lo:lo + 128], v[:, lo:lo + 128]
                if j % 2 == 0:
                    first = jnp.where(low_half((8, 128)), qj, swap_halves(kj))
                else:
                    first = jnp.where(low_half((8, 128)), swap_halves(qj), kj)
                    vj = swap_halves(vj)
                second = jnp.where(low_half((8, 128)), vj, swap_halves(vj))
                gq_send[j] = jnp.concatenate([first, second], axis=1)
            gq_recv[row] = gq_send[row]
            to_axis(("gb", kind), "row", lambda d: gq_send.at[d], gq_recv)
        else:
            for name in ("g2", "b2", "bf1", ("wf1", 0), ("wf1", 1)):
                need(name)
            part = product(g2, b2, wf1, bf1)
            for j in range(2):
                gf_send[j] = part[:, j * FF_HALF:(j + 1) * FF_HALF]
            gf_recv[row] = gf_send[side]
            to_axis(("gb", kind), "row", lambda d: gf_send.at[lax.rem(d, 2)], gf_recv)

    gb_done = set()

    def affine_lines(kind):
        if kind not in gb_done:
            gb_done.add(kind)
            arrived(("gb", kind))

    def gain_line(buf, layer, r):
        return buf[r, 2 * layer:2 * layer + 1]

    def const_line(buf, layer):
        at = slice(2 * layer + 1, 2 * layer + 2)
        return buf[0, at] + buf[1, at] + buf[2, at] + buf[3, at]

    def attend(layer, stream):
        slot = layer * STREAMS + stream
        span = slice(stream * ROWS, (stream + 1) * ROWS)
        arrived(("st1", slot))
        cols = stat_columns([block_stats(2 * slot, r) for r in range(N_ROW)])
        affine_lines(0)
        gains = [gain_line(gq_recv, layer, r) for r in range(N_ROW)]
        const = const_line(gq_recv, layer)
        arrived(("qkv", slot))
        low = low_half((HALF, 128))
        qk = const[:, 0:128]
        vv = const[:, 128:256]
        for r in range(N_ROW):
            part = qkv_recv[slot, r].astype(F32)
            scale, shift = cols[r], cols[4 + r]
            qk = qk + part[0:ROWS] * scale + shift * gains[r][:, 0:128]
            scale_v = jnp.where(low, scale[0:HALF], scale[HALF:ROWS])
            shift_v = jnp.where(low, shift[0:HALF], shift[HALF:ROWS])
            vv = vv + part[ROWS:ROWS + HALF] * scale_v + shift_v * gains[r][:, 128:256]
        full_low = low_half((ROWS, 128))
        qk_turn = swap_halves(qk)
        q2 = (jnp.where(full_low, qk, qk_turn) * (HEAD ** -0.5)).astype(BF16)
        k2 = jnp.where(full_low, qk_turn, qk).astype(BF16)
        vv_turn = swap_halves(vv)
        v2 = jnp.concatenate([jnp.where(low, vv, vv_turn), jnp.where(low, vv_turn, vv)], axis=0).astype(BF16)
        kv_mix[layer, span, :] = jnp.where(full_low, k2.astype(F32), v2.astype(F32))
        score_new = jnp.sum(jnp.where(full_low, q2.astype(F32) * k2.astype(F32), 0.0), axis=-1, keepdims=True)

        need(("kv", layer, stream, 0))
        q_row = lax.broadcasted_iota(jnp.int32, (GROUP, 128), 0)
        q_half = lane_iota((GROUP, 128)) // HEAD
        for g in range(ROWS // GROUP):
            base = (stream * ROWS + g * GROUP) * HEAD
            qg = q2[g * GROUP:(g + 1) * GROUP].astype(F32)
            spread = [jnp.where(q_row == 2 * j + q_half, qg, 0.0).astype(BF16) for j in range(GROUP // 2)]
            s_buf[g * GROUP:(g + 1) * GROUP, :] = dot(jnp.concatenate(spread, axis=1),
                                                      k_buf[layer, base:base + GROUP * HEAD, :])
        positions = lane_iota((ROWS, SEQ)).astype(F32)
        limit = len_mat[span, 0:1]
        scores = jnp.where(positions < limit, s_buf[...], -jnp.inf)
        peak = jnp.maximum(jnp.max(scores, axis=-1, keepdims=True), score_new)
        exp_cache = jnp.exp(scores - peak)
        exp_new = jnp.exp(score_new - peak)
        inv = 1.0 / (jnp.sum(exp_cache, axis=-1, keepdims=True) + exp_new)
        p_buf[...] = (exp_cache * inv).astype(BF16)
        prob_new = (exp_new * inv).astype(BF16).astype(F32)

        need(("kv", layer, stream, 1))
        for g in range(ROWS // GROUP):
            base = (stream * ROWS + g * GROUP) * HEAD
            wide = lax.dot_general(p_buf[g * GROUP:(g + 1) * GROUP, :], v_buf[layer, base:base + GROUP * HEAD, :],
                                   (((1,), (1,)), ((), ())), preferred_element_type=F32)
            acc = jnp.zeros((GROUP, 128), F32)
            for j in range(GROUP // 2):
                acc = acc + jnp.where(q_row == 2 * j + q_half, wide[:, j * 128:(j + 1) * 128], 0.0)
            o_mix[g * GROUP:(g + 1) * GROUP, :] = acc + swap_halves(acc)
        o2 = o_mix[...] + prob_new * v2.astype(F32)
        packed = jnp.where(low, o2[0:HALF], o2[HALF:ROWS]).astype(BF16)
        o_recv[slot, row] = packed
        to_axis(("o", slot), "row", lambda d: o_recv.at[slot, row], o_recv.at[slot])

    def unpack_heads(buf, first):
        low = low_half((HALF, 128))
        parts = [buf[first + r].astype(F32) for r in range(N_ROW)]
        turns = [swap_halves(p) for p in parts]
        pairs = []
        for a, b in ((0, 1), (2, 3)):
            top = jnp.where(low, parts[a], turns[b])
            bottom = jnp.where(low, turns[a], parts[b])
            pairs.append(jnp.concatenate([top, bottom], axis=0).astype(BF16))
        return jnp.concatenate(pairs, axis=1)

    def project(layer, stream):
        slot = layer * STREAMS + stream
        need(("wo", layer))
        arrived(("o", slot))
        proj_recv[slot, col] = dot(unpack_heads(o_recv.at[slot], 0), wo[layer]).astype(BF16)
        to_col(("proj", slot), proj_recv.at[slot])

    def col_sum(buf):
        total = buf[0].astype(F32)
        for c in range(1, N_COL):
            total = total + buf[c].astype(F32)
        return total

    def residual(total, bias, stream):
        span = slice(stream * ROWS, (stream + 1) * ROWS)
        new = (x_buf[span, :].astype(F32) + (total + bias)).astype(BF16)
        x_buf[span, :] = new
        return new.astype(F32)

    def send_inner(layer, stream):
        slot = layer * STREAMS + stream
        need("bo")
        need("g2")
        need(("wf1", layer))
        arrived(("proj", slot))
        total = col_sum(proj_recv.at[slot])
        state = residual(total, bo[layer:layer + 1, :].astype(F32), stream)
        normed, tile = local_norm(state, g2[layer:layer + 1, :].astype(F32))
        index = 2 * slot + 1
        st_send[index] = tile
        st_recv[index, row] = tile
        mine = st_send.at[index]
        spot = st_recv.at[index, row]
        exchange(("st2", slot), [(mine, spot, {"row": partner})], mine)
        far = lax.rem(partner + 2, N_ROW)
        exchange(("st3", slot), [(mine, spot, {"row": across}), (mine, spot, {"row": far})], st_recv.at[index, 0:2])
        theirs = pl.ds(pl.multiple_of((1 - side) * FF_HALF, FF_HALF), FF_HALF)
        f1_send[slot] = dot(normed, wf1[layer, :, theirs]).astype(BF16)
        exchange(("f1", slot), [(f1_send.at[slot], f1_recv.at[slot], {"row": partner})], f1_recv.at[slot])
        ours = pl.ds(pl.multiple_of(side * FF_HALF, FF_HALF), FF_HALF)
        f1_mine[stream] = dot(normed, wf1[layer, :, ours])

    def send_pair(layer, stream):
        slot = layer * STREAMS + stream
        arrived(("st2", slot))
        cols = stat_columns([block_stats(2 * slot + 1, r) for r in (row, partner)])
        affine_lines(1)
        arrived(("f1", slot))
        total = f1_mine[stream] * cols[0] + cols[2] * gain_line(gf_recv, layer, row)
        total = total + f1_recv[slot].astype(F32) * cols[1] + cols[3] * gain_line(gf_recv, layer, partner)
        pair_recv[slot, chip] = total.astype(BF16)
        mine = pair_recv.at[slot, chip]
        exchange(("pair", slot), [(mine, mine, {"row": across})], mine)

    def send_act(layer, stream):
        slot = layer * STREAMS + stream
        arrived(("st3", slot))
        pairs = [merge_stats([block_stats(2 * slot + 1, 2 * k + r) for r in range(2)]) for k in range(2)]
        cols = stat_columns(pairs)
        total = const_line(gf_recv, layer)
        arrived(("pair", slot))
        for k in range(2):
            gain = gain_line(gf_recv, layer, 2 * k) + gain_line(gf_recv, layer, 2 * k + 1)
            total = total + pair_recv[slot, k].astype(F32) * cols[k] + cols[2 + k] * gain
        u_recv[slot, side] = jnp.maximum(total, 0.0).astype(BF16)
        mine = u_recv.at[slot, side]
        exchange(("u", slot), [(mine, mine, {"row": partner})], mine)

    def send_out(layer, stream):
        slot = layer * STREAMS + stream
        need(("wf2", layer))
        arrived(("u", slot))
        acc = dot(u_recv[slot, 0], wf2[layer, 0:FF_HALF, :]) + dot(u_recv[slot, 1], wf2[layer, FF_HALF:, :])
        out_recv[slot, col] = acc.astype(BF16)
        to_col(("out", slot), out_recv.at[slot])

    def finish(layer, stream):
        slot = layer * STREAMS + stream
        need("bf2")
        arrived(("out", slot))
        residual(col_sum(out_recv.at[slot]), bf2[layer:layer + 1, :].astype(F32), stream)

    stores = []

    def store(src, dst, index):
        copy = pltpu.make_async_copy(src, dst, store_sem.at[index])
        copy.start()
        stores.append(copy)

    for stream in range(STREAMS):
        send_qkv(0, stream)
    send_affine(0)
    send_affine(1)
    need("len")
    len_mat[...] = jnp.transpose(jnp.broadcast_to(len_buf[...].astype(F32), (128, 128)))
    for layer in range(LAYERS):
        for stream in range(STREAMS):
            attend(layer, stream)
        kv_turn[layer] = jnp.transpose(kv_mix[layer]).astype(BF16)
        store(kv_turn.at[layer, 0:HEAD], k_out.at[layer], 2 * layer)
        store(kv_turn.at[layer, HEAD:2 * HEAD], v_out.at[layer], 2 * layer + 1)
        for stream in range(STREAMS):
            project(layer, stream)
        for stream in range(STREAMS):
            send_inner(layer, stream)
        for stream in range(STREAMS):
            send_pair(layer, stream)
        for stream in range(STREAMS):
            send_act(layer, stream)
        for stream in range(STREAMS):
            send_out(layer, stream)
        for stream in range(STREAMS):
            finish(layer, stream)
            if layer + 1 < LAYERS:
                send_qkv(layer + 1, stream)
            else:
                span = pl.ds(stream * ROWS, ROWS)
                store(x_buf.at[span], h_out.at[span], 2 * LAYERS + stream)
    for copy in stores:
        copy.wait()
    for copy in drains:
        copy.wait()


N_SLOT = LAYERS * STREAMS
N_COPY = 10 * N_SLOT + 2
N_PEER = N_ROW + N_COL - 2


def emit_kernel(h_in, k_in, v_in, h_out, k_out, v_out, h_buf, k_buf, v_buf, sem):
    moves = ((h_in, h_buf, h_out), (k_in, k_buf, k_out), (v_in, v_buf, v_out))
    loads = [pltpu.make_async_copy(src, buf, sem.at[i]) for i, (src, buf, _) in enumerate(moves)]
    for copy in loads:
        copy.start()
    stores = []
    for i, (_, buf, dst) in enumerate(moves):
        loads[i].wait()
        copy = pltpu.make_async_copy(buf, dst, sem.at[i])
        copy.start()
        stores.append(copy)
    for copy in stores:
        copy.wait()


def run_step(x, lens, k_cache, v_cache, g1, b1, wq, bq, wk, bk, wv, bv, wo, bo, g2, b2, wf1, bf1, wf2, bf2):
    any_spec = pl.BlockSpec(memory_space=pl.ANY)
    args = (x, lens.reshape(1, BATCH),
            jnp.swapaxes(k_cache, 3, 4).reshape(LAYERS, BATCH * HEAD, SEQ),
            jnp.swapaxes(v_cache, 3, 4).reshape(LAYERS, BATCH * HEAD, SEQ),
            g1, b1, wq, bq, wk, bk, wv, bv, wo, bo, g2, b2, wf1, bf1, wf2, bf2)
    vm = pltpu.VMEM
    in_scratch = [vm(a.shape, a.dtype) for a in args]
    scratch = in_scratch + [
        vm((BATCH, 128), F32),
        vm((LAYERS, BATCH, 128), F32),
        vm((LAYERS, BATCH, 128), BF16),
        vm((ROWS, SEQ), F32),
        vm((ROWS, SEQ), BF16),
        vm((ROWS, 128), F32),
        vm((2 * N_SLOT, 8, 128), F32),
        vm((2 * N_SLOT, N_ROW, 8, 128), F32),
        vm((N_ROW, 8, WIDTH), F32),
        vm((N_ROW, 8, WIDTH), F32),
        vm((2, 8, FF_HALF), F32),
        vm((N_ROW, 8, FF_HALF), F32),
        vm((N_SLOT, N_ROW, ROWS + HALF, 128), BF16),
        vm((N_SLOT, N_ROW, ROWS + HALF, 128), BF16),
        vm((N_SLOT, N_ROW, HALF, 128), BF16),
        vm((N_SLOT, N_COL, ROWS, WIDTH), BF16),
        vm((STREAMS, ROWS, FF_HALF), F32),
        vm((N_SLOT, ROWS, FF_HALF), BF16),
        vm((N_SLOT, ROWS, FF_HALF), BF16),
        vm((N_SLOT, 2, ROWS, FF_HALF), BF16),
        vm((N_SLOT, 2, ROWS, FF_HALF), BF16),
        vm((N_SLOT, N_COL, ROWS, WIDTH), BF16),
        pltpu.SemaphoreType.DMA((32,)),
        pltpu.SemaphoreType.DMA((2 * N_SLOT,)),
        pltpu.SemaphoreType.DMA((2 * LAYERS + STREAMS,)),
        pltpu.SemaphoreType.DMA((N_COPY,)),
        pltpu.SemaphoreType.DMA((N_COPY,)),
    ]
    shapes = (jax.ShapeDtypeStruct((BATCH, WIDTH), BF16),
              jax.ShapeDtypeStruct((LAYERS, HEAD, BATCH), BF16),
              jax.ShapeDtypeStruct((LAYERS, HEAD, BATCH), BF16))
    results = pl.pallas_call(
        step_kernel,
        out_shape=shapes,
        in_specs=[pl.BlockSpec(memory_space=pltpu.HBM)] * len(args),
        out_specs=(any_spec,) * 3,
        scratch_shapes=scratch,
        compiler_params=pltpu.CompilerParams(
            collective_id=0, has_side_effects=True, vmem_limit_bytes=60 * 1024 * 1024),
        name="decode_step",
    )(*args)
    h_out, k_new, v_new = pl.pallas_call(
        emit_kernel,
        out_shape=shapes,
        in_specs=[any_spec] * 3,
        out_specs=(pl.BlockSpec(memory_space=pltpu.HBM),) * 3,
        scratch_shapes=[vm(a.shape, a.dtype) for a in shapes] + [pltpu.SemaphoreType.DMA((3,))],
        compiler_params=pltpu.CompilerParams(vmem_limit_bytes=60 * 1024 * 1024),
        name="emit",
    )(*results)

    def fresh(rows):
        return jnp.swapaxes(rows, 1, 2).reshape(LAYERS, BATCH, 1, HEAD)

    return h_out, fresh(k_new), fresh(v_new)


def solution(mesh):
    act_spec = P("dp", "row")
    cache_spec = P(None, "dp", ("col", "row"), None, None)
    fresh_spec = P(None, "dp", ("col", "row"), None)
    in_weight = P(None, "row", "col")
    out_weight = P(None, "col", "row")
    col_vec = P(None, "col")
    row_vec = P(None, "row")
    in_specs = (act_spec, P("dp"), cache_spec, cache_spec, row_vec, row_vec,
                in_weight, col_vec, in_weight, col_vec, in_weight, col_vec,
                out_weight, row_vec, row_vec, row_vec, in_weight, col_vec, out_weight, row_vec)
    return jax.shard_map(run_step, mesh=mesh, in_specs=in_specs,
                         out_specs=(act_spec, fresh_spec, fresh_spec), check_vma=False)
```

```python
import functools

import jax
import jax.numpy as jnp
from jax import lax
from jax.experimental import pallas as pl
from jax.experimental.pallas import tpu as pltpu
from jax.sharding import PartitionSpec as P

EPS_LN = 1e-5
MESH = pl.DeviceIdType.MESH
F32 = jnp.float32
BF16 = jnp.bfloat16

LAYERS = 2
BATCH = 128
STREAMS = 2
ROWS = BATCH // STREAMS
HALF = ROWS // 2
GROUP = 16
COL_PIECES = 4
N_ROW = 4
N_COL = 4
HEAD = 64
SEQ = 512
WIDTH = 256
D_MODEL = 1024
FF_LOC = 1024
FF_HALF = FF_LOC // 2

VEC_NAMES = ("g1", "b1", "bq", "bk", "bv", "bo", "g2", "b2", "bf2")
MAT_NAMES = ("wq", "wk", "wv", "wo", "wf1", "wf2")


def lane_iota(shape):
    return lax.broadcasted_iota(jnp.int32, shape, len(shape) - 1)


def swap_halves(val):
    return pltpu.roll(val, HEAD, 1)


def low_half(shape):
    return lane_iota(shape) < HEAD


def step_kernel(*refs):
    (x_in, len_in, k_in, v_in, g1_in, b1_in, wq_in, bq_in, wk_in, bk_in, wv_in, bv_in,
     wo_in, bo_in, g2_in, b2_in, wf1_in, bf1_in, wf2_in, bf2_in,
     h_out, k_out, v_out,
     x_buf, len_buf, k_buf, v_buf, g1, b1, wq, bq, wk, bk, wv, bv, wo, bo, g2, b2, wf1, bf1, wf2, bf2,
     len_mat, kv_mix, s_buf, p_buf, o_mix,
     st_send, st_recv, gq_send, gq_recv, gf_send, gf_recv, qkv_send, qkv_recv, o_recv,
     proj_recv, f1_mine, f1_send, f1_recv, pair_recv, u_recv, out_recv,
     load_sem, big_sem, send_sem, recv_sem) = refs

    row = lax.axis_index("row")
    col = lax.axis_index("col")
    side = lax.rem(row, 2)
    chip = row // 2
    partner = chip * 2 + (1 - side)
    across = lax.rem(row + 2, N_ROW)

    loads = {}

    def load(name, src, dst, sem):
        copy = pltpu.make_async_copy(src, dst, sem)
        copy.start()
        loads[name] = copy

    n_load = [0]

    def small(name, src, dst):
        load(name, src, dst, load_sem.at[n_load[0]])
        n_load[0] += 1

    small("x", x_in, x_buf)
    small("g1", g1_in, g1)
    for layer in range(LAYERS):
        for name, src, dst in (("wq", wq_in, wq), ("wk", wk_in, wk), ("wv", wv_in, wv)):
            if layer == 0:
                small((name, layer), src.at[layer], dst.at[layer])
    for name, src, dst in (("wq", wq_in, wq), ("wk", wk_in, wk), ("wv", wv_in, wv)):
        small((name, 1), src.at[1], dst.at[1])
    for name, src, dst in (("b1", b1_in, b1), ("bq", bq_in, bq), ("bk", bk_in, bk), ("bv", bv_in, bv),
                           ("len", len_in, len_buf), ("bo", bo_in, bo), ("g2", g2_in, g2), ("b2", b2_in, b2),
                           ("bf1", bf1_in, bf1), ("bf2", bf2_in, bf2)):
        small(name, src, dst)
    for layer in range(LAYERS):
        small(("wf1", layer), wf1_in.at[layer], wf1.at[layer])

    barrier = pltpu.get_barrier_semaphore()
    for off in range(1, 4):
        pl.semaphore_signal(barrier, inc=1, device_id={"row": lax.rem(row + off, N_ROW)}, device_id_type=MESH)
        pl.semaphore_signal(barrier, inc=1, device_id={"col": lax.rem(col + off, N_COL)}, device_id_type=MESH)

    def big(layer, stream, which):
        src, dst = (k_in, k_buf) if which == 0 else (v_in, v_buf)
        span = pl.ds(stream * ROWS * HEAD, ROWS * HEAD)
        load(("kv", layer, stream, which), src.at[layer, span], dst.at[layer, span],
             big_sem.at[(layer * STREAMS + stream) * 2 + which])

    for stream in range(STREAMS):
        for which in range(2):
            big(0, stream, which)
    for name, src, dst in (("wo", wo_in, wo), ("wf2", wf2_in, wf2)):
        small((name, 0), src.at[0], dst.at[0])
    for name, src, dst in (("wo", wo_in, wo), ("wf2", wf2_in, wf2)):
        small((name, 1), src.at[1], dst.at[1])
    for stream in range(STREAMS):
        for which in range(2):
            big(1, stream, which)

    waited = set()

    def need(name):
        if name not in waited:
            waited.add(name)
            loads[name].wait()

    drains = []
    recvs = {}
    n_sem = [0]

    def exchange(tag, copies, span):
        index = n_sem[0]
        n_sem[0] += 1
        for src, dst, device in copies:
            pltpu.make_async_remote_copy(
                src_ref=src, dst_ref=dst, send_sem=send_sem.at[index],
                recv_sem=recv_sem.at[index], device_id=device, device_id_type=MESH).start()
        drains.append(pltpu.make_async_copy(span, span, send_sem.at[index]))
        recvs[tag] = pltpu.make_async_copy(span, span, recv_sem.at[index])

    def to_col(tag, buf):
        peers = (3 - col, lax.rem(col + 2, N_COL), col + 1 - 2 * lax.rem(col, 2))
        rows = ROWS // COL_PIECES
        copies = []
        for piece in range(COL_PIECES):
            mine = buf.at[col, piece * rows:(piece + 1) * rows]
            copies += [(mine, mine, {"col": peer}) for peer in peers]
        exchange(tag, copies, buf.at[0:3])

    def to_axis(tag, axis, src_of, buf):
        me = row if axis == "row" else col
        dests = [lax.rem(me + off, 4) for off in (2, 3, 1)]
        exchange(tag, [(src_of(d), buf.at[me], {axis: d}) for d in dests], buf.at[0:3])

    def arrived(tag):
        recvs[tag].wait()

    def local_norm(state, gain):
        mean = jnp.sum(state, axis=-1, keepdims=True) * (1.0 / WIDTH)
        delta = state - mean
        var = jnp.sum(delta * delta, axis=-1, keepdims=True) * (1.0 / WIDTH)
        normed = (delta * lax.rsqrt(var + EPS_LN) * gain).astype(BF16)
        lanes = lane_iota((ROWS, 128))
        tile = jnp.where(lanes == 0, mean, jnp.where(lanes == 1, var, 0.0))
        if ROWS < 128:
            tile = jnp.concatenate([tile] * (128 // ROWS), axis=0)
        return normed, jnp.transpose(tile)[0:8]

    def merge_stats(blocks):
        share = 1.0 / len(blocks)
        mean = sum(m for m, _ in blocks) * share
        var = sum(v + (m - mean) * (m - mean) for m, v in blocks) * share
        return mean, var

    def stat_columns(blocks):
        mean, var = merge_stats(blocks)
        inv = lax.rsqrt(var + EPS_LN)
        lines = [jnp.sqrt(v + EPS_LN) * inv for _, v in blocks] + [(m - mean) * inv for m, _ in blocks]
        sub = lax.broadcasted_iota(jnp.int32, (8, 128), 0)
        tile = jnp.zeros((8, 128), F32)
        for i, line in enumerate(lines):
            tile = jnp.where(sub == i, line, tile)
        turned = jnp.transpose(jnp.concatenate([tile] * 16, axis=0))[0:ROWS]
        return [turned[:, i:i + 1] for i in range(len(lines))]

    def block_stats(index, r):
        tile = st_recv[index, r]
        return tile[0:1], tile[1:2]

    def pack_heads(q, k, v, j, rows):
        half = rows // 2
        lo = (j // 2) * 128
        q, k, v = q[:, lo:lo + 128], k[:, lo:lo + 128], v[:, lo:lo + 128]
        if j % 2 == 0:
            first = jnp.where(low_half((rows, 128)), q, swap_halves(k))
            second = jnp.where(low_half((half, 128)), v[:half], swap_halves(v[half:]))
        else:
            first = jnp.where(low_half((rows, 128)), swap_halves(q), k)
            second = jnp.where(low_half((half, 128)), swap_halves(v[:half]), v[half:])
        return first, second

    def dot(a, b):
        return jnp.dot(a, b, preferred_element_type=F32)

    def send_qkv(layer, stream):
        slot = layer * STREAMS + stream
        need("x")
        need("g1")
        state = x_buf[stream * ROWS:(stream + 1) * ROWS, :].astype(F32)
        normed, tile = local_norm(state, g1[layer:layer + 1, :].astype(F32))
        st_send[2 * slot] = tile
        st_recv[2 * slot, row] = tile
        for name in ("wq", "wk", "wv"):
            need((name, layer))
        q, k, v = dot(normed, wq[layer]), dot(normed, wk[layer]), dot(normed, wv[layer])
        for j in range(N_ROW):
            first, second = pack_heads(q, k, v, j, ROWS)
            qkv_send[slot, j, 0:ROWS] = first.astype(BF16)
            qkv_send[slot, j, ROWS:ROWS + HALF] = second.astype(BF16)
        qkv_recv[slot, row] = qkv_send[slot, row]
        if layer == 0 and stream == 0:
            pl.semaphore_wait(barrier, N_PEER)
        to_axis(("st1", slot), "row", lambda d: st_send.at[2 * slot], st_recv.at[2 * slot])
        to_axis(("qkv", slot), "row", lambda d: qkv_send.at[slot, d], qkv_recv.at[slot])

    def affine_rows(gains, shifts, layer):
        gain, shift = gains[layer:layer + 1, :].astype(F32), shifts[layer:layer + 1, :].astype(F32)
        sub = lax.broadcasted_iota(jnp.int32, (16, WIDTH), 0)
        return jnp.where(sub == 2 * layer, gain, jnp.where(sub == 2 * layer + 1, shift, 0.0)).astype(BF16)

    def send_affine(kind):
        bias_on = jnp.where(row == 0, 1.0, 0.0)

        def product(gains, shifts, w, b):
            total = None
            for layer in range(LAYERS):
                part = dot(affine_rows(gains, shifts, layer), w[layer])[0:8]
                sub = lax.broadcasted_iota(jnp.int32, part.shape, 0)
                part = part + jnp.where(sub == 2 * layer + 1, b[layer:layer + 1, :].astype(F32) * bias_on, 0.0)
                total = part if total is None else total + part
            return total

        if kind == 0:
            for name in ("b1", "bq", "bk", "bv", ("wq", 1), ("wk", 1), ("wv", 1)):
                need(name)
            q, k, v = product(g1, b1, wq, bq), product(g1, b1, wk, bk), product(g1, b1, wv, bv)
            for j in range(N_ROW):
                lo = (j // 2) * 128
                qj, kj, vj = q[:, lo:lo + 128], k[:, lo:lo + 128], v[:, lo:lo + 128]
                if j % 2 == 0:
                    first = jnp.where(low_half((8, 128)), qj, swap_halves(kj))
                else:
                    first = jnp.where(low_half((8, 128)), swap_halves(qj), kj)
                    vj = swap_halves(vj)
                second = jnp.where(low_half((8, 128)), vj, swap_halves(vj))
                gq_send[j] = jnp.concatenate([first, second], axis=1)
            gq_recv[row] = gq_send[row]
            to_axis(("gb", kind), "row", lambda d: gq_send.at[d], gq_recv)
        else:
            for name in ("g2", "b2", "bf1", ("wf1", 0), ("wf1", 1)):
                need(name)
            part = product(g2, b2, wf1, bf1)
            for j in range(2):
                gf_send[j] = part[:, j * FF_HALF:(j + 1) * FF_HALF]
            gf_recv[row] = gf_send[side]
            to_axis(("gb", kind), "row", lambda d: gf_send.at[lax.rem(d, 2)], gf_recv)

    gb_done = set()

    def affine_lines(kind):
        if kind not in gb_done:
            gb_done.add(kind)
            arrived(("gb", kind))

    def gain_line(buf, layer, r):
        return buf[r, 2 * layer:2 * layer + 1]

    def const_line(buf, layer):
        at = slice(2 * layer + 1, 2 * layer + 2)
        return buf[0, at] + buf[1, at] + buf[2, at] + buf[3, at]

    def attend(layer, stream):
        slot = layer * STREAMS + stream
        span = slice(stream * ROWS, (stream + 1) * ROWS)
        arrived(("st1", slot))
        cols = stat_columns([block_stats(2 * slot, r) for r in range(N_ROW)])
        affine_lines(0)
        gains = [gain_line(gq_recv, layer, r) for r in range(N_ROW)]
        const = const_line(gq_recv, layer)
        arrived(("qkv", slot))
        low = low_half((HALF, 128))
        qk = const[:, 0:128]
        vv = const[:, 128:256]
        for r in range(N_ROW):
            part = qkv_recv[slot, r].astype(F32)
            scale, shift = cols[r], cols[4 + r]
            qk = qk + part[0:ROWS] * scale + shift * gains[r][:, 0:128]
            scale_v = jnp.where(low, scale[0:HALF], scale[HALF:ROWS])
            shift_v = jnp.where(low, shift[0:HALF], shift[HALF:ROWS])
            vv = vv + part[ROWS:ROWS + HALF] * scale_v + shift_v * gains[r][:, 128:256]
        full_low = low_half((ROWS, 128))
        qk_turn = swap_halves(qk)
        q2 = (jnp.where(full_low, qk, qk_turn) * (HEAD ** -0.5)).astype(BF16)
        k2 = jnp.where(full_low, qk_turn, qk).astype(BF16)
        vv_turn = swap_halves(vv)
        v2 = jnp.concatenate([jnp.where(low, vv, vv_turn), jnp.where(low, vv_turn, vv)], axis=0).astype(BF16)
        kv_mix[layer, span, :] = jnp.where(full_low, k2.astype(F32), v2.astype(F32))
        score_new = jnp.sum(jnp.where(full_low, q2.astype(F32) * k2.astype(F32), 0.0), axis=-1, keepdims=True)

        need(("kv", layer, stream, 0))
        q_row = lax.broadcasted_iota(jnp.int32, (GROUP, 128), 0)
        q_half = lane_iota((GROUP, 128)) // HEAD
        for g in range(ROWS // GROUP):
            base = (stream * ROWS + g * GROUP) * HEAD
            qg = q2[g * GROUP:(g + 1) * GROUP].astype(F32)
            spread = [jnp.where(q_row == 2 * j + q_half, qg, 0.0).astype(BF16) for j in range(GROUP // 2)]
            s_buf[g * GROUP:(g + 1) * GROUP, :] = dot(jnp.concatenate(spread, axis=1),
                                                      k_buf[layer, base:base + GROUP * HEAD, :])
        positions = lane_iota((ROWS, SEQ)).astype(F32)
        limit = len_mat[span, 0:1]
        scores = jnp.where(positions < limit, s_buf[...], -jnp.inf)
        peak = jnp.maximum(jnp.max(scores, axis=-1, keepdims=True), score_new)
        exp_cache = jnp.exp(scores - peak)
        exp_new = jnp.exp(score_new - peak)
        inv = 1.0 / (jnp.sum(exp_cache, axis=-1, keepdims=True) + exp_new)
        p_buf[...] = (exp_cache * inv).astype(BF16)
        prob_new = (exp_new * inv).astype(BF16).astype(F32)

        need(("kv", layer, stream, 1))
        for g in range(ROWS // GROUP):
            base = (stream * ROWS + g * GROUP) * HEAD
            wide = lax.dot_general(p_buf[g * GROUP:(g + 1) * GROUP, :], v_buf[layer, base:base + GROUP * HEAD, :],
                                   (((1,), (1,)), ((), ())), preferred_element_type=F32)
            acc = jnp.zeros((GROUP, 128), F32)
            for j in range(GROUP // 2):
                acc = acc + jnp.where(q_row == 2 * j + q_half, wide[:, j * 128:(j + 1) * 128], 0.0)
            o_mix[g * GROUP:(g + 1) * GROUP, :] = acc + swap_halves(acc)
        o2 = o_mix[...] + prob_new * v2.astype(F32)
        packed = jnp.where(low, o2[0:HALF], o2[HALF:ROWS]).astype(BF16)
        o_recv[slot, row] = packed
        to_axis(("o", slot), "row", lambda d: o_recv.at[slot, row], o_recv.at[slot])

    def unpack_heads(buf, first):
        low = low_half((HALF, 128))
        parts = [buf[first + r].astype(F32) for r in range(N_ROW)]
        turns = [swap_halves(p) for p in parts]
        pairs = []
        for a, b in ((0, 1), (2, 3)):
            top = jnp.where(low, parts[a], turns[b])
            bottom = jnp.where(low, turns[a], parts[b])
            pairs.append(jnp.concatenate([top, bottom], axis=0).astype(BF16))
        return jnp.concatenate(pairs, axis=1)

    def project(layer, stream):
        slot = layer * STREAMS + stream
        need(("wo", layer))
        arrived(("o", slot))
        proj_recv[slot, col] = dot(unpack_heads(o_recv.at[slot], 0), wo[layer]).astype(BF16)
        to_col(("proj", slot), proj_recv.at[slot])

    def col_sum(buf):
        total = buf[0].astype(F32)
        for c in range(1, N_COL):
            total = total + buf[c].astype(F32)
        return total

    def residual(total, bias, stream):
        span = slice(stream * ROWS, (stream + 1) * ROWS)
        new = (x_buf[span, :].astype(F32) + (total + bias)).astype(BF16)
        x_buf[span, :] = new
        return new.astype(F32)

    def send_inner(layer, stream):
        slot = layer * STREAMS + stream
        need("bo")
        need("g2")
        need(("wf1", layer))
        arrived(("proj", slot))
        total = col_sum(proj_recv.at[slot])
        state = residual(total, bo[layer:layer + 1, :].astype(F32), stream)
        normed, tile = local_norm(state, g2[layer:layer + 1, :].astype(F32))
        index = 2 * slot + 1
        st_send[index] = tile
        st_recv[index, row] = tile
        mine = st_send.at[index]
        spot = st_recv.at[index, row]
        exchange(("st2", slot), [(mine, spot, {"row": partner})], mine)
        far = lax.rem(partner + 2, N_ROW)
        exchange(("st3", slot), [(mine, spot, {"row": across}), (mine, spot, {"row": far})], st_recv.at[index, 0:2])
        theirs = pl.ds(pl.multiple_of((1 - side) * FF_HALF, FF_HALF), FF_HALF)
        f1_send[slot] = dot(normed, wf1[layer, :, theirs]).astype(BF16)
        exchange(("f1", slot), [(f1_send.at[slot], f1_recv.at[slot], {"row": partner})], f1_recv.at[slot])
        ours = pl.ds(pl.multiple_of(side * FF_HALF, FF_HALF), FF_HALF)
        f1_mine[stream] = dot(normed, wf1[layer, :, ours])

    def send_pair(layer, stream):
        slot = layer * STREAMS + stream
        arrived(("st2", slot))
        cols = stat_columns([block_stats(2 * slot + 1, r) for r in (row, partner)])
        affine_lines(1)
        arrived(("f1", slot))
        total = f1_mine[stream] * cols[0] + cols[2] * gain_line(gf_recv, layer, row)
        total = total + f1_recv[slot].astype(F32) * cols[1] + cols[3] * gain_line(gf_recv, layer, partner)
        pair_recv[slot, chip] = total.astype(BF16)
        mine = pair_recv.at[slot, chip]
        exchange(("pair", slot), [(mine, mine, {"row": across})], mine)

    def send_act(layer, stream):
        slot = layer * STREAMS + stream
        arrived(("st3", slot))
        pairs = [merge_stats([block_stats(2 * slot + 1, 2 * k + r) for r in range(2)]) for k in range(2)]
        cols = stat_columns(pairs)
        total = const_line(gf_recv, layer)
        arrived(("pair", slot))
        for k in range(2):
            gain = gain_line(gf_recv, layer, 2 * k) + gain_line(gf_recv, layer, 2 * k + 1)
            total = total + pair_recv[slot, k].astype(F32) * cols[k] + cols[2 + k] * gain
        u_recv[slot, side] = jnp.maximum(total, 0.0).astype(BF16)
        mine = u_recv.at[slot, side]
        exchange(("u", slot), [(mine, mine, {"row": partner})], mine)

    def send_out(layer, stream):
        slot = layer * STREAMS + stream
        need(("wf2", layer))
        arrived(("u", slot))
        acc = dot(u_recv[slot, 0], wf2[layer, 0:FF_HALF, :]) + dot(u_recv[slot, 1], wf2[layer, FF_HALF:, :])
        out_recv[slot, col] = acc.astype(BF16)
        to_col(("out", slot), out_recv.at[slot])

    def finish(layer, stream):
        slot = layer * STREAMS + stream
        need("bf2")
        arrived(("out", slot))
        residual(col_sum(out_recv.at[slot]), bf2[layer:layer + 1, :].astype(F32), stream)

    for stream in range(STREAMS):
        send_qkv(0, stream)
    send_affine(0)
    send_affine(1)
    need("len")
    len_mat[...] = jnp.transpose(jnp.broadcast_to(len_buf[...].astype(F32), (128, 128)))
    for layer in range(LAYERS):
        for stream in range(STREAMS):
            attend(layer, stream)
        turned = jnp.transpose(kv_mix[layer]).astype(BF16)
        k_out[layer] = turned[0:HEAD]
        v_out[layer] = turned[HEAD:2 * HEAD]
        for stream in range(STREAMS):
            project(layer, stream)
        for stream in range(STREAMS):
            send_inner(layer, stream)
        for stream in range(STREAMS):
            send_pair(layer, stream)
        for stream in range(STREAMS):
            send_act(layer, stream)
        for stream in range(STREAMS):
            send_out(layer, stream)
        for stream in range(STREAMS):
            finish(layer, stream)
            if layer + 1 < LAYERS:
                send_qkv(layer + 1, stream)
            else:
                span = slice(stream * ROWS, (stream + 1) * ROWS)
                h_out[span, :] = x_buf[span, :]
    for copy in drains:
        copy.wait()


N_SLOT = LAYERS * STREAMS
N_COPY = 10 * N_SLOT + 2
N_PEER = N_ROW + N_COL - 2


def emit_kernel(h_in, k_in, v_in, h_out, k_out, v_out, sem):
    copies = [pltpu.make_async_copy(src, dst, sem.at[i])
              for i, (src, dst) in enumerate(((h_in, h_out), (k_in, k_out), (v_in, v_out)))]
    for copy in copies:
        copy.start()
    for copy in copies:
        copy.wait()


def run_step(x, lens, k_cache, v_cache, g1, b1, wq, bq, wk, bk, wv, bv, wo, bo, g2, b2, wf1, bf1, wf2, bf2):
    any_spec = pl.BlockSpec(memory_space=pl.ANY)
    args = (x, lens.reshape(1, BATCH),
            jnp.swapaxes(k_cache, 3, 4).reshape(LAYERS, BATCH * HEAD, SEQ),
            jnp.swapaxes(v_cache, 3, 4).reshape(LAYERS, BATCH * HEAD, SEQ),
            g1, b1, wq, bq, wk, bk, wv, bv, wo, bo, g2, b2, wf1, bf1, wf2, bf2)
    vm = pltpu.VMEM
    in_scratch = [vm(a.shape, a.dtype) for a in args]
    scratch = in_scratch + [
        vm((BATCH, 128), F32),
        vm((LAYERS, BATCH, 128), F32),
        vm((ROWS, SEQ), F32),
        vm((ROWS, SEQ), BF16),
        vm((ROWS, 128), F32),
        vm((2 * N_SLOT, 8, 128), F32),
        vm((2 * N_SLOT, N_ROW, 8, 128), F32),
        vm((N_ROW, 8, WIDTH), F32),
        vm((N_ROW, 8, WIDTH), F32),
        vm((2, 8, FF_HALF), F32),
        vm((N_ROW, 8, FF_HALF), F32),
        vm((N_SLOT, N_ROW, ROWS + HALF, 128), BF16),
        vm((N_SLOT, N_ROW, ROWS + HALF, 128), BF16),
        vm((N_SLOT, N_ROW, HALF, 128), BF16),
        vm((N_SLOT, N_COL, ROWS, WIDTH), BF16),
        vm((STREAMS, ROWS, FF_HALF), F32),
        vm((N_SLOT, ROWS, FF_HALF), BF16),
        vm((N_SLOT, ROWS, FF_HALF), BF16),
        vm((N_SLOT, 2, ROWS, FF_HALF), BF16),
        vm((N_SLOT, 2, ROWS, FF_HALF), BF16),
        vm((N_SLOT, N_COL, ROWS, WIDTH), BF16),
        pltpu.SemaphoreType.DMA((32,)),
        pltpu.SemaphoreType.DMA((2 * N_SLOT,)),
        pltpu.SemaphoreType.DMA((N_COPY,)),
        pltpu.SemaphoreType.DMA((N_COPY,)),
    ]
    shapes = (jax.ShapeDtypeStruct((BATCH, WIDTH), BF16),
              jax.ShapeDtypeStruct((LAYERS, HEAD, BATCH), BF16),
              jax.ShapeDtypeStruct((LAYERS, HEAD, BATCH), BF16))
    vmem_spec = pl.BlockSpec(memory_space=pltpu.VMEM)
    results = pl.pallas_call(
        step_kernel,
        out_shape=tuple(vm(a.shape, a.dtype) for a in shapes),
        in_specs=[pl.BlockSpec(memory_space=pltpu.HBM)] * len(args),
        out_specs=(vmem_spec,) * 3,
        scratch_shapes=scratch,
        compiler_params=pltpu.CompilerParams(
            collective_id=0, has_side_effects=True, vmem_limit_bytes=60 * 1024 * 1024),
        name="decode_step",
    )(*args)
    h_out, k_new, v_new = pl.pallas_call(
        emit_kernel,
        out_shape=shapes,
        in_specs=[vmem_spec] * 3,
        out_specs=(any_spec,) * 3,
        scratch_shapes=[pltpu.SemaphoreType.DMA((3,))],
        compiler_params=pltpu.CompilerParams(vmem_limit_bytes=1024 * 1024),
        name="emit",
    )(*results)

    def fresh(rows):
        return jnp.swapaxes(rows, 1, 2).reshape(LAYERS, BATCH, 1, HEAD)

    return h_out, fresh(k_new), fresh(v_new)


def solution(mesh):
    act_spec = P("dp", "row")
    cache_spec = P(None, "dp", ("col", "row"), None, None)
    fresh_spec = P(None, "dp", ("col", "row"), None)
    in_weight = P(None, "row", "col")
    out_weight = P(None, "col", "row")
    col_vec = P(None, "col")
    row_vec = P(None, "row")
    in_specs = (act_spec, P("dp"), cache_spec, cache_spec, row_vec, row_vec,
                in_weight, col_vec, in_weight, col_vec, in_weight, col_vec,
                out_weight, row_vec, row_vec, row_vec, in_weight, col_vec, out_weight, row_vec)
    return jax.shard_map(run_step, mesh=mesh, in_specs=in_specs,
                         out_specs=(act_spec, fresh_spec, fresh_spec), check_vma=False)
```

```python
import functools

import jax
import jax.numpy as jnp
from jax import lax
from jax.experimental import pallas as pl
from jax.experimental.pallas import tpu as pltpu
from jax.sharding import PartitionSpec as P

EPS_LN = 1e-5
MESH = pl.DeviceIdType.MESH
F32 = jnp.float32
BF16 = jnp.bfloat16

LAYERS = 2
BATCH = 128
STREAMS = 2
ROWS = BATCH // STREAMS
HALF = ROWS // 2
GROUP = 16
COL_PIECES = 2
N_ROW = 4
N_COL = 4
HEAD = 64
SEQ = 512
WIDTH = 256
D_MODEL = 1024
FF_LOC = 1024
FF_HALF = FF_LOC // 2

VEC_NAMES = ("g1", "b1", "bq", "bk", "bv", "bo", "g2", "b2", "bf2")
MAT_NAMES = ("wq", "wk", "wv", "wo", "wf1", "wf2")


def lane_iota(shape):
    return lax.broadcasted_iota(jnp.int32, shape, len(shape) - 1)


def swap_halves(val):
    return pltpu.roll(val, HEAD, 1)


def low_half(shape):
    return lane_iota(shape) < HEAD


def step_kernel(*refs):
    (x_in, len_in, k_in, v_in, g1_in, b1_in, wq_in, bq_in, wk_in, bk_in, wv_in, bv_in,
     wo_in, bo_in, g2_in, b2_in, wf1_in, bf1_in, wf2_in, bf2_in,
     h_out, k_out, v_out,
     x_buf, len_buf, k_buf, v_buf, g1, b1, wq, bq, wk, bk, wv, bv, wo, bo, g2, b2, wf1, bf1, wf2, bf2,
     len_mat, kv_mix, s_buf, p_buf, o_mix,
     st_send, st_recv, gq_send, gq_recv, gf_send, gf_recv, qkv_send, qkv_recv, o_recv,
     proj_recv, f1_mine, f1_send, f1_recv, pair_recv, u_recv, out_recv,
     load_sem, big_sem, send_sem, recv_sem) = refs

    row = lax.axis_index("row")
    col = lax.axis_index("col")
    side = lax.rem(row, 2)
    chip = row // 2
    partner = chip * 2 + (1 - side)
    across = lax.rem(row + 2, N_ROW)

    loads = {}

    def load(name, src, dst, sem):
        copy = pltpu.make_async_copy(src, dst, sem)
        copy.start()
        loads[name] = copy

    n_load = [0]

    def small(name, src, dst):
        load(name, src, dst, load_sem.at[n_load[0]])
        n_load[0] += 1

    small("x", x_in, x_buf)
    small("g1", g1_in, g1)
    for layer in range(LAYERS):
        for name, src, dst in (("wq", wq_in, wq), ("wk", wk_in, wk), ("wv", wv_in, wv)):
            if layer == 0:
                small((name, layer), src.at[layer], dst.at[layer])
    for name, src, dst in (("wq", wq_in, wq), ("wk", wk_in, wk), ("wv", wv_in, wv)):
        small((name, 1), src.at[1], dst.at[1])
    for name, src, dst in (("b1", b1_in, b1), ("bq", bq_in, bq), ("bk", bk_in, bk), ("bv", bv_in, bv),
                           ("len", len_in, len_buf), ("bo", bo_in, bo), ("g2", g2_in, g2), ("b2", b2_in, b2),
                           ("bf1", bf1_in, bf1), ("bf2", bf2_in, bf2)):
        small(name, src, dst)
    for layer in range(LAYERS):
        small(("wf1", layer), wf1_in.at[layer], wf1.at[layer])

    barrier = pltpu.get_barrier_semaphore()
    for off in range(1, 4):
        pl.semaphore_signal(barrier, inc=1, device_id={"row": lax.rem(row + off, N_ROW)}, device_id_type=MESH)
        pl.semaphore_signal(barrier, inc=1, device_id={"col": lax.rem(col + off, N_COL)}, device_id_type=MESH)

    def big(layer, stream, which):
        src, dst = (k_in, k_buf) if which == 0 else (v_in, v_buf)
        span = pl.ds(stream * ROWS * HEAD, ROWS * HEAD)
        load(("kv", layer, stream, which), src.at[layer, span], dst.at[layer, span],
             big_sem.at[(layer * STREAMS + stream) * 2 + which])

    for stream in range(STREAMS):
        for which in range(2):
            big(0, stream, which)
    for name, src, dst in (("wo", wo_in, wo), ("wf2", wf2_in, wf2)):
        small((name, 0), src.at[0], dst.at[0])
    for name, src, dst in (("wo", wo_in, wo), ("wf2", wf2_in, wf2)):
        small((name, 1), src.at[1], dst.at[1])
    for stream in range(STREAMS):
        for which in range(2):
            big(1, stream, which)

    waited = set()

    def need(name):
        if name not in waited:
            waited.add(name)
            loads[name].wait()

    drains = []
    recvs = {}
    n_sem = [0]

    def exchange(tag, copies, span):
        index = n_sem[0]
        n_sem[0] += 1
        for src, dst, device in copies:
            pltpu.make_async_remote_copy(
                src_ref=src, dst_ref=dst, send_sem=send_sem.at[index],
                recv_sem=recv_sem.at[index], device_id=device, device_id_type=MESH).start()
        drains.append(pltpu.make_async_copy(span, span, send_sem.at[index]))
        recvs[tag] = pltpu.make_async_copy(span, span, recv_sem.at[index])

    def to_col(tag, buf):
        peers = [lax.rem(col + off, N_COL) for off in (2, 3, 1)]
        rows = ROWS // COL_PIECES
        copies = []
        for piece in range(COL_PIECES):
            mine = buf.at[col, piece * rows:(piece + 1) * rows]
            copies += [(mine, mine, {"col": peer}) for peer in peers]
        exchange(tag, copies, buf.at[0:3])

    def to_axis(tag, axis, src_of, buf):
        me = row if axis == "row" else col
        dests = [lax.rem(me + off, 4) for off in (2, 3, 1)]
        exchange(tag, [(src_of(d), buf.at[me], {axis: d}) for d in dests], buf.at[0:3])

    def arrived(tag):
        recvs[tag].wait()

    def local_norm(state, gain):
        mean = jnp.sum(state, axis=-1, keepdims=True) * (1.0 / WIDTH)
        delta = state - mean
        var = jnp.sum(delta * delta, axis=-1, keepdims=True) * (1.0 / WIDTH)
        normed = (delta * lax.rsqrt(var + EPS_LN) * gain).astype(BF16)
        lanes = lane_iota((ROWS, 128))
        tile = jnp.where(lanes == 0, mean, jnp.where(lanes == 1, var, 0.0))
        if ROWS < 128:
            tile = jnp.concatenate([tile] * (128 // ROWS), axis=0)
        return normed, jnp.transpose(tile)[0:8]

    def merge_stats(blocks):
        share = 1.0 / len(blocks)
        mean = sum(m for m, _ in blocks) * share
        var = sum(v + (m - mean) * (m - mean) for m, v in blocks) * share
        return mean, var

    def stat_columns(blocks):
        mean, var = merge_stats(blocks)
        inv = lax.rsqrt(var + EPS_LN)
        lines = [jnp.sqrt(v + EPS_LN) * inv for _, v in blocks] + [(m - mean) * inv for m, _ in blocks]
        sub = lax.broadcasted_iota(jnp.int32, (8, 128), 0)
        tile = jnp.zeros((8, 128), F32)
        for i, line in enumerate(lines):
            tile = jnp.where(sub == i, line, tile)
        turned = jnp.transpose(jnp.concatenate([tile] * 16, axis=0))[0:ROWS]
        return [turned[:, i:i + 1] for i in range(len(lines))]

    def block_stats(index, r):
        tile = st_recv[index, r]
        return tile[0:1], tile[1:2]

    def pack_heads(q, k, v, j, rows):
        half = rows // 2
        lo = (j // 2) * 128
        q, k, v = q[:, lo:lo + 128], k[:, lo:lo + 128], v[:, lo:lo + 128]
        if j % 2 == 0:
            first = jnp.where(low_half((rows, 128)), q, swap_halves(k))
            second = jnp.where(low_half((half, 128)), v[:half], swap_halves(v[half:]))
        else:
            first = jnp.where(low_half((rows, 128)), swap_halves(q), k)
            second = jnp.where(low_half((half, 128)), swap_halves(v[:half]), v[half:])
        return first, second

    def dot(a, b):
        return jnp.dot(a, b, preferred_element_type=F32)

    def send_qkv(layer, stream):
        slot = layer * STREAMS + stream
        need("x")
        need("g1")
        state = x_buf[stream * ROWS:(stream + 1) * ROWS, :].astype(F32)
        normed, tile = local_norm(state, g1[layer:layer + 1, :].astype(F32))
        st_send[2 * slot] = tile
        st_recv[2 * slot, row] = tile
        for name in ("wq", "wk", "wv"):
            need((name, layer))
        q, k, v = dot(normed, wq[layer]), dot(normed, wk[layer]), dot(normed, wv[layer])
        for j in range(N_ROW):
            first, second = pack_heads(q, k, v, j, ROWS)
            qkv_send[slot, j, 0:ROWS] = first.astype(BF16)
            qkv_send[slot, j, ROWS:ROWS + HALF] = second.astype(BF16)
        qkv_recv[slot, row] = qkv_send[slot, row]
        if layer == 0 and stream == 0:
            pl.semaphore_wait(barrier, N_PEER)
        to_axis(("st1", slot), "row", lambda d: st_send.at[2 * slot], st_recv.at[2 * slot])
        to_axis(("qkv", slot), "row", lambda d: qkv_send.at[slot, d], qkv_recv.at[slot])

    def affine_rows(gains, shifts, layer):
        gain, shift = gains[layer:layer + 1, :].astype(F32), shifts[layer:layer + 1, :].astype(F32)
        sub = lax.broadcasted_iota(jnp.int32, (16, WIDTH), 0)
        return jnp.where(sub == 2 * layer, gain, jnp.where(sub == 2 * layer + 1, shift, 0.0)).astype(BF16)

    def send_affine(kind):
        bias_on = jnp.where(row == 0, 1.0, 0.0)

        def product(gains, shifts, w, b):
            total = None
            for layer in range(LAYERS):
                part = dot(affine_rows(gains, shifts, layer), w[layer])[0:8]
                sub = lax.broadcasted_iota(jnp.int32, part.shape, 0)
                part = part + jnp.where(sub == 2 * layer + 1, b[layer:layer + 1, :].astype(F32) * bias_on, 0.0)
                total = part if total is None else total + part
            return total

        if kind == 0:
            for name in ("b1", "bq", "bk", "bv", ("wq", 1), ("wk", 1), ("wv", 1)):
                need(name)
            q, k, v = product(g1, b1, wq, bq), product(g1, b1, wk, bk), product(g1, b1, wv, bv)
            for j in range(N_ROW):
                lo = (j // 2) * 128
                qj, kj, vj = q[:, lo:lo + 128], k[:, lo:lo + 128], v[:, lo:lo + 128]
                if j % 2 == 0:
                    first = jnp.where(low_half((8, 128)), qj, swap_halves(kj))
                else:
                    first = jnp.where(low_half((8, 128)), swap_halves(qj), kj)
                    vj = swap_halves(vj)
                second = jnp.where(low_half((8, 128)), vj, swap_halves(vj))
                gq_send[j] = jnp.concatenate([first, second], axis=1)
            gq_recv[row] = gq_send[row]
            to_axis(("gb", kind), "row", lambda d: gq_send.at[d], gq_recv)
        else:
            for name in ("g2", "b2", "bf1", ("wf1", 0), ("wf1", 1)):
                need(name)
            part = product(g2, b2, wf1, bf1)
            for j in range(2):
                gf_send[j] = part[:, j * FF_HALF:(j + 1) * FF_HALF]
            gf_recv[row] = gf_send[side]
            to_axis(("gb", kind), "row", lambda d: gf_send.at[lax.rem(d, 2)], gf_recv)

    gb_done = set()

    def affine_lines(kind):
        if kind not in gb_done:
            gb_done.add(kind)
            arrived(("gb", kind))

    def gain_line(buf, layer, r):
        return buf[r, 2 * layer:2 * layer + 1]

    def const_line(buf, layer):
        at = slice(2 * layer + 1, 2 * layer + 2)
        return buf[0, at] + buf[1, at] + buf[2, at] + buf[3, at]

    def attend(layer, stream):
        slot = layer * STREAMS + stream
        span = slice(stream * ROWS, (stream + 1) * ROWS)
        arrived(("st1", slot))
        cols = stat_columns([block_stats(2 * slot, r) for r in range(N_ROW)])
        affine_lines(0)
        gains = [gain_line(gq_recv, layer, r) for r in range(N_ROW)]
        const = const_line(gq_recv, layer)
        arrived(("qkv", slot))
        low = low_half((HALF, 128))
        qk = const[:, 0:128]
        vv = const[:, 128:256]
        for r in range(N_ROW):
            part = qkv_recv[slot, r].astype(F32)
            scale, shift = cols[r], cols[4 + r]
            qk = qk + part[0:ROWS] * scale + shift * gains[r][:, 0:128]
            scale_v = jnp.where(low, scale[0:HALF], scale[HALF:ROWS])
            shift_v = jnp.where(low, shift[0:HALF], shift[HALF:ROWS])
            vv = vv + part[ROWS:ROWS + HALF] * scale_v + shift_v * gains[r][:, 128:256]
        full_low = low_half((ROWS, 128))
        qk_turn = swap_halves(qk)
        q2 = (jnp.where(full_low, qk, qk_turn) * (HEAD ** -0.5)).astype(BF16)
        k2 = jnp.where(full_low, qk_turn, qk).astype(BF16)
        vv_turn = swap_halves(vv)
        v2 = jnp.concatenate([jnp.where(low, vv, vv_turn), jnp.where(low, vv_turn, vv)], axis=0).astype(BF16)
        kv_mix[layer, span, :] = jnp.where(full_low, k2.astype(F32), v2.astype(F32))
        score_new = jnp.sum(jnp.where(full_low, q2.astype(F32) * k2.astype(F32), 0.0), axis=-1, keepdims=True)

        need(("kv", layer, stream, 0))
        q_row = lax.broadcasted_iota(jnp.int32, (GROUP, 128), 0)
        q_half = lane_iota((GROUP, 128)) // HEAD
        for g in range(ROWS // GROUP):
            base = (stream * ROWS + g * GROUP) * HEAD
            qg = q2[g * GROUP:(g + 1) * GROUP].astype(F32)
            spread = [jnp.where(q_row == 2 * j + q_half, qg, 0.0).astype(BF16) for j in range(GROUP // 2)]
            s_buf[g * GROUP:(g + 1) * GROUP, :] = dot(jnp.concatenate(spread, axis=1),
                                                      k_buf[layer, base:base + GROUP * HEAD, :])
        positions = lane_iota((ROWS, SEQ)).astype(F32)
        limit = len_mat[span, 0:1]
        scores = jnp.where(positions < limit, s_buf[...], -jnp.inf)
        peak = jnp.maximum(jnp.max(scores, axis=-1, keepdims=True), score_new)
        exp_cache = jnp.exp(scores - peak)
        exp_new = jnp.exp(score_new - peak)
        inv = 1.0 / (jnp.sum(exp_cache, axis=-1, keepdims=True) + exp_new)
        p_buf[...] = (exp_cache * inv).astype(BF16)
        prob_new = (exp_new * inv).astype(BF16).astype(F32)

        need(("kv", layer, stream, 1))
        for g in range(ROWS // GROUP):
            base = (stream * ROWS + g * GROUP) * HEAD
            wide = lax.dot_general(p_buf[g * GROUP:(g + 1) * GROUP, :], v_buf[layer, base:base + GROUP * HEAD, :],
                                   (((1,), (1,)), ((), ())), preferred_element_type=F32)
            acc = jnp.zeros((GROUP, 128), F32)
            for j in range(GROUP // 2):
                acc = acc + jnp.where(q_row == 2 * j + q_half, wide[:, j * 128:(j + 1) * 128], 0.0)
            o_mix[g * GROUP:(g + 1) * GROUP, :] = acc + swap_halves(acc)
        o2 = o_mix[...] + prob_new * v2.astype(F32)
        packed = jnp.where(low, o2[0:HALF], o2[HALF:ROWS]).astype(BF16)
        o_recv[slot, row] = packed
        to_axis(("o", slot), "row", lambda d: o_recv.at[slot, row], o_recv.at[slot])

    def unpack_heads(buf, first):
        low = low_half((HALF, 128))
        parts = [buf[first + r].astype(F32) for r in range(N_ROW)]
        turns = [swap_halves(p) for p in parts]
        pairs = []
        for a, b in ((0, 1), (2, 3)):
            top = jnp.where(low, parts[a], turns[b])
            bottom = jnp.where(low, turns[a], parts[b])
            pairs.append(jnp.concatenate([top, bottom], axis=0).astype(BF16))
        return jnp.concatenate(pairs, axis=1)

    def project(layer, stream):
        slot = layer * STREAMS + stream
        need(("wo", layer))
        arrived(("o", slot))
        proj_recv[slot, col] = dot(unpack_heads(o_recv.at[slot], 0), wo[layer]).astype(BF16)
        to_col(("proj", slot), proj_recv.at[slot])

    def col_sum(buf):
        total = buf[0].astype(F32)
        for c in range(1, N_COL):
            total = total + buf[c].astype(F32)
        return total

    def residual(total, bias, stream):
        span = slice(stream * ROWS, (stream + 1) * ROWS)
        new = (x_buf[span, :].astype(F32) + (total + bias)).astype(BF16)
        x_buf[span, :] = new
        return new.astype(F32)

    def send_inner(layer, stream):
        slot = layer * STREAMS + stream
        need("bo")
        need("g2")
        need(("wf1", layer))
        arrived(("proj", slot))
        total = col_sum(proj_recv.at[slot])
        state = residual(total, bo[layer:layer + 1, :].astype(F32), stream)
        normed, tile = local_norm(state, g2[layer:layer + 1, :].astype(F32))
        index = 2 * slot + 1
        st_send[index] = tile
        st_recv[index, row] = tile
        mine = st_send.at[index]
        spot = st_recv.at[index, row]
        exchange(("st2", slot), [(mine, spot, {"row": partner})], mine)
        far = lax.rem(partner + 2, N_ROW)
        exchange(("st3", slot), [(mine, spot, {"row": across}), (mine, spot, {"row": far})], st_recv.at[index, 0:2])
        theirs = pl.ds(pl.multiple_of((1 - side) * FF_HALF, FF_HALF), FF_HALF)
        f1_send[slot] = dot(normed, wf1[layer, :, theirs]).astype(BF16)
        exchange(("f1", slot), [(f1_send.at[slot], f1_recv.at[slot], {"row": partner})], f1_recv.at[slot])
        ours = pl.ds(pl.multiple_of(side * FF_HALF, FF_HALF), FF_HALF)
        f1_mine[stream] = dot(normed, wf1[layer, :, ours])

    def send_pair(layer, stream):
        slot = layer * STREAMS + stream
        arrived(("st2", slot))
        cols = stat_columns([block_stats(2 * slot + 1, r) for r in (row, partner)])
        affine_lines(1)
        arrived(("f1", slot))
        total = f1_mine[stream] * cols[0] + cols[2] * gain_line(gf_recv, layer, row)
        total = total + f1_recv[slot].astype(F32) * cols[1] + cols[3] * gain_line(gf_recv, layer, partner)
        pair_recv[slot, chip] = total.astype(BF16)
        mine = pair_recv.at[slot, chip]
        exchange(("pair", slot), [(mine, mine, {"row": across})], mine)

    def send_act(layer, stream):
        slot = layer * STREAMS + stream
        arrived(("st3", slot))
        pairs = [merge_stats([block_stats(2 * slot + 1, 2 * k + r) for r in range(2)]) for k in range(2)]
        cols = stat_columns(pairs)
        total = const_line(gf_recv, layer)
        arrived(("pair", slot))
        for k in range(2):
            gain = gain_line(gf_recv, layer, 2 * k) + gain_line(gf_recv, layer, 2 * k + 1)
            total = total + pair_recv[slot, k].astype(F32) * cols[k] + cols[2 + k] * gain
        u_recv[slot, side] = jnp.maximum(total, 0.0).astype(BF16)
        mine = u_recv.at[slot, side]
        exchange(("u", slot), [(mine, mine, {"row": partner})], mine)

    def send_out(layer, stream):
        slot = layer * STREAMS + stream
        need(("wf2", layer))
        arrived(("u", slot))
        acc = dot(u_recv[slot, 0], wf2[layer, 0:FF_HALF, :]) + dot(u_recv[slot, 1], wf2[layer, FF_HALF:, :])
        out_recv[slot, col] = acc.astype(BF16)
        to_col(("out", slot), out_recv.at[slot])

    def finish(layer, stream):
        slot = layer * STREAMS + stream
        need("bf2")
        arrived(("out", slot))
        residual(col_sum(out_recv.at[slot]), bf2[layer:layer + 1, :].astype(F32), stream)

    for stream in range(STREAMS):
        send_qkv(0, stream)
    send_affine(0)
    send_affine(1)
    need("len")
    len_mat[...] = jnp.transpose(jnp.broadcast_to(len_buf[...].astype(F32), (128, 128)))
    for layer in range(LAYERS):
        for stream in range(STREAMS):
            attend(layer, stream)
        turned = jnp.transpose(kv_mix[layer]).astype(BF16)
        k_out[layer] = turned[0:HEAD]
        v_out[layer] = turned[HEAD:2 * HEAD]
        for stream in range(STREAMS):
            project(layer, stream)
        for stream in range(STREAMS):
            send_inner(layer, stream)
        for stream in range(STREAMS):
            send_pair(layer, stream)
        for stream in range(STREAMS):
            send_act(layer, stream)
        for stream in range(STREAMS):
            send_out(layer, stream)
        for stream in range(STREAMS):
            finish(layer, stream)
            if layer + 1 < LAYERS:
                send_qkv(layer + 1, stream)
            else:
                span = slice(stream * ROWS, (stream + 1) * ROWS)
                h_out[span, :] = x_buf[span, :]
    for copy in drains:
        copy.wait()


N_SLOT = LAYERS * STREAMS
N_COPY = 10 * N_SLOT + 2
N_PEER = N_ROW + N_COL - 2


def emit_kernel(h_in, k_in, v_in, h_out, k_out, v_out, sem):
    copies = [pltpu.make_async_copy(src, dst, sem.at[i])
              for i, (src, dst) in enumerate(((h_in, h_out), (k_in, k_out), (v_in, v_out)))]
    for copy in copies:
        copy.start()
    for copy in copies:
        copy.wait()


def run_step(x, lens, k_cache, v_cache, g1, b1, wq, bq, wk, bk, wv, bv, wo, bo, g2, b2, wf1, bf1, wf2, bf2):
    any_spec = pl.BlockSpec(memory_space=pl.ANY)
    args = (x, lens.reshape(1, BATCH),
            jnp.swapaxes(k_cache, 3, 4).reshape(LAYERS, BATCH * HEAD, SEQ),
            jnp.swapaxes(v_cache, 3, 4).reshape(LAYERS, BATCH * HEAD, SEQ),
            g1, b1, wq, bq, wk, bk, wv, bv, wo, bo, g2, b2, wf1, bf1, wf2, bf2)
    vm = pltpu.VMEM
    in_scratch = [vm(a.shape, a.dtype) for a in args]
    scratch = in_scratch + [
        vm((BATCH, 128), F32),
        vm((LAYERS, BATCH, 128), F32),
        vm((ROWS, SEQ), F32),
        vm((ROWS, SEQ), BF16),
        vm((ROWS, 128), F32),
        vm((2 * N_SLOT, 8, 128), F32),
        vm((2 * N_SLOT, N_ROW, 8, 128), F32),
        vm((N_ROW, 8, WIDTH), F32),
        vm((N_ROW, 8, WIDTH), F32),
        vm((2, 8, FF_HALF), F32),
        vm((N_ROW, 8, FF_HALF), F32),
        vm((N_SLOT, N_ROW, ROWS + HALF, 128), BF16),
        vm((N_SLOT, N_ROW, ROWS + HALF, 128), BF16),
        vm((N_SLOT, N_ROW, HALF, 128), BF16),
        vm((N_SLOT, N_COL, ROWS, WIDTH), BF16),
        vm((STREAMS, ROWS, FF_HALF), F32),
        vm((N_SLOT, ROWS, FF_HALF), BF16),
        vm((N_SLOT, ROWS, FF_HALF), BF16),
        vm((N_SLOT, 2, ROWS, FF_HALF), BF16),
        vm((N_SLOT, 2, ROWS, FF_HALF), BF16),
        vm((N_SLOT, N_COL, ROWS, WIDTH), BF16),
        pltpu.SemaphoreType.DMA((32,)),
        pltpu.SemaphoreType.DMA((2 * N_SLOT,)),
        pltpu.SemaphoreType.DMA((N_COPY,)),
        pltpu.SemaphoreType.DMA((N_COPY,)),
    ]
    shapes = (jax.ShapeDtypeStruct((BATCH, WIDTH), BF16),
              jax.ShapeDtypeStruct((LAYERS, HEAD, BATCH), BF16),
              jax.ShapeDtypeStruct((LAYERS, HEAD, BATCH), BF16))
    vmem_spec = pl.BlockSpec(memory_space=pltpu.VMEM)
    results = pl.pallas_call(
        step_kernel,
        out_shape=tuple(vm(a.shape, a.dtype) for a in shapes),
        in_specs=[pl.BlockSpec(memory_space=pltpu.HBM)] * len(args),
        out_specs=(vmem_spec,) * 3,
        scratch_shapes=scratch,
        compiler_params=pltpu.CompilerParams(
            collective_id=0, has_side_effects=True, vmem_limit_bytes=60 * 1024 * 1024),
        name="decode_step",
    )(*args)
    h_out, k_new, v_new = pl.pallas_call(
        emit_kernel,
        out_shape=shapes,
        in_specs=[vmem_spec] * 3,
        out_specs=(any_spec,) * 3,
        scratch_shapes=[pltpu.SemaphoreType.DMA((3,))],
        compiler_params=pltpu.CompilerParams(vmem_limit_bytes=1024 * 1024),
        name="emit",
    )(*results)

    def fresh(rows):
        return jnp.swapaxes(rows, 1, 2).reshape(LAYERS, BATCH, 1, HEAD)

    return h_out, fresh(k_new), fresh(v_new)


def solution(mesh):
    act_spec = P("dp", "row")
    cache_spec = P(None, "dp", ("col", "row"), None, None)
    fresh_spec = P(None, "dp", ("col", "row"), None)
    in_weight = P(None, "row", "col")
    out_weight = P(None, "col", "row")
    col_vec = P(None, "col")
    row_vec = P(None, "row")
    in_specs = (act_spec, P("dp"), cache_spec, cache_spec, row_vec, row_vec,
                in_weight, col_vec, in_weight, col_vec, in_weight, col_vec,
                out_weight, row_vec, row_vec, row_vec, in_weight, col_vec, out_weight, row_vec)
    return jax.shard_map(run_step, mesh=mesh, in_specs=in_specs,
                         out_specs=(act_spec, fresh_spec, fresh_spec), check_vma=False)
```

```python
import functools

import jax
import jax.numpy as jnp
from jax import lax
from jax.experimental import pallas as pl
from jax.experimental.pallas import tpu as pltpu
from jax.sharding import PartitionSpec as P

EPS_LN = 1e-5
MESH = pl.DeviceIdType.MESH
F32 = jnp.float32
BF16 = jnp.bfloat16

LAYERS = 2
BATCH = 128
STREAMS = 2
ROWS = BATCH // STREAMS
HALF = ROWS // 2
GROUP = 16
COL_PIECES = 1
N_ROW = 4
N_COL = 4
HEAD = 64
SEQ = 512
WIDTH = 256
D_MODEL = 1024
FF_LOC = 1024
FF_HALF = FF_LOC // 2

VEC_NAMES = ("g1", "b1", "bq", "bk", "bv", "bo", "g2", "b2", "bf2")
MAT_NAMES = ("wq", "wk", "wv", "wo", "wf1", "wf2")


def lane_iota(shape):
    return lax.broadcasted_iota(jnp.int32, shape, len(shape) - 1)


def swap_halves(val):
    return pltpu.roll(val, HEAD, 1)


def low_half(shape):
    return lane_iota(shape) < HEAD


def step_kernel(*refs):
    (x_in, len_in, k_in, v_in, g1_in, b1_in, wq_in, bq_in, wk_in, bk_in, wv_in, bv_in,
     wo_in, bo_in, g2_in, b2_in, wf1_in, bf1_in, wf2_in, bf2_in,
     h_out, k_out, v_out,
     x_buf, len_buf, k_buf, v_buf, g1, b1, wq, bq, wk, bk, wv, bv, wo, bo, g2, b2, wf1, bf1, wf2, bf2,
     len_mat, kv_mix, s_buf, p_buf, o_mix,
     st_send, st_recv, gq_send, gq_recv, gf_send, gf_recv, qkv_send, qkv_recv, o_recv,
     proj_recv, f1_mine, f1_send, f1_recv, pair_recv, u_recv, out_recv,
     load_sem, big_sem, send_sem, recv_sem) = refs

    row = lax.axis_index("row")
    col = lax.axis_index("col")
    side = lax.rem(row, 2)
    chip = row // 2
    partner = chip * 2 + (1 - side)
    across = lax.rem(row + 2, N_ROW)

    loads = {}

    def load(name, src, dst, sem):
        copy = pltpu.make_async_copy(src, dst, sem)
        copy.start()
        loads[name] = copy

    n_load = [0]

    def small(name, src, dst):
        load(name, src, dst, load_sem.at[n_load[0]])
        n_load[0] += 1

    small("x", x_in, x_buf)
    small("g1", g1_in, g1)
    for layer in range(LAYERS):
        for name, src, dst in (("wq", wq_in, wq), ("wk", wk_in, wk), ("wv", wv_in, wv)):
            if layer == 0:
                small((name, layer), src.at[layer], dst.at[layer])
    for name, src, dst in (("wq", wq_in, wq), ("wk", wk_in, wk), ("wv", wv_in, wv)):
        small((name, 1), src.at[1], dst.at[1])
    for name, src, dst in (("b1", b1_in, b1), ("bq", bq_in, bq), ("bk", bk_in, bk), ("bv", bv_in, bv),
                           ("len", len_in, len_buf), ("bo", bo_in, bo), ("g2", g2_in, g2), ("b2", b2_in, b2),
                           ("bf1", bf1_in, bf1), ("bf2", bf2_in, bf2)):
        small(name, src, dst)
    for layer in range(LAYERS):
        small(("wf1", layer), wf1_in.at[layer], wf1.at[layer])

    barrier = pltpu.get_barrier_semaphore()
    for off in range(1, 4):
        pl.semaphore_signal(barrier, inc=1, device_id={"row": lax.rem(row + off, N_ROW)}, device_id_type=MESH)
        pl.semaphore_signal(barrier, inc=1, device_id={"col": lax.rem(col + off, N_COL)}, device_id_type=MESH)

    def big(layer, stream, which):
        src, dst = (k_in, k_buf) if which == 0 else (v_in, v_buf)
        span = pl.ds(stream * ROWS * HEAD, ROWS * HEAD)
        load(("kv", layer, stream, which), src.at[layer, span], dst.at[layer, span],
             big_sem.at[(layer * STREAMS + stream) * 2 + which])

    for stream in range(STREAMS):
        for which in range(2):
            big(0, stream, which)
    for name, src, dst in (("wo", wo_in, wo), ("wf2", wf2_in, wf2)):
        small((name, 0), src.at[0], dst.at[0])
    for name, src, dst in (("wo", wo_in, wo), ("wf2", wf2_in, wf2)):
        small((name, 1), src.at[1], dst.at[1])
    for stream in range(STREAMS):
        for which in range(2):
            big(1, stream, which)

    waited = set()

    def need(name):
        if name not in waited:
            waited.add(name)
            loads[name].wait()

    drains = []
    recvs = {}
    n_sem = [0]

    def exchange(tag, copies, span):
        index = n_sem[0]
        n_sem[0] += 1
        for src, dst, device in copies:
            pltpu.make_async_remote_copy(
                src_ref=src, dst_ref=dst, send_sem=send_sem.at[index],
                recv_sem=recv_sem.at[index], device_id=device, device_id_type=MESH).start()
        drains.append(pltpu.make_async_copy(span, span, send_sem.at[index]))
        recvs[tag] = pltpu.make_async_copy(span, span, recv_sem.at[index])

    def to_col(tag, buf):
        peers = (3 - col, lax.rem(col + 2, N_COL), col + 1 - 2 * lax.rem(col, 2))
        rows = ROWS // COL_PIECES
        copies = []
        for piece in range(COL_PIECES):
            mine = buf.at[col, piece * rows:(piece + 1) * rows]
            copies += [(mine, mine, {"col": peer}) for peer in peers]
        exchange(tag, copies, buf.at[0:3])

    def to_axis(tag, axis, src_of, buf):
        me = row if axis == "row" else col
        dests = [lax.rem(me + off, 4) for off in (2, 3, 1)]
        exchange(tag, [(src_of(d), buf.at[me], {axis: d}) for d in dests], buf.at[0:3])

    def arrived(tag):
        recvs[tag].wait()

    def local_norm(state, gain):
        mean = jnp.sum(state, axis=-1, keepdims=True) * (1.0 / WIDTH)
        delta = state - mean
        var = jnp.sum(delta * delta, axis=-1, keepdims=True) * (1.0 / WIDTH)
        normed = (delta * lax.rsqrt(var + EPS_LN) * gain).astype(BF16)
        lanes = lane_iota((ROWS, 128))
        tile = jnp.where(lanes == 0, mean, jnp.where(lanes == 1, var, 0.0))
        if ROWS < 128:
            tile = jnp.concatenate([tile] * (128 // ROWS), axis=0)
        return normed, jnp.transpose(tile)[0:8]

    def merge_stats(blocks):
        share = 1.0 / len(blocks)
        mean = sum(m for m, _ in blocks) * share
        var = sum(v + (m - mean) * (m - mean) for m, v in blocks) * share
        return mean, var

    def stat_columns(blocks):
        mean, var = merge_stats(blocks)
        inv = lax.rsqrt(var + EPS_LN)
        lines = [jnp.sqrt(v + EPS_LN) * inv for _, v in blocks] + [(m - mean) * inv for m, _ in blocks]
        sub = lax.broadcasted_iota(jnp.int32, (8, 128), 0)
        tile = jnp.zeros((8, 128), F32)
        for i, line in enumerate(lines):
            tile = jnp.where(sub == i, line, tile)
        turned = jnp.transpose(jnp.concatenate([tile] * 16, axis=0))[0:ROWS]
        return [turned[:, i:i + 1] for i in range(len(lines))]

    def block_stats(index, r):
        tile = st_recv[index, r]
        return tile[0:1], tile[1:2]

    def pack_heads(q, k, v, j, rows):
        half = rows // 2
        lo = (j // 2) * 128
        q, k, v = q[:, lo:lo + 128], k[:, lo:lo + 128], v[:, lo:lo + 128]
        if j % 2 == 0:
            first = jnp.where(low_half((rows, 128)), q, swap_halves(k))
            second = jnp.where(low_half((half, 128)), v[:half], swap_halves(v[half:]))
        else:
            first = jnp.where(low_half((rows, 128)), swap_halves(q), k)
            second = jnp.where(low_half((half, 128)), swap_halves(v[:half]), v[half:])
        return first, second

    def dot(a, b):
        return jnp.dot(a, b, preferred_element_type=F32)

    def send_qkv(layer, stream):
        slot = layer * STREAMS + stream
        need("x")
        need("g1")
        state = x_buf[stream * ROWS:(stream + 1) * ROWS, :].astype(F32)
        normed, tile = local_norm(state, g1[layer:layer + 1, :].astype(F32))
        st_send[2 * slot] = tile
        st_recv[2 * slot, row] = tile
        for name in ("wq", "wk", "wv"):
            need((name, layer))
        q, k, v = dot(normed, wq[layer]), dot(normed, wk[layer]), dot(normed, wv[layer])
        for j in range(N_ROW):
            first, second = pack_heads(q, k, v, j, ROWS)
            qkv_send[slot, j, 0:ROWS] = first.astype(BF16)
            qkv_send[slot, j, ROWS:ROWS + HALF] = second.astype(BF16)
        qkv_recv[slot, row] = qkv_send[slot, row]
        if layer == 0 and stream == 0:
            pl.semaphore_wait(barrier, N_PEER)
        to_axis(("st1", slot), "row", lambda d: st_send.at[2 * slot], st_recv.at[2 * slot])
        to_axis(("qkv", slot), "row", lambda d: qkv_send.at[slot, d], qkv_recv.at[slot])

    def affine_rows(gains, shifts, layer):
        gain, shift = gains[layer:layer + 1, :].astype(F32), shifts[layer:layer + 1, :].astype(F32)
        sub = lax.broadcasted_iota(jnp.int32, (16, WIDTH), 0)
        return jnp.where(sub == 2 * layer, gain, jnp.where(sub == 2 * layer + 1, shift, 0.0)).astype(BF16)

    def send_affine(kind):
        bias_on = jnp.where(row == 0, 1.0, 0.0)

        def product(gains, shifts, w, b):
            total = None
            for layer in range(LAYERS):
                part = dot(affine_rows(gains, shifts, layer), w[layer])[0:8]
                sub = lax.broadcasted_iota(jnp.int32, part.shape, 0)
                part = part + jnp.where(sub == 2 * layer + 1, b[layer:layer + 1, :].astype(F32) * bias_on, 0.0)
                total = part if total is None else total + part
            return total

        if kind == 0:
            for name in ("b1", "bq", "bk", "bv", ("wq", 1), ("wk", 1), ("wv", 1)):
                need(name)
            q, k, v = product(g1, b1, wq, bq), product(g1, b1, wk, bk), product(g1, b1, wv, bv)
            for j in range(N_ROW):
                lo = (j // 2) * 128
                qj, kj, vj = q[:, lo:lo + 128], k[:, lo:lo + 128], v[:, lo:lo + 128]
                if j % 2 == 0:
                    first = jnp.where(low_half((8, 128)), qj, swap_halves(kj))
                else:
                    first = jnp.where(low_half((8, 128)), swap_halves(qj), kj)
                    vj = swap_halves(vj)
                second = jnp.where(low_half((8, 128)), vj, swap_halves(vj))
                gq_send[j] = jnp.concatenate([first, second], axis=1)
            gq_recv[row] = gq_send[row]
            to_axis(("gb", kind), "row", lambda d: gq_send.at[d], gq_recv)
        else:
            for name in ("g2", "b2", "bf1", ("wf1", 0), ("wf1", 1)):
                need(name)
            part = product(g2, b2, wf1, bf1)
            for j in range(2):
                gf_send[j] = part[:, j * FF_HALF:(j + 1) * FF_HALF]
            gf_recv[row] = gf_send[side]
            to_axis(("gb", kind), "row", lambda d: gf_send.at[lax.rem(d, 2)], gf_recv)

    gb_done = set()

    def affine_lines(kind):
        if kind not in gb_done:
            gb_done.add(kind)
            arrived(("gb", kind))

    def gain_line(buf, layer, r):
        return buf[r, 2 * layer:2 * layer + 1]

    def const_line(buf, layer):
        at = slice(2 * layer + 1, 2 * layer + 2)
        return buf[0, at] + buf[1, at] + buf[2, at] + buf[3, at]

    def attend(layer, stream):
        slot = layer * STREAMS + stream
        span = slice(stream * ROWS, (stream + 1) * ROWS)
        arrived(("st1", slot))
        cols = stat_columns([block_stats(2 * slot, r) for r in range(N_ROW)])
        affine_lines(0)
        gains = [gain_line(gq_recv, layer, r) for r in range(N_ROW)]
        const = const_line(gq_recv, layer)
        arrived(("qkv", slot))
        low = low_half((HALF, 128))
        qk = const[:, 0:128]
        vv = const[:, 128:256]
        for r in range(N_ROW):
            part = qkv_recv[slot, r].astype(F32)
            scale, shift = cols[r], cols[4 + r]
            qk = qk + part[0:ROWS] * scale + shift * gains[r][:, 0:128]
            scale_v = jnp.where(low, scale[0:HALF], scale[HALF:ROWS])
            shift_v = jnp.where(low, shift[0:HALF], shift[HALF:ROWS])
            vv = vv + part[ROWS:ROWS + HALF] * scale_v + shift_v * gains[r][:, 128:256]
        full_low = low_half((ROWS, 128))
        qk_turn = swap_halves(qk)
        q2 = (jnp.where(full_low, qk, qk_turn) * (HEAD ** -0.5)).astype(BF16)
        k2 = jnp.where(full_low, qk_turn, qk).astype(BF16)
        vv_turn = swap_halves(vv)
        v2 = jnp.concatenate([jnp.where(low, vv, vv_turn), jnp.where(low, vv_turn, vv)], axis=0).astype(BF16)
        kv_mix[layer, span, :] = jnp.where(full_low, k2.astype(F32), v2.astype(F32))
        score_new = jnp.sum(jnp.where(full_low, q2.astype(F32) * k2.astype(F32), 0.0), axis=-1, keepdims=True)

        need(("kv", layer, stream, 0))
        q_row = lax.broadcasted_iota(jnp.int32, (GROUP, 128), 0)
        q_half = lane_iota((GROUP, 128)) // HEAD
        for g in range(ROWS // GROUP):
            base = (stream * ROWS + g * GROUP) * HEAD
            qg = q2[g * GROUP:(g + 1) * GROUP].astype(F32)
            spread = [jnp.where(q_row == 2 * j + q_half, qg, 0.0).astype(BF16) for j in range(GROUP // 2)]
            s_buf[g * GROUP:(g + 1) * GROUP, :] = dot(jnp.concatenate(spread, axis=1),
                                                      k_buf[layer, base:base + GROUP * HEAD, :])
        positions = lane_iota((ROWS, SEQ)).astype(F32)
        limit = len_mat[span, 0:1]
        scores = jnp.where(positions < limit, s_buf[...], -jnp.inf)
        peak = jnp.maximum(jnp.max(scores, axis=-1, keepdims=True), score_new)
        exp_cache = jnp.exp(scores - peak)
        exp_new = jnp.exp(score_new - peak)
        inv = 1.0 / (jnp.sum(exp_cache, axis=-1, keepdims=True) + exp_new)
        p_buf[...] = (exp_cache * inv).astype(BF16)
        prob_new = (exp_new * inv).astype(BF16).astype(F32)

        need(("kv", layer, stream, 1))
        for g in range(ROWS // GROUP):
            base = (stream * ROWS + g * GROUP) * HEAD
            wide = lax.dot_general(p_buf[g * GROUP:(g + 1) * GROUP, :], v_buf[layer, base:base + GROUP * HEAD, :],
                                   (((1,), (1,)), ((), ())), preferred_element_type=F32)
            acc = jnp.zeros((GROUP, 128), F32)
            for j in range(GROUP // 2):
                acc = acc + jnp.where(q_row == 2 * j + q_half, wide[:, j * 128:(j + 1) * 128], 0.0)
            o_mix[g * GROUP:(g + 1) * GROUP, :] = acc + swap_halves(acc)
        o2 = o_mix[...] + prob_new * v2.astype(F32)
        packed = jnp.where(low, o2[0:HALF], o2[HALF:ROWS]).astype(BF16)
        o_recv[slot, row] = packed
        to_axis(("o", slot), "row", lambda d: o_recv.at[slot, row], o_recv.at[slot])

    def unpack_heads(buf, first):
        low = low_half((HALF, 128))
        parts = [buf[first + r].astype(F32) for r in range(N_ROW)]
        turns = [swap_halves(p) for p in parts]
        pairs = []
        for a, b in ((0, 1), (2, 3)):
            top = jnp.where(low, parts[a], turns[b])
            bottom = jnp.where(low, turns[a], parts[b])
            pairs.append(jnp.concatenate([top, bottom], axis=0).astype(BF16))
        return jnp.concatenate(pairs, axis=1)

    def project(layer, stream):
        slot = layer * STREAMS + stream
        need(("wo", layer))
        arrived(("o", slot))
        proj_recv[slot, col] = dot(unpack_heads(o_recv.at[slot], 0), wo[layer]).astype(BF16)
        to_col(("proj", slot), proj_recv.at[slot])

    def col_sum(buf):
        total = buf[0].astype(F32)
        for c in range(1, N_COL):
            total = total + buf[c].astype(F32)
        return total

    def residual(total, bias, stream):
        span = slice(stream * ROWS, (stream + 1) * ROWS)
        new = (x_buf[span, :].astype(F32) + (total + bias)).astype(BF16)
        x_buf[span, :] = new
        return new.astype(F32)

    def send_inner(layer, stream):
        slot = layer * STREAMS + stream
        need("bo")
        need("g2")
        need(("wf1", layer))
        arrived(("proj", slot))
        total = col_sum(proj_recv.at[slot])
        state = residual(total, bo[layer:layer + 1, :].astype(F32), stream)
        normed, tile = local_norm(state, g2[layer:layer + 1, :].astype(F32))
        index = 2 * slot + 1
        st_send[index] = tile
        st_recv[index, row] = tile
        mine = st_send.at[index]
        spot = st_recv.at[index, row]
        exchange(("st2", slot), [(mine, spot, {"row": partner})], mine)
        far = lax.rem(partner + 2, N_ROW)
        exchange(("st3", slot), [(mine, spot, {"row": across}), (mine, spot, {"row": far})], st_recv.at[index, 0:2])
        theirs = pl.ds(pl.multiple_of((1 - side) * FF_HALF, FF_HALF), FF_HALF)
        f1_send[slot] = dot(normed, wf1[layer, :, theirs]).astype(BF16)
        exchange(("f1", slot), [(f1_send.at[slot], f1_recv.at[slot], {"row": partner})], f1_recv.at[slot])
        ours = pl.ds(pl.multiple_of(side * FF_HALF, FF_HALF), FF_HALF)
        f1_mine[stream] = dot(normed, wf1[layer, :, ours])

    def send_pair(layer, stream):
        slot = layer * STREAMS + stream
        arrived(("st2", slot))
        cols = stat_columns([block_stats(2 * slot + 1, r) for r in (row, partner)])
        affine_lines(1)
        arrived(("f1", slot))
        total = f1_mine[stream] * cols[0] + cols[2] * gain_line(gf_recv, layer, row)
        total = total + f1_recv[slot].astype(F32) * cols[1] + cols[3] * gain_line(gf_recv, layer, partner)
        pair_recv[slot, chip] = total.astype(BF16)
        mine = pair_recv.at[slot, chip]
        exchange(("pair", slot), [(mine, mine, {"row": across})], mine)

    def send_act(layer, stream):
        slot = layer * STREAMS + stream
        arrived(("st3", slot))
        pairs = [merge_stats([block_stats(2 * slot + 1, 2 * k + r) for r in range(2)]) for k in range(2)]
        cols = stat_columns(pairs)
        total = const_line(gf_recv, layer)
        arrived(("pair", slot))
        for k in range(2):
            gain = gain_line(gf_recv, layer, 2 * k) + gain_line(gf_recv, layer, 2 * k + 1)
            total = total + pair_recv[slot, k].astype(F32) * cols[k] + cols[2 + k] * gain
        u_recv[slot, side] = jnp.maximum(total, 0.0).astype(BF16)
        mine = u_recv.at[slot, side]
        exchange(("u", slot), [(mine, mine, {"row": partner})], mine)

    def send_out(layer, stream):
        slot = layer * STREAMS + stream
        need(("wf2", layer))
        arrived(("u", slot))
        acc = dot(u_recv[slot, 0], wf2[layer, 0:FF_HALF, :]) + dot(u_recv[slot, 1], wf2[layer, FF_HALF:, :])
        out_recv[slot, col] = acc.astype(BF16)
        to_col(("out", slot), out_recv.at[slot])

    def finish(layer, stream):
        slot = layer * STREAMS + stream
        need("bf2")
        arrived(("out", slot))
        residual(col_sum(out_recv.at[slot]), bf2[layer:layer + 1, :].astype(F32), stream)

    for stream in range(STREAMS):
        send_qkv(0, stream)
    send_affine(0)
    send_affine(1)
    need("len")
    len_mat[...] = jnp.transpose(jnp.broadcast_to(len_buf[...].astype(F32), (128, 128)))
    for layer in range(LAYERS):
        for stream in range(STREAMS):
            attend(layer, stream)
        turned = jnp.transpose(kv_mix[layer]).astype(BF16)
        k_out[layer] = turned[0:HEAD]
        v_out[layer] = turned[HEAD:2 * HEAD]
        for stream in range(STREAMS):
            project(layer, stream)
        for stream in range(STREAMS):
            send_inner(layer, stream)
        for stream in range(STREAMS):
            send_pair(layer, stream)
        for stream in range(STREAMS):
            send_act(layer, stream)
        for stream in range(STREAMS):
            send_out(layer, stream)
        for stream in range(STREAMS):
            finish(layer, stream)
            if layer + 1 < LAYERS:
                send_qkv(layer + 1, stream)
            else:
                span = slice(stream * ROWS, (stream + 1) * ROWS)
                h_out[span, :] = x_buf[span, :]
    for copy in drains:
        copy.wait()


N_SLOT = LAYERS * STREAMS
N_COPY = 10 * N_SLOT + 2
N_PEER = N_ROW + N_COL - 2


def emit_kernel(h_in, k_in, v_in, h_out, k_out, v_out, sem):
    copies = [pltpu.make_async_copy(src, dst, sem.at[i])
              for i, (src, dst) in enumerate(((h_in, h_out), (k_in, k_out), (v_in, v_out)))]
    for copy in copies:
        copy.start()
    for copy in copies:
        copy.wait()


def run_step(x, lens, k_cache, v_cache, g1, b1, wq, bq, wk, bk, wv, bv, wo, bo, g2, b2, wf1, bf1, wf2, bf2):
    any_spec = pl.BlockSpec(memory_space=pl.ANY)
    args = (x, lens.reshape(1, BATCH),
            jnp.swapaxes(k_cache, 3, 4).reshape(LAYERS, BATCH * HEAD, SEQ),
            jnp.swapaxes(v_cache, 3, 4).reshape(LAYERS, BATCH * HEAD, SEQ),
            g1, b1, wq, bq, wk, bk, wv, bv, wo, bo, g2, b2, wf1, bf1, wf2, bf2)
    vm = pltpu.VMEM
    in_scratch = [vm(a.shape, a.dtype) for a in args]
    scratch = in_scratch + [
        vm((BATCH, 128), F32),
        vm((LAYERS, BATCH, 128), F32),
        vm((ROWS, SEQ), F32),
        vm((ROWS, SEQ), BF16),
        vm((ROWS, 128), F32),
        vm((2 * N_SLOT, 8, 128), F32),
        vm((2 * N_SLOT, N_ROW, 8, 128), F32),
        vm((N_ROW, 8, WIDTH), F32),
        vm((N_ROW, 8, WIDTH), F32),
        vm((2, 8, FF_HALF), F32),
        vm((N_ROW, 8, FF_HALF), F32),
        vm((N_SLOT, N_ROW, ROWS + HALF, 128), BF16),
        vm((N_SLOT, N_ROW, ROWS + HALF, 128), BF16),
        vm((N_SLOT, N_ROW, HALF, 128), BF16),
        vm((N_SLOT, N_COL, ROWS, WIDTH), BF16),
        vm((STREAMS, ROWS, FF_HALF), F32),
        vm((N_SLOT, ROWS, FF_HALF), BF16),
        vm((N_SLOT, ROWS, FF_HALF), BF16),
        vm((N_SLOT, 2, ROWS, FF_HALF), BF16),
        vm((N_SLOT, 2, ROWS, FF_HALF), BF16),
        vm((N_SLOT, N_COL, ROWS, WIDTH), BF16),
        pltpu.SemaphoreType.DMA((32,)),
        pltpu.SemaphoreType.DMA((2 * N_SLOT,)),
        pltpu.SemaphoreType.DMA((N_COPY,)),
        pltpu.SemaphoreType.DMA((N_COPY,)),
    ]
    shapes = (jax.ShapeDtypeStruct((BATCH, WIDTH), BF16),
              jax.ShapeDtypeStruct((LAYERS, HEAD, BATCH), BF16),
              jax.ShapeDtypeStruct((LAYERS, HEAD, BATCH), BF16))
    vmem_spec = pl.BlockSpec(memory_space=pltpu.VMEM)
    results = pl.pallas_call(
        step_kernel,
        out_shape=tuple(vm(a.shape, a.dtype) for a in shapes),
        in_specs=[pl.BlockSpec(memory_space=pltpu.HBM)] * len(args),
        out_specs=(vmem_spec,) * 3,
        scratch_shapes=scratch,
        compiler_params=pltpu.CompilerParams(
            collective_id=0, has_side_effects=True, vmem_limit_bytes=60 * 1024 * 1024),
        name="decode_step",
    )(*args)
    h_out, k_new, v_new = pl.pallas_call(
        emit_kernel,
        out_shape=shapes,
        in_specs=[vmem_spec] * 3,
        out_specs=(any_spec,) * 3,
        scratch_shapes=[pltpu.SemaphoreType.DMA((3,))],
        compiler_params=pltpu.CompilerParams(vmem_limit_bytes=1024 * 1024),
        name="emit",
    )(*results)

    def fresh(rows):
        return jnp.swapaxes(rows, 1, 2).reshape(LAYERS, BATCH, 1, HEAD)

    return h_out, fresh(k_new), fresh(v_new)


def solution(mesh):
    act_spec = P("dp", "row")
    cache_spec = P(None, "dp", ("col", "row"), None, None)
    fresh_spec = P(None, "dp", ("col", "row"), None)
    in_weight = P(None, "row", "col")
    out_weight = P(None, "col", "row")
    col_vec = P(None, "col")
    row_vec = P(None, "row")
    in_specs = (act_spec, P("dp"), cache_spec, cache_spec, row_vec, row_vec,
                in_weight, col_vec, in_weight, col_vec, in_weight, col_vec,
                out_weight, row_vec, row_vec, row_vec, in_weight, col_vec, out_weight, row_vec)
    return jax.shard_map(run_step, mesh=mesh, in_specs=in_specs,
                         out_specs=(act_spec, fresh_spec, fresh_spec), check_vma=False)
```
